32 devices in a mesh: clip: 4 (over x, core), seq: 2 (over y), head: 4 (over z).
Axes of the slice: x: 2, y: 2, z: 4, core: 2. Of those that a mesh axis runs over, the one named last changes fastest.
Arguments:
- inputs: bfloat16 [4, 1500, 768], P('clip', 'seq'), may hold values from -6 to 6
- gain_one: bfloat16 [768], P(('clip', 'seq')), may hold values from 0.25 to 1.75
- shift_one: bfloat16 [768], P(('clip', 'seq')), may hold values from -1.75 to 1.75
- w_query: bfloat16 [768, 768], P(('clip', 'seq'), 'head'), may hold values from -0.21875 to 0.21875
- b_query: bfloat16 [768], P('head'), may hold values from -3 to 3
- w_key: bfloat16 [768, 768], P(('clip', 'seq'), 'head'), may hold values from -0.21875 to 0.21875
- w_value: bfloat16 [768, 768], P(('clip', 'seq'), 'head'), may hold values from -0.21875 to 0.21875
- b_value: bfloat16 [768], P('head'), may hold values from -0.3125 to 0.3125
- w_out: bfloat16 [768, 768], P('head', ('clip', 'seq')), may hold values from -3.5 to 3.5
- b_out: bfloat16 [768], P(('clip', 'seq')), may hold values from -3 to 3
- gain_two: bfloat16 [768], P(('clip', 'seq')), may hold values from 0.25 to 1.75
- shift_two: bfloat16 [768], P(('clip', 'seq')), may hold values from -1.75 to 1.75
- w_fc_one: bfloat16 [768, 3072], P(('clip', 'seq'), 'head'), may hold values from -0.21875 to 0.21875
- b_fc_one: bfloat16 [3072], P('head'), may hold values from -3 to 3
- w_fc_two: bfloat16 [3072, 768], P('head', ('clip', 'seq')), may hold values from -0.3125 to 0.3125
- b_fc_two: bfloat16 [768], P(('clip', 'seq')), may hold values from -3 to 3
- cotangent: bfloat16 [4, 1500, 768], P('clip', 'seq'), may hold values from -6 to 6
Outputs:
- outputs: bfloat16 [4, 1500, 768], P('clip', 'seq')
- input_gradient: float32 [4, 1500, 768], P('clip', 'seq')
- first_gain_gradient: float32 [768], P(('clip', 'seq'))
- grad_shift_one: float32 [768], P(('clip', 'seq'))
- grad_w_query: float32 [768, 768], P(('clip', 'seq'), 'head')
- grad_b_query: float32 [768], P('head')
- grad_w_key: float32 [768, 768], P(('clip', 'seq'), 'head')
- grad_w_value: float32 [768, 768], P(('clip', 'seq'), 'head')
- grad_b_value: float32 [768], P('head')
- grad_w_out: float32 [768, 768], P('head', ('clip', 'seq'))
- grad_b_out: float32 [768], P(('clip', 'seq'))
- second_gain_gradient: float32 [768], P(('clip', 'seq'))
- grad_shift_two: float32 [768], P(('clip', 'seq'))
- grad_w_fc_one: float32 [768, 3072], P(('clip', 'seq'), 'head')
- grad_b_fc_one: float32 [3072], P('head')
- grad_w_fc_two: float32 [3072, 768], P('head', ('clip', 'seq'))
- grad_b_fc_two: float32 [768], P(('clip', 'seq'))
The draws below stay inside these ranges and needn't reach their ends.
All inputs are finite; a program needn't handle non-finite values.
Results may differ from the reference program's by a relative error of at most 0.012.
Values may be sent and summed in bfloat16 or wider, within the bound.
A program may use at most 128 MiB of HBM per device.

```python
import jax
import jax.numpy as jnp
from jax import lax

D = 768
HEADS = 12
HEAD_DIM = 64
FF = 3072
FRAMES = 1500
CLIPS = 4


def with_spikes(entries, key, source, target, shards_of, factor):
    owner, partner = [(jnp.arange(entries.shape[dim]) // (entries.shape[dim] // shards_of)).reshape([-1 if axis == dim else 1 for axis in range(entries.ndim)]) for dim in (source, target)]
    chosen = jax.random.permutation(key, shards_of)[partner]
    strong = (owner == chosen) | (owner == (partner + shards_of // 2) % shards_of)
    return jnp.where(strong, factor * entries, entries)


def steps_of(own_key, shape, pieces, smallest, high):
    def one(axis_at, shards_of):
        draws = jax.random.uniform(jax.random.fold_in(jax.random.fold_in(own_key, 6), axis_at), (shards_of,), jnp.float32, smallest / len(pieces), high / len(pieces))
        return jnp.repeat(jnp.exp(draws), shape[axis_at] // shards_of).reshape((-1,) + (1,) * (len(shape) - axis_at - 1))

    loudness = one(*pieces[0])
    for cut in pieces[1:]:
        loudness = loudness * one(*cut)
    return loudness


def bell_draw(rng, dims, scale, reach, split=(), held_as=jnp.bfloat16):
    array = jax.random.normal(rng, dims, jnp.float32) * scale
    if len(split) > 0:
        array = steps_of(rng, dims, split, -0.22, 0.18) * array
    return jnp.clip(array, min=-reach, max=reach).astype(held_as)


def heavy_noise(rng, shape, deviation, most, shards, heavy, kind=jnp.bfloat16):
    values = deviation * jax.random.normal(rng, shape, jnp.float32)
    if shards:
        values = values * steps_of(rng, shape, shards, -0.22, 0.18)
    return jnp.clip(with_spikes(values, jax.random.fold_in(rng, 3), *heavy), -most, most).astype(kind)


def setup_inputs(seed: int = 0) -> dict:
    arg_keys = jax.random.split(jax.random.key(seed), 18)
    inputs = heavy_noise(arg_keys[0], (CLIPS, FRAMES, D), 1.0, 6.0, ((0, 4), (1, 2)), (0, 2, 4, 2.0))
    gain_one = jnp.clip(1.0 + 0.15 * jax.random.normal(arg_keys[1], (D,), jnp.float32), 0.25, 1.75).astype(jnp.bfloat16)
    shift_one = bell_draw(arg_keys[2], (D,), 0.3, 1.75, ((0, 8),))
    w_query = bell_draw(arg_keys[3], (D, HEADS * HEAD_DIM), D ** -0.5, 0.21875, ((0, 8), (1, 4)))
    b_query = bell_draw(arg_keys[4], (HEADS * HEAD_DIM,), 0.5, 3.0, ((0, 4),))
    w_key = bell_draw(arg_keys[5], (D, HEADS * HEAD_DIM), D ** -0.5, 0.21875, ((0, 8), (1, 4)))
    w_value = bell_draw(arg_keys[6], (D, HEADS * HEAD_DIM), D ** -0.5, 0.21875, ((0, 8), (1, 4)))
    b_value = bell_draw(arg_keys[7], (HEADS * HEAD_DIM,), 0.05, 0.3125, ((0, 4),))
    w_out = bell_draw(arg_keys[8], (HEADS * HEAD_DIM, D), (max(HEADS * HEAD_DIM // 256, 1)) ** -0.5, 3.5, ((0, 4), (1, 8)))
    b_out = bell_draw(arg_keys[9], (D,), 0.5, 3.0, ((0, 8),))
    gain_two = jnp.clip(1.0 + 0.15 * jax.random.normal(arg_keys[10], (D,), jnp.float32), 0.25, 1.75).astype(jnp.bfloat16)
    shift_two = bell_draw(arg_keys[11], (D,), 0.3, 1.75, ((0, 8),))
    w_fc_one = bell_draw(arg_keys[12], (D, FF), D ** -0.5, 0.21875, ((0, 8), (1, 4)))
    b_fc_one = bell_draw(arg_keys[13], (FF,), 0.5, 3.0, ((0, 4),))
    w_fc_two = bell_draw(arg_keys[14], (FF, D), (max(FF // 9, 1)) ** -0.5, 0.3125, ((0, 4), (1, 8)))
    b_fc_two = bell_draw(arg_keys[15], (D,), 0.5, 3.0, ((0, 8),))
    cotangent = heavy_noise(arg_keys[16], (CLIPS, FRAMES, D), 1.0, 6.0, ((0, 4), (1, 2)), (0, 2, 4, 2.0))
    return dict(inputs=inputs, gain_one=gain_one, shift_one=shift_one, w_query=w_query, b_query=b_query, w_key=w_key, w_value=w_value, b_value=b_value, w_out=w_out, b_out=b_out, gain_two=gain_two, shift_two=shift_two, w_fc_one=w_fc_one, b_fc_one=b_fc_one, w_fc_two=w_fc_two, b_fc_two=b_fc_two, cotangent=cotangent)


@jax.custom_vjp
def low(v):
    return lax.optimization_barrier(v.astype(jnp.bfloat16)).astype(jnp.float32)

@jax.custom_vjp
def low_back(v):
    return v

def low_keep(v):
    return (low(v), None)

def low_pass(kept, grad):
    return (grad,)

def back_keep(v):
    return (v, None)

def back_low(kept, grad):
    return (low(grad),)
low.defvjp(low_keep, low_pass)
low_back.defvjp(back_keep, back_low)
eps = 1e-05

def norm_rows(values, norm_gain, norm_shift):
    row_mean = lax.optimization_barrier(jnp.mean(values, axis=-1, keepdims=True))
    centered_values = values - row_mean
    spread = lax.optimization_barrier(jnp.mean(centered_values * centered_values, axis=-1, keepdims=True))
    return centered_values * lax.rsqrt(spread + eps) * norm_gain + norm_shift

def matmul(left, right):
    return jnp.dot(left, right, precision=lax.Precision.HIGHEST)

def clip_layer(params, clip_rows):
    gain_one, shift_one, w_query, b_query, w_key, w_value, b_value, w_out, b_out, gain_two, shift_two, w_fc_one, b_fc_one, w_fc_two, b_fc_two = params
    scale = HEAD_DIM ** (-0.5)
    normed_one = low(norm_rows(clip_rows, gain_one, shift_one))
    query = low(low_back(matmul(normed_one, w_query) + b_query))
    key = low(low_back(matmul(normed_one, w_key)))
    value = low(low_back(matmul(normed_one, w_value) + b_value))
    query_heads = query.reshape(FRAMES, HEADS, HEAD_DIM)
    key_heads = key.reshape(FRAMES, HEADS, HEAD_DIM)
    value_heads = value.reshape(FRAMES, HEADS, HEAD_DIM)
    scores = jnp.einsum('qhd,khd->hqk', query_heads, key_heads, precision=lax.Precision.HIGHEST)
    scores = low_back(scores * scale)
    probs = low(jax.nn.softmax(scores, axis=-1))
    attended = jnp.einsum('hqk,khd->qhd', probs, value_heads, precision=lax.Precision.HIGHEST)
    attended = low(low_back(attended.reshape(FRAMES, HEADS * HEAD_DIM)))
    middle_state = clip_rows + low_back(matmul(attended, w_out)) + b_out
    normed_two = low(norm_rows(middle_state, gain_two, shift_two))
    pre = low_back(matmul(normed_two, w_fc_one) + b_fc_one)
    act = low(jax.nn.gelu(pre, approximate=False))
    return middle_state + low_back(matmul(act, w_fc_two)) + b_fc_two

def reference(inputs, gain_one, shift_one, w_query, b_query, w_key, w_value, b_value, w_out, b_out, gain_two, shift_two, w_fc_one, b_fc_one, w_fc_two, b_fc_two, cotangent):
    params = tuple((p.astype(jnp.float32) for p in (gain_one, shift_one, w_query, b_query, w_key, w_value, b_value, w_out, b_out, gain_two, shift_two, w_fc_one, b_fc_one, w_fc_two, b_fc_two)))
    inputs_wide = inputs.astype(jnp.float32)

    def whole(params_in, rows_in):
        layer = jax.checkpoint(clip_layer)
        return lax.map(lambda clip_rows: layer(params_in, clip_rows), rows_in)
    outputs, pullback = jax.vjp(whole, params, inputs_wide)
    grads, input_gradient = pullback(cotangent.astype(jnp.float32))
    return (outputs.astype(jnp.bfloat16), input_gradient, grads[0], grads[1], grads[2], grads[3], grads[4], grads[5], grads[6], grads[7], grads[8], grads[9], grads[10], grads[11], grads[12], grads[13], grads[14])
```

```python
from functools import partial
import types

import jax
import jax.numpy as jnp
from jax import lax
from jax.experimental import pallas as pl
from jax.experimental.pallas import tpu as pltpu
from jax.sharding import PartitionSpec as P

HEAD_DIM = 64
EPS = 1e-05
F32 = jnp.float32
BF16 = jnp.bfloat16
MESH = pl.DeviceIdType.MESH


def flip(value, bit):
    return value + bit * (1 - 2 * lax.rem(lax.div(value, bit), 2))


def flips(value, mask, bits):
    for bit in bits:
        if mask & bit:
            value = flip(value, bit)
    return value


def powers(size):
    bits, bit = [], 1
    while bit < size:
        bits.append(bit)
        bit *= 2
    return bits


class Cube:
    def __init__(self, clips, seqs):
        self.clips, self.seqs, self.size = clips, seqs, clips * seqs
        self.seq_bits = [(bit, "seq", bit) for bit in powers(seqs)]
        self.clip_bits = [(bit * seqs, "clip", bit) for bit in powers(clips)]
        core, rest = self.clip_bits[:1], self.clip_bits[1:]
        self.orders = (
            self.seq_bits + rest + core,
            rest[:1] + self.seq_bits + rest[1:] + core,
        )
        self.all_bits = [bit for bit, _, _ in self.seq_bits + self.clip_bits]

    def rank(self):
        return lax.axis_index("clip") * self.seqs + lax.axis_index("seq")

    def block(self, mask):
        return flips(self.rank(), mask, self.all_bits)

    @staticmethod
    def peer(step):
        _, axis, bit = step
        return {axis: flip(lax.axis_index(axis), bit)}


class Sems:
    def __init__(self, send, recv):
        self.send, self.recv, self.used = send, recv, 0

    def take(self):
        self.used += 1
        return self.send.at[self.used - 1], self.recv.at[self.used - 1]


def remote(src, dst, sems, device):
    return pltpu.make_async_remote_copy(
        src_ref=src,
        dst_ref=dst,
        send_sem=sems[0],
        recv_sem=sems[1],
        device_id=device,
        device_id_type=MESH,
    )


class Gather:
    def __init__(self, cube, sems, view, colors):
        self.cube, self.view, self.colors = cube, view, colors
        self.steps = len(cube.orders[0])
        self.copies = [[[] for _ in range(self.steps)] for _ in range(colors)]
        for color in range(colors):
            masks = [0]
            for k, step in enumerate(cube.orders[color]):
                for mask in masks:
                    block = cube.block(mask)
                    piece = view(block, color)
                    self.copies[color][k].append(
                        remote(piece, piece, sems.take(), cube.peer(step))
                    )
                masks = masks + [mask ^ step[0] for mask in masks]

    def start(self, k):
        for color in range(self.colors):
            for copy in self.copies[color][k]:
                copy.start()

    def arrive(self, k):
        for color in range(self.colors):
            for copy in self.copies[color][k]:
                copy.wait_recv()

    def advance(self, k):
        for color in range(self.colors):
            for copy in self.copies[color][k]:
                copy.wait_recv()
            if k + 1 < self.steps:
                for copy in self.copies[color][k + 1]:
                    copy.start()

    def drain(self):
        for color in range(self.colors):
            for step in self.copies[color]:
                for copy in step:
                    copy.wait_send()


def normalize(rows):
    mean = jnp.mean(rows, axis=-1, keepdims=True)
    centered = rows - mean
    spread = jnp.mean(centered * centered, axis=-1, keepdims=True)
    inverse = lax.rsqrt(spread + EPS)
    return centered * inverse, inverse


def dot(a, b):
    return jnp.dot(a, b, preferred_element_type=F32)


def dot_nt(a, b):
    return lax.dot_general(a, b, (((1,), (1,)), ((), ())), preferred_element_type=F32)


def dot_tn(a, b):
    return lax.dot_general(a, b, (((0,), (0,)), ((), ())), preferred_element_type=F32)


NEG = -1e30


def fill(shape, value, dtype=F32):
    return jnp.full(shape, value, dtype)


def lane(shape):
    return lax.broadcasted_iota(jnp.int32, shape, len(shape) - 1)


class Line:
    def __init__(self, nodes, sems, view, parts):
        self.n, self.z = nodes, lax.axis_index("head")
        self.view = view
        self.right = [[sems.take() for _ in range(parts)] for _ in range(nodes - 1)]
        self.left = [[sems.take() for _ in range(parts)] for _ in range(nodes - 1)]

    def moves(self, hop, part):
        z, n = self.z, self.n

        def copy(origin, sems, target):
            piece = self.view(origin, part)
            return remote(piece, piece, sems, {"head": target})

        sends = (
            (
                (z >= hop) & (z < n - 1),
                lambda: copy(z - hop, self.right[hop][part], z + 1),
            ),
            (
                (n - 1 - z >= hop) & (z > 0),
                lambda: copy(z + hop, self.left[hop][part], z - 1),
            ),
        )
        arrivals = (
            (z > hop, lambda: copy(z - 1 - hop, self.right[hop][part], z - 1)),
            (n - 1 - z > hop, lambda: copy(z + 1 + hop, self.left[hop][part], z + 1)),
        )
        return sends, arrivals

    def start(self, hop, part):
        for condition, copy in self.moves(hop, part)[0]:
            pl.when(condition)(lambda copy=copy: copy().start())

    def arrive(self, hop, part):
        for condition, copy in self.moves(hop, part)[1]:
            pl.when(condition)(lambda copy=copy: copy().wait_recv())

    def drain(self, part):
        for hop in range(self.n - 1):
            for condition, copy in self.moves(hop, part)[0]:
                pl.when(condition)(lambda copy=copy: copy().wait_send())


def entry_barrier(cube, heads):
    barrier = pltpu.get_barrier_semaphore()
    z = lax.axis_index("head")
    peers = [cube.peer(step) for step in cube.orders[0]]
    peers += [{"head": lax.rem(z + d, heads)} for d in range(1, heads)]
    for peer in peers:
        pl.semaphore_signal(barrier, inc=1, device_id=peer, device_id_type=MESH)
    pl.semaphore_wait(barrier, len(peers))


def stage_one(m, cube, nz, sems):
    z = lax.axis_index("head")
    r = cube.rank()
    rows = m.wq.shape[0]
    colors = m.gq.shape[1]
    half = rows // colors
    nh = m.q.shape[0]
    frames = m.x.shape[0]
    padded = m.xp.shape[0]
    tile = 128
    tiles = padded // tile
    width = m.x.shape[1]

    gq = Gather(cube, sems, lambda b, c: m.gq.at[b, c], colors)
    gv = Gather(cube, sems, lambda b, c: m.gv.at[b], 1)
    g1 = Gather(cube, sems, lambda b, c: m.g1.at[b, c], colors)
    g2 = Gather(cube, sems, lambda b, c: m.g2.at[b, c], colors)
    go = Gather(cube, sems, lambda b, c: m.go.at[:, b, c], colors)

    m.gv[r] = m.vsh[...]
    for c in range(colors):
        part = pl.ds(c * half, half)
        for h in range(nh):
            cols = slice(h * HEAD_DIM, (h + 1) * HEAD_DIM)
            m.gq[r, c, :, h * 128 : h * 128 + 64] = m.wk[part, cols]
            m.gq[r, c, :, h * 128 + 64 : (h + 1) * 128] = m.wv[part, cols]
        m.gq[r, c, :, nh * 128 : nh * 128 + nh * 64] = m.wq[part, :]
        spare = m.gq.shape[3] - nh * 192
        if spare:
            m.gq[r, c, :, nh * 192 :] = fill((half, spare), 0, BF16)

    entry_barrier(cube, nz)
    gv.start(0)
    gq.start(0)

    wot = m.wo[...].T
    w2t = m.w2[...].T
    for c in range(colors):
        part = slice(c * half, (c + 1) * half)
        m.go[z, r, c] = wot[part]
        m.g2[r, c] = w2t[part]
        m.g1[r, c] = m.w1[part, :]
    out_sems = [sems.take() for _ in range(nz - 1)]

    def out_copies(arriving):
        for d in range(1, nz):
            origin = lax.rem(z + nz - d, nz) if arriving else z
            target = lax.rem(z + d, nz)
            piece = m.go.at[origin, r]
            yield remote(piece, piece, out_sems[d - 1], {"head": target})

    for copy in out_copies(False):
        copy.start()

    m.xp[0:frames] = m.x[...]
    m.xp[frames:padded] = fill((padded - frames, width), 0, BF16)

    def norm_tile(i, carry):
        at = pl.ds(pl.multiple_of(i * tile, tile), tile)
        xhat, inverse = normalize(m.xp[at].astype(F32))
        m.xh1[at] = xhat
        m.r1[at] = jnp.broadcast_to(inverse, (tile, 128))
        return carry

    third = tiles // cube_steps(gq)
    for k in range(gq.steps):
        top = tiles if k == gq.steps - 1 else third * (k + 1)
        lax.fori_loop(third * k, top, norm_tile, 0)
        gv.advance(k)
        gq.advance(k)
    for b in range(cube.size):
        m.vec[:, b * rows : (b + 1) * rows] = m.gv[b, :, :rows]
    g1.start(0)
    g2.start(0)

    gain, shift = m.vec[0:1, :], m.vec[1:2, :]
    bias = m.bias[0:1, : m.gq.shape[3]]
    scale = HEAD_DIM**-0.5

    def project(i, carry):
        at = pl.ds(pl.multiple_of(i * tile, tile), tile)
        n1 = (m.xh1[at] * gain + shift).astype(BF16)
        m.n1[at] = n1
        packed = dot(n1, m.gq[...].reshape(cube.size * rows, m.gq.shape[3])) + bias
        left = lane((tile, 128)) < 64
        for h in range(nh):
            m.kv[0, h, at] = packed[:, h * 128 : (h + 1) * 128].astype(BF16)
            base = nh * 128 + (h // 2) * 128
            pair = packed[:, base : base + 128]
            if h % 2:
                pair = pltpu.roll(pair, 64, 1)
            pair = pair.astype(BF16).astype(F32) * scale
            m.q[h, at] = jnp.where(left, pair, 0.0).astype(BF16)
        return carry

    lax.fori_loop(0, tiles, project, 0)

    kv_sems = [sems.take() for _ in range(nh)]
    other = {"seq": flip(lax.axis_index("seq"), 1)}
    kv_copies = [
        remote(m.kv.at[0, h], m.kv.at[1, h], kv_sems[h], other) for h in range(nh)
    ]
    for copy in kv_copies:
        copy.start()
    for copy in out_copies(True):
        copy.wait_recv()
    go.start(0)

    left = lane((padded, 128)) < 64

    def prepare(part, h):
        block = m.kv[part, h]
        m.kvt[part, h] = block.T
        m.vo[part, h] = jnp.where(left, jnp.ones_like(block), block)

    for h in range(nh):
        prepare(0, h)

    line = Line(nz, sems, lambda origin, part: m.attz.at[origin, part], nh)
    block = 256
    valid = frames - (padded - 128)

    def attend(h):
        def one(b, carry):
            at = pl.ds(pl.multiple_of(b * block, block), block)
            query = m.q[h, at]
            keep = lane((block, 128)) < valid
            parts = []
            top = None
            for part in range(2):
                s = dot(query, m.kvt[part, h])
                body, tail = s[:, : padded - 128], s[:, padded - 128 :]
                tail = jnp.where(keep, tail, NEG)
                parts += [body, tail]
                high = jnp.maximum(jnp.max(body, axis=1, keepdims=True), jnp.max(tail, axis=1, keepdims=True))
                top = high if top is None else jnp.maximum(top, high)
            place = 0
            for s in parts:
                m.p[h, at, place : place + s.shape[1]] = jnp.exp(s - top).astype(BF16)
                place += s.shape[1]
            acc = dot(m.p[h, at, :padded], m.vo[0, h]) + dot(m.p[h, at, padded:], m.vo[1, h])
            inverse = 1.0 / pltpu.roll(acc, 64, 1)
            att = acc * inverse
            right = lane((block, 128)) >= 64
            m.il[h, at] = jnp.where(right, inverse, 0.0)
            m.atto[h, at] = jnp.where(right, att, 0.0).astype(BF16)
            turned = pltpu.roll(att, 64, 1)
            packed = jnp.where(right[: block // 2], att[block // 2 :], turned[: block // 2])
            to = pl.ds(pl.multiple_of(b * (block // 2), block // 2), block // 2)
            m.attz[z, h, to] = packed.astype(BF16)
            return carry

        lax.fori_loop(0, padded // block, one, 0)

    last = g1.steps - 1
    for h in range(nh):
        kv_copies[h].wait_recv()
        prepare(1, h)
        attend(h)
        line.start(0, h)
        if h < g1.steps:
            for g in (g1, g2, go):
                g.advance(h)
        if h:
            line.arrive(0, h - 1)
            line.start(1, h - 1)
        if h > 1:
            line.arrive(1, h - 2)
            line.start(2, h - 2)
    for k in range(min(nh, g1.steps), g1.steps):
        for g in (g1, g2, go):
            g.advance(k)
    for hop in range(nz - 1):
        for h in range(nh):
            done = nh - 1 - h
            if hop >= done:
                line.arrive(hop, h)
                if hop + 1 < nz - 1:
                    line.start(hop + 1, h)

    for copy in kv_copies:
        copy.wait_send()
    for copy in out_copies(False):
        copy.wait_send()
    for g in (gv, gq, g1, g2, go):
        g.drain()
    for h in range(nh):
        line.drain(h)


def cube_steps(gather):
    return gather.steps


def front(inputs, vectors, biases, w_query, w_key, w_value, w_out, w_fc_one, w_fc_two, mesh_shape):
    nz = mesh_shape["head"]
    cube = Cube(mesh_shape["clip"], mesh_shape["seq"])
    frames, width = inputs.shape
    rows, local = w_query.shape
    hidden = w_fc_one.shape[1]
    nh = local // HEAD_DIM
    padded = -(-frames // 256) * 256
    colors = 2 if rows % 32 == 0 else 1
    half = rows // colors
    packed = -(-(nh * 192) // 128) * 128
    outs = dict(
        n1=((padded, width), BF16),
        q=((nh, padded, 128), BF16),
        kv=((2, nh, padded, 128), BF16),
        atto=((nh, padded, 128), BF16),
        attz=((nz, nh, padded // 2, 128), BF16),
        gq=((cube.size, colors, half, packed), BF16),
        go=((nz, cube.size, colors, half, local), BF16),
        g1=((cube.size, colors, half, hidden), BF16),
        g2=((cube.size, colors, half, hidden), BF16),
        vec=((8, width), F32),
    )
    scratch = dict(
        gv=((cube.size, 8, 128), F32),
        xp=((padded, width), BF16),
        xh1=((padded, width), F32),
        r1=((padded, 128), F32),
        kvt=((2, nh, 128, padded), BF16),
        vo=((2, nh, padded, 128), BF16),
        p=((nh, padded, 2 * padded), BF16),
        il=((nh, padded, 128), F32),
    )
    ins = dict(x=inputs, vsh=vectors, bias=biases, wq=w_query, wk=w_key, wv=w_value, wo=w_out, w1=w_fc_one, w2=w_fc_two)
    count = 200

    def body(*refs):
        names = list(ins) + list(outs) + list(scratch)
        m = types.SimpleNamespace(**dict(zip(names, refs)))
        sems = Sems(*refs[len(names):])
        stage_one(m, cube, nz, sems)

    res = pl.pallas_call(
        body,
        out_shape=[jax.ShapeDtypeStruct(*v) for v in outs.values()],
        in_specs=[pl.BlockSpec(memory_space=pltpu.VMEM)] * len(ins),
        out_specs=[pl.BlockSpec(memory_space=pltpu.VMEM)] * len(outs),
        scratch_shapes=[pltpu.VMEM(*v) for v in scratch.values()] + [pltpu.SemaphoreType.DMA((count,))] * 2,
        compiler_params=pltpu.CompilerParams(collective_id=0, has_side_effects=True, vmem_limit_bytes=60 * 2**20),
        name="front",
    )(*ins.values())
    return types.SimpleNamespace(**dict(zip(outs, res)))


def vector_pack(vectors):
    stack = jnp.stack([v.astype(F32) for v in vectors])
    return jnp.pad(stack, ((0, 8 - stack.shape[0]), (0, 128 - stack.shape[1])))


def biases_pack(b_query, b_value, b_fc_one, heads):
    zero = jnp.zeros((HEAD_DIM,), F32)
    parts = []
    for h in range(heads):
        parts += [zero, b_value[h * HEAD_DIM : (h + 1) * HEAD_DIM].astype(F32)]
    row = jnp.concatenate(parts + [b_query.astype(F32)])
    width = b_fc_one.shape[0]
    row = jnp.pad(row, (0, width - row.shape[0]))
    return jnp.pad(jnp.stack([row, b_fc_one.astype(F32)]), ((0, 6), (0, 0)))

def layer_norm_forward(values, norm_gain, norm_shift):
    row_mean = jnp.mean(values, axis=-1, keepdims=True)
    centered_values = values - row_mean
    spread = jnp.mean(centered_values * centered_values, axis=-1, keepdims=True)
    inverse_deviation = lax.rsqrt(spread + EPS)
    standardized = centered_values * inverse_deviation
    return (standardized * norm_gain + norm_shift, standardized, inverse_deviation)


def layer_norm_backward(output_gradient, standardized, inverse_deviation, norm_gain):
    scaled_rows = output_gradient * norm_gain
    first_row_mean = jnp.mean(scaled_rows, axis=-1, keepdims=True)
    second_row_mean = jnp.mean(scaled_rows * standardized, axis=-1, keepdims=True)
    return inverse_deviation * (scaled_rows - first_row_mean - standardized * second_row_mean)


def fetch_weights(
    gain_one,
    shift_one,
    w_query,
    w_key,
    w_value,
    b_out,
    gain_two,
    shift_two,
    w_fc_one,
    b_fc_two,
    w_out,
    w_fc_two,
):
    rows = (
        lax.all_gather(gain_one, ("clip", "seq"), axis=0, tiled=True),
        lax.all_gather(shift_one, ("clip", "seq"), axis=0, tiled=True),
        lax.all_gather(w_query, ("clip", "seq"), axis=0, tiled=True),
        lax.all_gather(w_key, ("clip", "seq"), axis=0, tiled=True),
        lax.all_gather(w_value, ("clip", "seq"), axis=0, tiled=True),
        lax.all_gather(b_out, ("clip", "seq"), axis=0, tiled=True),
        lax.all_gather(gain_two, ("clip", "seq"), axis=0, tiled=True),
        lax.all_gather(shift_two, ("clip", "seq"), axis=0, tiled=True),
        lax.all_gather(w_fc_one, ("clip", "seq"), axis=0, tiled=True),
        lax.all_gather(b_fc_two, ("clip", "seq"), axis=0, tiled=True),
    )
    columns = (
        lax.all_gather(w_out, ("clip", "seq"), axis=1, tiled=True),
        lax.all_gather(w_fc_two, ("clip", "seq"), axis=1, tiled=True),
    )
    return (rows, columns)


def head_total(partial_sum):
    return lax.psum(partial_sum, "head")


def on_device(
    inputs,
    gain_one,
    shift_one,
    w_query,
    b_query,
    w_key,
    w_value,
    b_value,
    w_out,
    b_out,
    gain_two,
    shift_two,
    w_fc_one,
    b_fc_one,
    w_fc_two,
    b_fc_two,
    cotangent,
    mesh_shape=None,
):
    clips, frames, width = inputs.shape
    local = w_query.shape[1]
    heads = local // HEAD_DIM
    scale = HEAD_DIM ** (-0.5)
    gathered_rows = jnp.float32
    count = clips * frames
    token_rows = inputs.astype(jnp.float32).reshape(count, width)
    wide = biases_pack(b_query, b_value, b_fc_one, heads)
    vectors = vector_pack((gain_one, shift_one, gain_two, shift_two, b_out, b_fc_two))
    f = front(inputs.reshape(count, width), vectors, wide, w_query, w_key, w_value, w_out, w_fc_one, w_fc_two, mesh_shape)
    gq = f.gq.reshape(width, -1)
    full_key = jnp.concatenate([gq[:, i*128:i*128+64] for i in range(heads)], 1)
    full_value = jnp.concatenate([gq[:, i*128+64:i*128+128] for i in range(heads)], 1)
    full_query = gq[:, heads*128:heads*192]
    z = lax.axis_index("head")
    full_out = lax.dynamic_index_in_dim(f.go.reshape(4, width, local), z, 0, False).T
    full_fc_one = f.g1.reshape(width, -1)
    full_fc_two = f.g2.reshape(width, -1).T
    v = f.vec
    first_norm_gain, second_norm_gain = v[0], v[2]
    gathered_first_shift, gathered_second_shift, full_b_out, full_b_fc_two = v[1], v[3], v[4], v[5]
    normalized_gathered, first_standardized, first_inverse_deviation = layer_norm_forward(
        token_rows, first_norm_gain, gathered_first_shift.astype(gathered_rows)
    )
    normed_one = f.n1[:count]
    query = jnp.concatenate([f.q[i, :count, :64] for i in range(heads)], 1) * 8
    query_clips = query.reshape(clips, frames, local)
    sq = lax.axis_index("seq")
    kvs = jnp.where(sq == 0, f.kv, f.kv[::-1])[:, :, :count]
    key_all = jnp.concatenate([jnp.concatenate([kvs[p, i, :, :64] for i in range(heads)], 1) for p in range(2)], 0)[None]
    value_all = jnp.concatenate([jnp.concatenate([kvs[p, i, :, 64:] for i in range(heads)], 1) for p in range(2)], 0)[None]
    attended = jnp.concatenate([f.atto[i, :count, 64:] for i in range(heads)], 1)
    log_totals = None
    pk = f.attz.reshape(4, heads, 3, 128, 2, 64).transpose(2, 4, 3, 0, 1, 5).reshape(768, 768)[:count]
    full_out_all = f.go.transpose(0, 4, 1, 2, 3).reshape(width, width)
    attn_all = jnp.dot(pk, full_out_all, preferred_element_type=gathered_rows)
    attn_terms = jnp.dot(attended, full_out, preferred_element_type=gathered_rows)
    middle_state = token_rows + attn_all + full_b_out.astype(gathered_rows)
    normalized_middle, second_standardized, second_inverse_deviation = layer_norm_forward(
        middle_state, second_norm_gain, gathered_second_shift.astype(gathered_rows)
    )
    normed_two = normalized_middle.astype(jnp.bfloat16)
    pre = jnp.dot(normed_two, full_fc_one, preferred_element_type=gathered_rows) + b_fc_one.astype(
        gathered_rows
    )
    act = jax.nn.gelu(pre, approximate=False).astype(jnp.bfloat16)
    ffn_terms = jnp.dot(act, full_fc_two, preferred_element_type=gathered_rows)
    outputs = (middle_state + head_total(ffn_terms) + full_b_fc_two.astype(gathered_rows)).astype(
        jnp.bfloat16
    )
    upstream_gradient = cotangent.astype(gathered_rows).reshape(count, width)
    grad_b_fc_two = jnp.sum(upstream_gradient, axis=0)
    grad_top_low = upstream_gradient.astype(jnp.bfloat16)
    grad_w_fc_two = jnp.einsum("tf,td->fd", act, grad_top_low, preferred_element_type=gathered_rows)
    grad_act = jnp.einsum(
        "td,fd->tf", grad_top_low, full_fc_two, preferred_element_type=gathered_rows
    )
    unused, gelu_back = jax.vjp(partial(jax.nn.gelu, approximate=False), pre)
    grad_pre = gelu_back(grad_act)[0].astype(jnp.bfloat16)
    grad_b_fc_one = jnp.sum(grad_pre.astype(gathered_rows), axis=0)
    grad_w_fc_one = jnp.einsum(
        "td,tf->df", normed_two, grad_pre, preferred_element_type=gathered_rows
    )
    normed_two_terms = jnp.einsum(
        "tf,df->td", grad_pre, full_fc_one, preferred_element_type=gathered_rows
    )
    second_normalized_gradient = head_total(normed_two_terms)
    middle_gradient = upstream_gradient + layer_norm_backward(
        second_normalized_gradient, second_standardized, second_inverse_deviation, second_norm_gain
    )
    grad_mid_low = middle_gradient.astype(jnp.bfloat16)
    second_gain_gradient = jnp.sum(second_normalized_gradient * second_standardized, axis=0)
    grad_shift_two = jnp.sum(second_normalized_gradient, axis=0)
    grad_b_out = jnp.sum(middle_gradient, axis=0)
    grad_w_out = jnp.einsum(
        "tj,td->jd", attended, grad_mid_low, preferred_element_type=gathered_rows
    )
    grad_attended = jnp.einsum(
        "td,jd->tj", grad_mid_low, full_out, preferred_element_type=gathered_rows
    ).astype(jnp.bfloat16)

    def attend_back(block):
        query_block, key_block, value_block, grad_block = block
        query_heads = query_block.reshape(frames, heads, HEAD_DIM)
        key_heads = key_block.reshape(-1, heads, HEAD_DIM)
        value_heads = value_block.reshape(-1, heads, HEAD_DIM)
        grad_heads = grad_block.reshape(frames, heads, HEAD_DIM)
        scores = (
            jnp.einsum("qhd,khd->hqk", query_heads, key_heads, preferred_element_type=gathered_rows)
            * scale
        )
        probs = jax.nn.softmax(scores, axis=-1)
        grad_values = jnp.einsum(
            "hqk,qhd->khd",
            probs.astype(jnp.bfloat16),
            grad_heads,
            preferred_element_type=gathered_rows,
        )
        grad_probs = jnp.einsum(
            "qhd,khd->hqk", grad_heads, value_heads, preferred_element_type=gathered_rows
        )
        inner = jnp.sum(probs * grad_probs, axis=-1, keepdims=True)
        grad_scores = (probs * (grad_probs - inner)).astype(jnp.bfloat16)
        grad_queries = (
            jnp.einsum("hqk,khd->qhd", grad_scores, key_heads, preferred_element_type=gathered_rows)
            * scale
        )
        grad_keys = (
            jnp.einsum(
                "hqk,qhd->khd", grad_scores, query_heads, preferred_element_type=gathered_rows
            )
            * scale
        )
        return (
            grad_queries.reshape(frames, local).astype(jnp.bfloat16),
            grad_keys.reshape(-1, local),
            grad_values.reshape(-1, local),
        )

    grad_query_clips, grad_key_all, grad_value_all = lax.map(
        attend_back,
        (query_clips, key_all, value_all, grad_attended.reshape(clips, frames, local)),
    )
    grad_key_own, grad_value_own = (
        lax.psum_scatter(grad_key_all, "seq", scatter_dimension=1, tiled=True),
        lax.psum_scatter(grad_value_all, "seq", scatter_dimension=1, tiled=True),
    )
    grad_query = grad_query_clips.reshape(count, local)
    grad_key = grad_key_own.reshape(count, local).astype(jnp.bfloat16)
    grad_value = grad_value_own.reshape(count, local).astype(jnp.bfloat16)
    grad_b_query = jnp.sum(grad_query.astype(gathered_rows), axis=0)
    grad_b_value = jnp.sum(grad_value.astype(gathered_rows), axis=0)
    grad_w_query = jnp.einsum(
        "td,tj->dj", normed_one, grad_query, preferred_element_type=gathered_rows
    )
    grad_w_key = jnp.einsum("td,tj->dj", normed_one, grad_key, preferred_element_type=gathered_rows)
    grad_w_value = jnp.einsum(
        "td,tj->dj", normed_one, grad_value, preferred_element_type=gathered_rows
    )
    grad_normed_part = jnp.einsum(
        "tj,dj->td", grad_query, full_query, preferred_element_type=gathered_rows
    )
    grad_normed_part = grad_normed_part + jnp.einsum(
        "tj,dj->td", grad_key, full_key, preferred_element_type=gathered_rows
    )
    grad_normed_part = grad_normed_part + jnp.einsum(
        "tj,dj->td", grad_value, full_value, preferred_element_type=gathered_rows
    )
    first_normalized_gradient = head_total(grad_normed_part)
    first_gain_gradient = jnp.sum(first_normalized_gradient * first_standardized, axis=0)
    grad_shift_one = jnp.sum(first_normalized_gradient, axis=0)
    input_gradient = middle_gradient + layer_norm_backward(
        first_normalized_gradient, first_standardized, first_inverse_deviation, first_norm_gain
    )
    owned_rows = (
        lax.psum_scatter(first_gain_gradient, ("clip", "seq"), scatter_dimension=0, tiled=True),
        lax.psum_scatter(grad_shift_one, ("clip", "seq"), scatter_dimension=0, tiled=True),
        lax.psum_scatter(grad_w_query, ("clip", "seq"), scatter_dimension=0, tiled=True),
        lax.psum_scatter(grad_w_key, ("clip", "seq"), scatter_dimension=0, tiled=True),
        lax.psum_scatter(grad_w_value, ("clip", "seq"), scatter_dimension=0, tiled=True),
        lax.psum_scatter(grad_b_out, ("clip", "seq"), scatter_dimension=0, tiled=True),
        lax.psum_scatter(second_gain_gradient, ("clip", "seq"), scatter_dimension=0, tiled=True),
        lax.psum_scatter(grad_shift_two, ("clip", "seq"), scatter_dimension=0, tiled=True),
        lax.psum_scatter(grad_w_fc_one, ("clip", "seq"), scatter_dimension=0, tiled=True),
        lax.psum_scatter(grad_b_fc_two, ("clip", "seq"), scatter_dimension=0, tiled=True),
    )
    owned_columns = (
        lax.psum_scatter(grad_w_out, ("clip", "seq"), scatter_dimension=1, tiled=True),
        lax.psum_scatter(grad_w_fc_two, ("clip", "seq"), scatter_dimension=1, tiled=True),
    )
    bias_totals = lax.psum((grad_b_query, grad_b_value, grad_b_fc_one), ("clip", "seq"))
    return (
        outputs.reshape(clips, frames, width),
        input_gradient.reshape(clips, frames, width),
        owned_rows[0],
        owned_rows[1],
        owned_rows[2],
        bias_totals[0],
        owned_rows[3],
        owned_rows[4],
        bias_totals[1],
        owned_columns[0],
        owned_rows[5],
        owned_rows[6],
        owned_rows[7],
        owned_rows[8],
        bias_totals[2],
        owned_columns[1],
        owned_rows[9],
    )


def solution(mesh):
    return jax.shard_map(
        partial(on_device, mesh_shape=dict(mesh.shape)),
        mesh=mesh,
        in_specs=(
            P("clip", "seq", None),
            P(("clip", "seq")),
            P(("clip", "seq")),
            P(("clip", "seq"), "head"),
            P("head"),
            P(("clip", "seq"), "head"),
            P(("clip", "seq"), "head"),
            P("head"),
            P("head", ("clip", "seq")),
            P(("clip", "seq")),
            P(("clip", "seq")),
            P(("clip", "seq")),
            P(("clip", "seq"), "head"),
            P("head"),
            P("head", ("clip", "seq")),
            P(("clip", "seq")),
            P("clip", "seq", None),
        ),
        out_specs=(
            P("clip", "seq", None),
            P("clip", "seq", None),
            P(("clip", "seq")),
            P(("clip", "seq")),
            P(("clip", "seq"), "head"),
            P("head"),
            P(("clip", "seq"), "head"),
            P(("clip", "seq"), "head"),
            P("head"),
            P("head", ("clip", "seq")),
            P(("clip", "seq")),
            P(("clip", "seq")),
            P(("clip", "seq")),
            P(("clip", "seq"), "head"),
            P("head"),
            P("head", ("clip", "seq")),
            P(("clip", "seq")),
        ),
        check_vma=False,
    )
```

```python
from functools import partial
import types

import jax
import jax.numpy as jnp
from jax import lax
from jax.experimental import pallas as pl
from jax.experimental.pallas import tpu as pltpu
from jax.sharding import PartitionSpec as P

HEAD_DIM = 64
EPS = 1e-05
F32 = jnp.float32
BF16 = jnp.bfloat16
MESH = pl.DeviceIdType.MESH


def flip(value, bit):
    return value + bit * (1 - 2 * lax.rem(lax.div(value, bit), 2))


def flips(value, mask, bits):
    for bit in bits:
        if mask & bit:
            value = flip(value, bit)
    return value


def powers(size):
    bits, bit = [], 1
    while bit < size:
        bits.append(bit)
        bit *= 2
    return bits


class Cube:
    def __init__(self, clips, seqs):
        self.clips, self.seqs, self.size = clips, seqs, clips * seqs
        self.seq_bits = [(bit, "seq", bit) for bit in powers(seqs)]
        self.clip_bits = [(bit * seqs, "clip", bit) for bit in powers(clips)]
        core, rest = self.clip_bits[:1], self.clip_bits[1:]
        self.orders = (
            self.seq_bits + rest + core,
            rest[:1] + self.seq_bits + rest[1:] + core,
        )
        self.all_bits = [bit for bit, _, _ in self.seq_bits + self.clip_bits]

    def rank(self):
        return lax.axis_index("clip") * self.seqs + lax.axis_index("seq")

    def block(self, mask):
        return flips(self.rank(), mask, self.all_bits)

    @staticmethod
    def peer(step):
        _, axis, bit = step
        return {axis: flip(lax.axis_index(axis), bit)}


class Sems:
    def __init__(self, send, recv):
        self.send, self.recv, self.used = send, recv, 0

    def take(self):
        self.used += 1
        return self.send.at[self.used - 1], self.recv.at[self.used - 1]


def remote(src, dst, sems, device):
    return pltpu.make_async_remote_copy(
        src_ref=src,
        dst_ref=dst,
        send_sem=sems[0],
        recv_sem=sems[1],
        device_id=device,
        device_id_type=MESH,
    )


class Gather:
    def __init__(self, cube, sems, view, colors):
        self.cube, self.view, self.colors = cube, view, colors
        self.steps = len(cube.orders[0])
        self.copies = [[[] for _ in range(self.steps)] for _ in range(colors)]
        for color in range(colors):
            masks = [0]
            for k, step in enumerate(cube.orders[color]):
                for mask in masks:
                    block = cube.block(mask)
                    piece = view(block, color)
                    self.copies[color][k].append(
                        remote(piece, piece, sems.take(), cube.peer(step))
                    )
                masks = masks + [mask ^ step[0] for mask in masks]

    def start(self, k):
        for color in range(self.colors):
            for copy in self.copies[color][k]:
                copy.start()

    def arrive(self, k):
        for color in range(self.colors):
            for copy in self.copies[color][k]:
                copy.wait_recv()

    def advance(self, k):
        for color in range(self.colors):
            for copy in self.copies[color][k]:
                copy.wait_recv()
            if k + 1 < self.steps:
                for copy in self.copies[color][k + 1]:
                    copy.start()

    def drain(self):
        for color in range(self.colors):
            for step in self.copies[color]:
                for copy in step:
                    copy.wait_send()


def normalize(rows):
    mean = jnp.mean(rows, axis=-1, keepdims=True)
    centered = rows - mean
    spread = jnp.mean(centered * centered, axis=-1, keepdims=True)
    inverse = lax.rsqrt(spread + EPS)
    return centered * inverse, inverse


def dot(a, b):
    return jnp.dot(a, b, preferred_element_type=F32)


def dot_nt(a, b):
    return lax.dot_general(a, b, (((1,), (1,)), ((), ())), preferred_element_type=F32)


def dot_tn(a, b):
    return lax.dot_general(a, b, (((0,), (0,)), ((), ())), preferred_element_type=F32)


NEG = -1e30


def fill(shape, value, dtype=F32):
    return jnp.full(shape, value, dtype)


def lane(shape):
    return lax.broadcasted_iota(jnp.int32, shape, len(shape) - 1)


class Line:
    def __init__(self, nodes, sems, view, parts):
        self.n, self.z = nodes, lax.axis_index("head")
        self.view = view
        self.right = [[sems.take() for _ in range(parts)] for _ in range(nodes - 1)]
        self.left = [[sems.take() for _ in range(parts)] for _ in range(nodes - 1)]

    def moves(self, hop, part):
        z, n = self.z, self.n

        def copy(origin, sems, target):
            piece = self.view(origin, part)
            return remote(piece, piece, sems, {"head": target})

        sends = (
            (
                (z >= hop) & (z < n - 1),
                lambda: copy(z - hop, self.right[hop][part], z + 1),
            ),
            (
                (n - 1 - z >= hop) & (z > 0),
                lambda: copy(z + hop, self.left[hop][part], z - 1),
            ),
        )
        arrivals = (
            (z > hop, lambda: copy(z - 1 - hop, self.right[hop][part], z - 1)),
            (n - 1 - z > hop, lambda: copy(z + 1 + hop, self.left[hop][part], z + 1)),
        )
        return sends, arrivals

    def start(self, hop, part):
        for condition, copy in self.moves(hop, part)[0]:
            pl.when(condition)(lambda copy=copy: copy().start())

    def arrive(self, hop, part):
        for condition, copy in self.moves(hop, part)[1]:
            pl.when(condition)(lambda copy=copy: copy().wait_recv())

    def drain(self, part):
        for hop in range(self.n - 1):
            for condition, copy in self.moves(hop, part)[0]:
                pl.when(condition)(lambda copy=copy: copy().wait_send())


def entry_barrier(cube, heads):
    barrier = pltpu.get_barrier_semaphore()
    z = lax.axis_index("head")
    peers = [cube.peer(step) for step in cube.orders[0]]
    peers += [{"head": lax.rem(z + d, heads)} for d in range(1, heads)]
    for peer in peers:
        pl.semaphore_signal(barrier, inc=1, device_id=peer, device_id_type=MESH)
    pl.semaphore_wait(barrier, len(peers))


def stage_one(m, cube, nz, sems):
    z = lax.axis_index("head")
    r = cube.rank()
    rows = m.wq.shape[0]
    colors = m.gq.shape[1]
    half = rows // colors
    nh = m.q.shape[0]
    frames = m.x.shape[0]
    padded = m.xp.shape[0]
    tile = 128
    tiles = padded // tile
    width = m.x.shape[1]

    gq = Gather(cube, sems, lambda b, c: m.gq.at[b, c], colors)
    gv = Gather(cube, sems, lambda b, c: m.gv.at[b], 1)
    g1 = Gather(cube, sems, lambda b, c: m.g1.at[b, c], colors)
    g2 = Gather(cube, sems, lambda b, c: m.g2.at[b, c], colors)
    go = Gather(cube, sems, lambda b, c: m.go.at[:, b, c], colors)

    m.gv[r] = m.vsh[...]
    for c in range(colors):
        part = pl.ds(c * half, half)
        for h in range(nh):
            cols = slice(h * HEAD_DIM, (h + 1) * HEAD_DIM)
            m.gq[r, c, :, h * 128 : h * 128 + 64] = m.wk[part, cols]
            m.gq[r, c, :, h * 128 + 64 : (h + 1) * 128] = m.wv[part, cols]
        m.gq[r, c, :, nh * 128 : nh * 128 + nh * 64] = m.wq[part, :]
        spare = m.gq.shape[3] - nh * 192
        if spare:
            m.gq[r, c, :, nh * 192 :] = fill((half, spare), 0, BF16)

    entry_barrier(cube, nz)
    gv.start(0)
    gq.start(0)

    wot = m.wo[...].T
    w2t = m.w2[...].T
    for c in range(colors):
        part = slice(c * half, (c + 1) * half)
        m.go[z, r, c] = wot[part]
        m.g2[r, c] = w2t[part]
        m.g1[r, c] = m.w1[part, :]
    out_sems = [sems.take() for _ in range(nz - 1)]

    def out_copies(arriving):
        for d in range(1, nz):
            origin = lax.rem(z + nz - d, nz) if arriving else z
            target = lax.rem(z + d, nz)
            piece = m.go.at[origin, r]
            yield remote(piece, piece, out_sems[d - 1], {"head": target})

    for copy in out_copies(False):
        copy.start()

    m.xp[0:frames] = m.x[...]
    m.xp[frames:padded] = fill((padded - frames, width), 0, BF16)

    def norm_tile(i, carry):
        at = pl.ds(pl.multiple_of(i * tile, tile), tile)
        xhat, _ = normalize(m.xp[at].astype(F32))
        m.xh2[at] = xhat
        return carry

    third = tiles // gq.steps
    for k in range(gq.steps):
        top = tiles if k == gq.steps - 1 else third * (k + 1)
        lax.fori_loop(third * k, top, norm_tile, 0)
        gv.advance(k)
        gq.advance(k)
    for b in range(cube.size):
        m.vec[:, b * rows : (b + 1) * rows] = m.gv[b, :, :rows]
    g1.start(0)
    g2.start(0)

    gain, shift = m.vec[0:1, :], m.vec[1:2, :]
    bias = m.bias[0:1, : m.gq.shape[3]]
    scale = HEAD_DIM**-0.5

    def project(i, carry):
        at = pl.ds(pl.multiple_of(i * tile, tile), tile)
        n1 = (m.xh2[at] * gain + shift).astype(BF16)
        m.n1[at] = n1
        packed = dot(n1, m.gq[...].reshape(cube.size * rows, m.gq.shape[3])) + bias
        left = lane((tile, 128)) < 64
        for h in range(nh):
            m.kv[0, h, at] = packed[:, h * 128 : (h + 1) * 128].astype(BF16)
            base = nh * 128 + (h // 2) * 128
            pair = packed[:, base : base + 128]
            if h % 2:
                pair = pltpu.roll(pair, 64, 1)
            pair = pair.astype(BF16).astype(F32) * scale
            m.q[h, at] = jnp.where(left, pair, 0.0).astype(BF16)
        return carry

    lax.fori_loop(0, tiles, project, 0)

    kv_sems = [sems.take() for _ in range(nh)]
    other = {"seq": flip(lax.axis_index("seq"), 1)}
    kv_copies = [
        remote(m.kv.at[0, h], m.kv.at[1, h], kv_sems[h], other) for h in range(nh)
    ]
    for copy in kv_copies:
        copy.start()
    for copy in out_copies(True):
        copy.wait_recv()
    go.start(0)

    left = lane((padded, 128)) < 64

    def prepare(part, h):
        block = m.kv[part, h]
        m.kvt[part, h] = block.T
        m.vo[part, h] = jnp.where(left, jnp.ones_like(block), block)

    for h in range(nh):
        prepare(0, h)

    line = Line(nz, sems, lambda origin, part: m.attz.at[origin, part], nh)
    block = 256
    valid = frames - (padded - 128)

    def attend(h):
        def one(b, carry):
            at = pl.ds(pl.multiple_of(b * block, block), block)
            query = m.q[h, at]
            keep = lane((block, 128)) < valid
            parts = []
            top = None
            for part in range(2):
                s = dot(query, m.kvt[part, h])
                body, tail = s[:, : padded - 128], s[:, padded - 128 :]
                tail = jnp.where(keep, tail, NEG)
                parts += [body, tail]
                high = jnp.maximum(jnp.max(body, axis=1, keepdims=True), jnp.max(tail, axis=1, keepdims=True))
                top = high if top is None else jnp.maximum(top, high)
            place = 0
            for s in parts:
                m.p[h, at, place : place + s.shape[1]] = jnp.exp(s - top).astype(BF16)
                place += s.shape[1]
            acc = dot(m.p[h, at, :padded], m.vo[0, h]) + dot(m.p[h, at, padded:], m.vo[1, h])
            inverse = 1.0 / pltpu.roll(acc, 64, 1)
            att = acc * inverse
            right = lane((block, 128)) >= 64
            m.il[h, at] = jnp.where(right, inverse, 0.0)
            m.atto[h, at] = jnp.where(right, att, 0.0).astype(BF16)
            turned = pltpu.roll(att, 64, 1)
            packed = jnp.where(right[: block // 2], att[block // 2 :], turned[: block // 2])
            to = pl.ds(pl.multiple_of(b * (block // 2), block // 2), block // 2)
            m.attz[z, h, to] = packed.astype(BF16)
            return carry

        lax.fori_loop(0, padded // block, one, 0)

    for h in range(nh):
        kv_copies[h].wait_recv()
        prepare(1, h)
        attend(h)
        line.start(0, h)
        if h < g1.steps:
            for g in (g1, g2, go):
                g.advance(h)
        if h:
            line.arrive(0, h - 1)
            line.start(1, h - 1)
        if h > 1:
            line.arrive(1, h - 2)
            line.start(2, h - 2)
    for k in range(min(nh, g1.steps), g1.steps):
        for g in (g1, g2, go):
            g.advance(k)
    for hop in range(nz - 1):
        for h in range(nh):
            done = nh - 1 - h
            if hop >= done:
                line.arrive(hop, h)
                if hop + 1 < nz - 1:
                    line.start(hop + 1, h)

    for copy in kv_copies:
        copy.wait_send()
    for copy in out_copies(False):
        copy.wait_send()
    for g in (gv, gq, g1, g2, go):
        g.drain()
    for h in range(nh):
        line.drain(h)


class Scatter:
    def __init__(self, cube, sems, buffer, landing, rows, colors):
        self.cube, self.buffer, self.landing = cube, buffer, landing
        self.rows, self.colors, self.half = rows, colors, rows // colors
        self.steps = len(cube.orders[0])
        self.plan = [[[] for _ in range(self.steps)] for _ in range(colors)]
        for color in range(colors):
            masks, slot = [0], 0
            for k, step in enumerate(cube.orders[color]):
                for mask in masks:
                    copy = remote(
                        self.view(cube.block(mask ^ step[0]), color),
                        landing.at[color, slot],
                        sems.take(),
                        cube.peer(step),
                    )
                    self.plan[color][k].append((mask, slot, copy))
                    slot += 1
                masks = masks + [mask ^ step[0] for mask in masks]

    def view(self, block, color):
        start = block * self.rows + color * self.half
        return self.buffer.at[pl.ds(pl.multiple_of(start, 8), self.half)]

    def start(self):
        self.left = self.steps - 1
        self.send(self.left)

    def step(self):
        if self.left > 0:
            self.advance(self.left)
            self.left -= 1

    def send(self, k):
        for color in range(self.colors):
            for _, _, copy in self.plan[color][k]:
                copy.start()

    def advance(self, k):
        for color in range(self.colors):
            for mask, slot, copy in self.plan[color][k]:
                copy.wait_recv()
                view = self.view(self.cube.block(mask), color)
                total = view[...].astype(F32) + self.landing[color, slot].astype(F32)
                view[...] = total.astype(BF16)
            for _, _, copy in self.plan[color][k - 1]:
                copy.start()

    def finish(self):
        while self.left > 0:
            self.step()
        parts = []
        for color in range(self.colors):
            ((_, slot, copy),) = self.plan[color][0]
            copy.wait_recv()
            view = self.view(self.cube.block(0), color)
            parts.append(view[...].astype(F32) + self.landing[color, slot].astype(F32))
        return parts[0] if len(parts) == 1 else jnp.concatenate(parts, axis=0)

    def drain(self):
        for color in range(self.colors):
            for step in self.plan[color]:
                for _, _, copy in step:
                    copy.wait_send()


class LineSum:
    def __init__(self, nz, send, recv, base, chunks, rows, part, landed, crossed, total):
        z = lax.axis_index("head")
        self.inner = (z > 0) & (z < nz - 1)
        self.mate, self.cross = {"head": flip(z, 1)}, {"head": nz - 1 - z}
        self.send_sem, self.recv_sem, self.base = send, recv, base
        self.chunks, self.rows = chunks, rows
        self.part, self.landed, self.crossed, self.total = part, landed, crossed, total

    def at(self, ref, i):
        return ref.at[pl.ds(pl.multiple_of(i * self.rows, self.rows), self.rows)]

    def sems(self, kind, i):
        place = self.base + kind * self.chunks + i
        return self.send_sem.at[place], self.recv_sem.at[place]

    def first(self, i):
        return remote(self.at(self.part, i), self.at(self.landed, i), self.sems(0, i), self.mate)

    def second(self, i):
        return remote(self.at(self.part, i), self.at(self.crossed, i), self.sems(1, i), self.cross)

    def third(self, i):
        piece = self.at(self.total, i)
        return remote(piece, piece, self.sems(2, i), self.mate)

    def offer(self, i):
        @pl.when(jnp.logical_not(self.inner))
        def _():
            self.first(i).start()

    def relay(self, i):
        @pl.when(self.inner)
        def _():
            self.first(i).wait_recv()
            view = self.at(self.part, i)
            total = view[...].astype(F32) + self.at(self.landed, i)[...].astype(F32)
            view[...] = total.astype(BF16)
            self.second(i).start()

    def ready(self, i):
        self.close(i)
        self.accept(i)

    def close(self, i):
        @pl.when(self.inner)
        def _():
            self.second(i).wait_recv()
            total = self.at(self.part, i)[...].astype(F32) + self.at(self.crossed, i)[...].astype(F32)
            self.at(self.total, i)[...] = total.astype(BF16)
            self.third(i).start()

    def accept(self, i):
        @pl.when(jnp.logical_not(self.inner))
        def _():
            self.third(i).wait_recv()

    def drain(self, i):
        @pl.when(self.inner)
        def _():
            self.second(i).wait_send()
            self.third(i).wait_send()

        @pl.when(jnp.logical_not(self.inner))
        def _():
            self.first(i).wait_send()


def loop(start, stop, step):
    lax.fori_loop(start, stop, lambda i, carry: (step(i), carry)[1], 0)


def rows_of(i, size):
    return pl.ds(pl.multiple_of(i * size, size), size)


def add_rows(m, row, values):
    count, width = values.shape
    m.acc[row, :, :width] += jnp.sum(values.reshape(count // 8, 8, width), axis=0)


B_FC_TWO, GAIN_TWO, SHIFT_TWO, B_OUT, GAIN_ONE, SHIFT_ONE, B_QKV, B_FC_ONE = range(8)
BLOCK = 256
CHUNK = 64


def stage_two(m, cube, nz, sum_two):
    padded, width = m.xp.shape
    rows = m.wq.shape[0]
    nh = m.q.shape[0]
    frames = m.cot.shape[0]
    hidden = m.w1.shape[1]
    m.gp[0:frames] = m.cot[...]
    m.gp[frames:padded] = fill((padded - frames, width), 0, BF16)
    m.acc[...] = fill(m.acc.shape, 0)
    gain, shift, b_out = m.vec[2:3, :], m.vec[3:4, :], m.vec[4:5, :]
    b_one = m.bias[1:2, :]
    per = BLOCK // CHUNK
    w_one = lambda: m.g1[...].reshape(cube.size * rows, hidden)
    w_two = lambda: m.g2[...].reshape(cube.size * rows, hidden)

    def block(b):
        at = rows_of(b, BLOCK)
        small = rows_of(b, BLOCK // 2)
        mid = m.xp[at].astype(F32) + b_out
        for zz in range(nz):
            pieces = [m.attz[zz, h, small] for h in range(nh)]
            top = jnp.concatenate([p[:, :64] for p in pieces], axis=1)
            low = jnp.concatenate([p[:, 64:] for p in pieces], axis=1)
            att = jnp.concatenate([top, low], axis=0)
            mid = mid + dot_nt(att, m.go[zz].reshape(cube.size * rows, nh * HEAD_DIM))
        xhat, inverse = normalize(mid)
        m.igrad[at] = mid
        m.xh2[at] = xhat
        m.r2[at] = jnp.broadcast_to(inverse, (BLOCK, 128))
        n2 = (xhat * gain + shift).astype(BF16)
        m.n2[at] = n2
        pre = dot(n2, w_one()) + b_one
        cdf = 0.5 + 0.5 * lax.erf(pre * 0.7071067811865476)
        act = (pre * cdf).astype(BF16)
        m.act[at] = act
        slope = cdf + pre * jnp.exp(pre * pre * -0.5) * 0.3989422804014327
        g = m.gp[at]
        add_rows(m, B_FC_TWO, g.astype(F32))
        gpre = (dot(g, w_two()) * slope).astype(BF16)
        m.gpre[at] = gpre
        add_rows(m, B_FC_ONE, gpre.astype(F32))
        back = dot_nt(gpre, w_one())
        add_rows(m, GAIN_TWO, back * m.xh2[at])
        add_rows(m, SHIFT_TWO, back)
        m.part[at] = back.astype(BF16)
        loop(0, per, lambda j: sum_two.offer(b * per + j))

        @pl.when(b > 0)
        def _():
            loop(0, per, lambda j: sum_two.relay((b - 1) * per + j))

        m.opart[at] = dot_nt(m.act[at], w_two()).astype(BF16)

    loop(0, padded // BLOCK, block)


def stage_three(m, cube, nz, sems, sum_two, sum_out, sum_one):
    z = lax.axis_index("head")
    padded, width = m.xp.shape
    rows = m.wq.shape[0]
    nh = m.q.shape[0]
    local = nh * HEAD_DIM
    colors = m.gq.shape[1]
    chunks = padded // CHUNK
    blocks = padded // BLOCK
    per = BLOCK // CHUNK
    scale = HEAD_DIM**-0.5
    packed = m.gq.shape[3]
    s1 = Scatter(cube, sems, m.dw1, m.dl1, rows, colors)
    s2 = Scatter(cube, sems, m.dw2, m.dl2, rows, colors)
    so = Scatter(cube, sems, m.dwo, m.dlo, rows, colors)
    sq = Scatter(cube, sems, m.dwq, m.dlq, rows, colors)
    tile = 128
    tiles = width // tile

    def product(left, right, into, columns):
        def one(i):
            cols = pl.ds(pl.multiple_of(i * tile, tile), tile)
            into[rows_of(i, tile)] = dot_tn(left[:, cols], right())[:, :columns].astype(BF16)

        return one

    one = product(m.n2, lambda: m.gpre[...], m.dw1, m.dw1.shape[1])

    def first(i):
        one(i)

        @pl.when(i < per)
        def _():
            sum_two.relay(chunks - per + i)

    loop(0, tiles, first)
    s1.start()
    loop(0, tiles, product(m.gp, lambda: m.act[...], m.dw2, m.dw2.shape[1]))
    s2.start()

    gain_two = m.vec[2:3, :]

    def middle(i):
        sum_two.ready(i)
        at = rows_of(i, CHUNK)
        n = m.total[at].astype(F32)
        e = n * gain_two
        xhat = m.xh2[at]
        r = m.r2[at][:, :1]
        mean = jnp.mean(e, axis=-1, keepdims=True)
        along = jnp.mean(e * xhat, axis=-1, keepdims=True)
        grad = m.gp[at].astype(F32) + r * (e - mean - xhat * along)
        m.xh2[at] = grad
        add_rows(m, B_OUT, grad)
        low = grad.astype(BF16)
        m.n2[at] = low
        da = dot(low, m.go[z].reshape(cube.size * rows, local)).astype(BF16).astype(F32)
        right = lane((CHUNK, 128)) >= 64
        for h in range(nh):
            base = (h // 2) * 128
            wide = da[:, base : min(base + 128, local)]
            if wide.shape[1] < 128:
                wide = jnp.concatenate([wide, jnp.zeros((CHUNK, 128 - wide.shape[1]), F32)], axis=1)
            if h % 2 == 0:
                wide = pltpu.roll(wide, 64, 1)
            m.act[at, h * 128 : (h + 1) * 128] = jnp.where(right, wide * m.il[h, at], 0.0).astype(BF16)
            m.at[at, h * 64 : (h + 1) * 64] = m.atto[h, at][:, 64:]

    third = chunks // 3
    loop(0, third, middle)
    s1.step()
    s2.step()
    loop(third, 2 * third, middle)
    s1.step()
    s2.step()
    loop(2 * third, chunks, middle)
    loop(0, tiles, product(m.n2, lambda: m.at[...], m.dwo, local))
    so.start()

    for h in range(nh):
        m.qt[h] = m.q[h].T
        m.dat[h] = m.act[:, h * 128 : (h + 1) * 128].T
    big = padded // sum_out.rows
    loop(0, big, sum_out.offer)
    kv_sems = [sems.take() for _ in range(nh)]
    other = {"seq": flip(lax.axis_index("seq"), 1)}
    kv_copies = [remote(m.kvs.at[h], m.kvr.at[h], kv_sems[h], other) for h in range(nh)]
    for h in range(nh):
        m.dkv[0, h] = fill((128, padded), 0)
        m.dkv[1, h] = fill((128, padded), 0)

        def back(b, h=h):
            at = rows_of(b, BLOCK)
            da = m.act[at, h * 128 : (h + 1) * 128]
            inner = jnp.sum(da.astype(F32) * m.atto[h, at].astype(F32), axis=1, keepdims=True)
            for part in (1, 0):
                keys = slice(part * padded, (part + 1) * padded)
                dp = dot(da, m.kvt[part, h])
                p = m.p[h, at, keys]
                ds = (p.astype(F32) * (dp - inner)).astype(BF16)
                m.ds[:, keys] = ds
                m.dkv[part, h] += dot(m.qt[h, :, at], m.ds[:, keys]) + dot(m.dat[h, :, at], p)
            dq = dot(m.ds[:, :padded], m.kv[0, h]) + dot(m.ds[:, padded:], m.kv[1, h])
            dq = (dq * scale)[:, :64].astype(BF16)
            m.gpre[at, nh * 128 + h * 64 : nh * 128 + (h + 1) * 64] = dq
            point = h * blocks + b

            @pl.when((point >= 2) & (point < 2 + big))
            def _():
                sum_out.relay(point - 2)

            @pl.when((point >= 5) & (point < 5 + big))
            def _():
                sum_out.close(point - 5)

        loop(0, blocks, back)
        m.kvs[h] = m.dkv[1, h].astype(BF16)
        kv_copies[h].start()
        if h == 0:
            so.step()
        if h == 1:
            so.step()
    points = nh * blocks
    for i in range(max(0, points - 2), big):
        sum_out.relay(i)
    for i in range(max(0, points - 5), big):
        sum_out.close(i)
    spare = packed - nh * 192
    if spare:
        m.gpre[:, nh * 192 : packed] = fill((padded, spare), 0, BF16)
    for h in range(nh):
        kv_copies[h].wait_recv()
        total = m.dkv[0, h] + m.kvr[h].astype(F32)
        m.gpre[:, h * 128 : (h + 1) * 128] = total.T.astype(BF16)

    def last(b):
        at = rows_of(b, BLOCK)
        grads = m.gpre[at, :packed]
        add_rows(m, B_QKV, grads.astype(F32))
        back = dot_nt(grads, m.gq[...].reshape(cube.size * rows, packed))
        xhat, _ = normalize(m.xp[at].astype(F32))
        add_rows(m, GAIN_ONE, back * xhat)
        add_rows(m, SHIFT_ONE, back)
        m.part[at] = back.astype(BF16)
        loop(0, per, lambda j: sum_one.offer(b * per + j))

        @pl.when(b > 0)
        def _():
            loop(0, per, lambda j: sum_one.relay((b - 1) * per + j))

    loop(0, chunks, sum_two.drain)
    loop(0, blocks, last)
    one_q = product(m.n1, lambda: m.gpre[:, :packed], m.dwq, packed)

    def qkv(i):
        one_q(i)

        @pl.when(i < per)
        def _():
            sum_one.relay(chunks - per + i)

    loop(0, tiles, qkv)
    sq.start()

    for row in range(8):
        m.vs[row : row + 1, :] = jnp.sum(m.acc[row], axis=0, keepdims=True)
    vec_steps = [(cube.peer(step), False) for step in cube.orders[0]]
    vec_steps += [({"head": flip(z, bit)}, True) for bit in powers(nz)]
    row_id = lax.broadcasted_iota(jnp.int32, m.vs.shape, 0)
    partial_rows = (row_id == GAIN_TWO) | (row_id == SHIFT_TWO) | (row_id == GAIN_ONE) | (row_id == SHIFT_ONE)
    vec_copies = []

    def vec_send(k):
        if k < len(vec_steps):
            m.vo_[k] = m.vs[...]
            copy = remote(m.vo_.at[k], m.vr.at[k], sems.take(), vec_steps[k][0])
            copy.start()
            vec_copies.append(copy)

    def vec_take(k):
        if k < len(vec_steps):
            vec_copies[k].wait_recv()
            arrived = m.vr[k]
            if vec_steps[k][1]:
                arrived = jnp.where(partial_rows, arrived, 0.0)
            m.vs[...] += arrived
            vec_send(k + 1)

    vec_send(0)
    b_two = m.vec[5:6, :]

    def output(i):
        sum_out.accept(i)
        at = rows_of(i, sum_out.rows)
        m.ototal[at] = (m.igrad[at] + m.ototal[at].astype(F32) + b_two).astype(BF16)

    gain_one = m.vec[0:1, :]

    def final(i):
        sum_one.ready(i)
        at = rows_of(i, CHUNK)
        e = m.total[at].astype(F32) * gain_one
        xhat, r = normalize(m.xp[at].astype(F32))
        mean = jnp.mean(e, axis=-1, keepdims=True)
        along = jnp.mean(e * xhat, axis=-1, keepdims=True)
        m.igrad[at] = m.xh2[at] + r * (e - mean - xhat * along)

    loop(0, big, sum_out.drain)
    loop(0, big, output)
    m.ow1[...] = s1.finish()
    m.ow2[...] = s2.finish().T
    m.owo[...] = so.finish().T
    vec_take(0)
    sq.step()
    loop(0, third, final)
    vec_take(1)
    sq.step()
    vec_take(2)
    loop(third, 2 * third, final)
    vec_take(3)
    got = sq.finish()
    for h in range(nh):
        cols = slice(h * HEAD_DIM, (h + 1) * HEAD_DIM)
        m.owk[:, cols] = got[:, h * 128 : h * 128 + 64]
        m.owv[:, cols] = got[:, h * 128 + 64 : (h + 1) * 128]
    m.owq[...] = got[:, nh * 128 : nh * 128 + local]
    vec_take(4)
    for k in range(5, len(vec_steps)):
        vec_take(k)
    m.ovec[...] = m.vs[...]
    loop(2 * third, chunks, final)

    for copy in kv_copies + vec_copies:
        copy.wait_send()
    for s in (s1, s2, so, sq):
        s.drain()
    loop(0, chunks, sum_one.drain)


def layer(inputs, cotangent, vectors, biases, w_query, w_key, w_value, w_out, w_fc_one, w_fc_two, mesh_shape):
    nz = mesh_shape["head"]
    cube = Cube(mesh_shape["clip"], mesh_shape["seq"])
    frames, width = inputs.shape
    rows, local = w_query.shape
    hidden = w_fc_one.shape[1]
    nh = local // HEAD_DIM
    padded = -(-frames // BLOCK) * BLOCK
    colors = 2 if rows % 32 == 0 else 1
    half = rows // colors
    packed = -(-(nh * 192) // 128) * 128
    nb = cube.size
    steps = len(cube.all_bits) + len(powers(nz))
    ins = dict(
        x=inputs,
        cot=cotangent,
        vsh=vectors,
        bias=biases,
        wq=w_query,
        wk=w_key,
        wv=w_value,
        wo=w_out,
        w1=w_fc_one,
        w2=w_fc_two,
    )
    outs = dict(
        ototal=((padded, width), BF16),
        igrad=((padded, width), F32),
        ovec=((8, width), F32),
        owq=((rows, local), F32),
        owk=((rows, local), F32),
        owv=((rows, local), F32),
        owo=((local, rows), F32),
        ow1=((rows, hidden), F32),
        ow2=((hidden, rows), F32),
    )
    flat = (padded, width)
    scratch = dict(
        gq=((nb, colors, half, packed), BF16),
        go=((nz, nb, colors, half, local), BF16),
        g1=((nb, colors, half, hidden), BF16),
        g2=((nb, colors, half, hidden), BF16),
        gv=((nb, 8, 128), F32),
        vec=((8, width), F32),
        n1=(flat, BF16),
        q=((nh, padded, 128), BF16),
        kv=((2, nh, padded, 128), BF16),
        kvt=((2, nh, 128, padded), BF16),
        vo=((2, nh, padded, 128), BF16),
        p=((nh, padded, 2 * padded), BF16),
        il=((nh, padded, 128), F32),
        atto=((nh, padded, 128), BF16),
        attz=((nz, nh, padded // 2, 128), BF16),
        xp=(flat, BF16),
        gp=(flat, BF16),
        xh2=(flat, F32),
        r2=((padded, 128), F32),
        n2=(flat, BF16),
        act=((padded, hidden), BF16),
        gpre=((padded, hidden), BF16),
        acc=((8, 8, width), F32),
        vs=((8, width), F32),
        vo_=((steps, 8, width), F32),
        vr=((steps, 8, width), F32),
        part=(flat, BF16),
        landed=(flat, BF16),
        crossed=(flat, BF16),
        crossed_one=(flat, BF16),
        total=(flat, BF16),
        opart=(flat, BF16),
        olanded=(flat, BF16),
        ocrossed=(flat, BF16),
        at=((padded, local), BF16),
        qt=((nh, 128, padded), BF16),
        dat=((nh, 128, padded), BF16),
        dkv=((2, nh, 128, padded), F32),
        kvs=((nh, 128, padded), BF16),
        kvr=((nh, 128, padded), BF16),
        ds=((BLOCK, 2 * padded), BF16),
        dw1=((width, hidden), BF16),
        dl1=((colors, nb - 1, half, hidden), BF16),
        dw2=((width, hidden), BF16),
        dl2=((colors, nb - 1, half, hidden), BF16),
        dwo=((width, local), BF16),
        dlo=((colors, nb - 1, half, local), BF16),
        dwq=((width, packed), BF16),
        dlq=((colors, nb - 1, half, packed), BF16),
    )
    small, large = padded // CHUNK, padded // 128
    lines = 3 * (2 * small + large)
    count = lines + 9 * colors * (nb - 1) + 60

    def body(*refs):
        names = list(ins) + list(outs) + list(scratch)
        m = types.SimpleNamespace(**dict(zip(names, refs)))
        send, recv = refs[len(names) :]
        sems = Sems(send, recv)
        sems.used = lines
        sum_two = LineSum(nz, send, recv, 0, small, CHUNK, m.part, m.landed, m.crossed, m.total)
        sum_one = LineSum(nz, send, recv, 3 * small, small, CHUNK, m.part, m.landed, m.crossed_one, m.total)
        sum_out = LineSum(nz, send, recv, 6 * small, large, 128, m.opart, m.olanded, m.ocrossed, m.ototal)
        stage_one(m, cube, nz, sems)
        stage_two(m, cube, nz, sum_two)
        stage_three(m, cube, nz, sems, sum_two, sum_out, sum_one)
        assert sems.used <= count, (sems.used, count)

    res = pl.pallas_call(
        body,
        out_shape=[jax.ShapeDtypeStruct(*v) for v in outs.values()],
        in_specs=[pl.BlockSpec(memory_space=pltpu.VMEM)] * len(ins),
        out_specs=[pl.BlockSpec(memory_space=pltpu.VMEM)] * len(outs),
        scratch_shapes=[pltpu.VMEM(*v) for v in scratch.values()] + [pltpu.SemaphoreType.DMA((count,))] * 2,
        compiler_params=pltpu.CompilerParams(
            collective_id=0, has_side_effects=True, vmem_limit_bytes=67_043_328
        ),
        name="layer",
    )(*ins.values())
    return types.SimpleNamespace(**dict(zip(outs, res)))


def vector_pack(vectors):
    stack = jnp.stack([v.astype(F32) for v in vectors])
    return jnp.pad(stack, ((0, 8 - stack.shape[0]), (0, 128 - stack.shape[1])))


def biases_pack(b_query, b_value, b_fc_one, heads):
    zero = jnp.zeros((HEAD_DIM,), F32)
    parts = []
    for h in range(heads):
        parts += [zero, b_value[h * HEAD_DIM : (h + 1) * HEAD_DIM].astype(F32)]
    row = jnp.concatenate(parts + [b_query.astype(F32)])
    width = b_fc_one.shape[0]
    row = jnp.pad(row, (0, width - row.shape[0]))
    return jnp.pad(jnp.stack([row, b_fc_one.astype(F32)]), ((0, 6), (0, 0)))


def on_device(
    inputs,
    gain_one,
    shift_one,
    w_query,
    b_query,
    w_key,
    w_value,
    b_value,
    w_out,
    b_out,
    gain_two,
    shift_two,
    w_fc_one,
    b_fc_one,
    w_fc_two,
    b_fc_two,
    cotangent,
    mesh_shape,
):
    clips, frames, width = inputs.shape
    count = clips * frames
    local = w_query.shape[1]
    heads = local // HEAD_DIM
    share = gain_one.shape[0]
    vectors = vector_pack((gain_one, shift_one, gain_two, shift_two, b_out, b_fc_two))
    biases = biases_pack(b_query, b_value, b_fc_one, heads)
    res = layer(
        inputs.reshape(count, width),
        cotangent.reshape(count, width),
        vectors,
        biases,
        w_query,
        w_key,
        w_value,
        w_out,
        w_fc_one,
        w_fc_two,
        mesh_shape,
    )
    rank = lax.axis_index("clip") * mesh_shape["seq"] + lax.axis_index("seq")
    owned = lax.dynamic_slice_in_dim(res.ovec, rank * share, share, axis=1)
    qkv = res.ovec[B_QKV]
    b_values = jnp.concatenate([qkv[h * 128 + 64 : (h + 1) * 128] for h in range(heads)])
    return (
        res.ototal[:count].reshape(clips, frames, width),
        res.igrad[:count].reshape(clips, frames, width),
        owned[GAIN_ONE],
        owned[SHIFT_ONE],
        res.owq,
        qkv[heads * 128 : heads * 128 + local],
        res.owk,
        res.owv,
        b_values,
        res.owo,
        owned[B_OUT],
        owned[GAIN_TWO],
        owned[SHIFT_TWO],
        res.ow1,
        res.ovec[B_FC_ONE],
        res.ow2,
        owned[B_FC_TWO],
    )


def solution(mesh):
    group = ("clip", "seq")
    rows, columns, own, heads = P(group, "head"), P("head", group), P(group), P("head")
    tokens = P("clip", "seq", None)
    return jax.shard_map(
        partial(on_device, mesh_shape=dict(mesh.shape)),
        mesh=mesh,
        in_specs=(
            tokens, own, own, rows, heads, rows, rows, heads, columns,
            own, own, own, rows, heads, columns, own, tokens,
        ),
        out_specs=(
            tokens, tokens, own, own, rows, heads, rows, rows, heads,
            columns, own, own, own, rows, heads, columns, own,
        ),
        check_vma=False,
    )
```

```python
from functools import partial
import types

import jax
import jax.numpy as jnp
from jax import lax
from jax.experimental import pallas as pl
from jax.experimental.pallas import tpu as pltpu
from jax.sharding import PartitionSpec as P

HEAD_DIM = 64
EPS = 1e-05
F32 = jnp.float32
BF16 = jnp.bfloat16
MESH = pl.DeviceIdType.MESH


def flip(value, bit):
    return value + bit * (1 - 2 * lax.rem(lax.div(value, bit), 2))


def flips(value, mask, bits):
    for bit in bits:
        if mask & bit:
            value = flip(value, bit)
    return value


def powers(size):
    bits, bit = [], 1
    while bit < size:
        bits.append(bit)
        bit *= 2
    return bits


class Cube:
    def __init__(self, clips, seqs):
        self.clips, self.seqs, self.size = clips, seqs, clips * seqs
        self.seq_bits = [(bit, "seq", bit) for bit in powers(seqs)]
        self.clip_bits = [(bit * seqs, "clip", bit) for bit in powers(clips)]
        core, rest = self.clip_bits[:1], self.clip_bits[1:]
        self.orders = (
            self.seq_bits + rest + core,
            rest[:1] + self.seq_bits + rest[1:] + core,
        )
        self.all_bits = [bit for bit, _, _ in self.seq_bits + self.clip_bits]

    def rank(self):
        return lax.axis_index("clip") * self.seqs + lax.axis_index("seq")

    def block(self, mask):
        return flips(self.rank(), mask, self.all_bits)

    @staticmethod
    def peer(step):
        _, axis, bit = step
        return {axis: flip(lax.axis_index(axis), bit)}


class Sems:
    def __init__(self, send, recv):
        self.send, self.recv, self.used = send, recv, 0

    def take(self):
        self.used += 1
        return self.send.at[self.used - 1], self.recv.at[self.used - 1]


def remote(src, dst, sems, device):
    return pltpu.make_async_remote_copy(
        src_ref=src,
        dst_ref=dst,
        send_sem=sems[0],
        recv_sem=sems[1],
        device_id=device,
        device_id_type=MESH,
    )


class Gather:
    def __init__(self, cube, sems, view, colors):
        self.cube, self.view, self.colors = cube, view, colors
        self.steps = len(cube.orders[0])
        self.copies = [[[] for _ in range(self.steps)] for _ in range(colors)]
        for color in range(colors):
            masks = [0]
            for k, step in enumerate(cube.orders[color]):
                for mask in masks:
                    block = cube.block(mask)
                    piece = view(block, color)
                    self.copies[color][k].append(
                        remote(piece, piece, sems.take(), cube.peer(step))
                    )
                masks = masks + [mask ^ step[0] for mask in masks]

    def start(self, k, color):
        for copy in self.copies[color][k]:
            copy.start()

    def advance(self, k, color):
        for copy in self.copies[color][k]:
            copy.wait_recv()
        if k + 1 < self.steps:
            self.start(k + 1, color)

    def drain(self):
        for color in range(self.colors):
            for step in self.copies[color]:
                for copy in step:
                    copy.wait_send()


def normalize(rows):
    mean = jnp.mean(rows, axis=-1, keepdims=True)
    centered = rows - mean
    spread = jnp.mean(centered * centered, axis=-1, keepdims=True)
    inverse = lax.rsqrt(spread + EPS)
    return centered * inverse, inverse


def dot(a, b):
    return jnp.dot(a, b, preferred_element_type=F32)


def dot_nt(a, b):
    return lax.dot_general(a, b, (((1,), (1,)), ((), ())), preferred_element_type=F32)


def dot_tn(a, b):
    return lax.dot_general(a, b, (((0,), (0,)), ((), ())), preferred_element_type=F32)


NEG = -1e30


def fill(shape, value, dtype=F32):
    return jnp.full(shape, value, dtype)


def lane(shape):
    return lax.broadcasted_iota(jnp.int32, shape, len(shape) - 1)


class Line:
    def __init__(self, nodes, sems, view, parts):
        self.n, self.z = nodes, lax.axis_index("head")
        self.view = view
        self.right = [[sems.take() for _ in range(parts)] for _ in range(nodes - 1)]
        self.left = [[sems.take() for _ in range(parts)] for _ in range(nodes - 1)]

    def moves(self, hop, part):
        z, n = self.z, self.n

        def copy(origin, sems, target):
            piece = self.view(origin, part)
            return remote(piece, piece, sems, {"head": target})

        sends = (
            (
                (z >= hop) & (z < n - 1),
                lambda: copy(z - hop, self.right[hop][part], z + 1),
            ),
            (
                (n - 1 - z >= hop) & (z > 0),
                lambda: copy(z + hop, self.left[hop][part], z - 1),
            ),
        )
        arrivals = (
            (z > hop, lambda: copy(z - 1 - hop, self.right[hop][part], z - 1)),
            (n - 1 - z > hop, lambda: copy(z + 1 + hop, self.left[hop][part], z + 1)),
        )
        return sends, arrivals

    def start(self, hop, part):
        for condition, copy in self.moves(hop, part)[0]:
            pl.when(condition)(lambda copy=copy: copy().start())

    def arrive(self, hop, part):
        for condition, copy in self.moves(hop, part)[1]:
            pl.when(condition)(lambda copy=copy: copy().wait_recv())

    def drain(self, part):
        for hop in range(self.n - 1):
            for condition, copy in self.moves(hop, part)[0]:
                pl.when(condition)(lambda copy=copy: copy().wait_send())


def entry_barrier(cube, heads):
    barrier = pltpu.get_barrier_semaphore()
    z = lax.axis_index("head")
    peers = [cube.peer(step) for step in cube.orders[0]]
    peers += [{"head": lax.rem(z + d, heads)} for d in range(1, heads)]
    for peer in peers:
        pl.semaphore_signal(barrier, inc=1, device_id=peer, device_id_type=MESH)
    pl.semaphore_wait(barrier, len(peers))


def stage_one(m, cube, nz, sems):
    z = lax.axis_index("head")
    r = cube.rank()
    rows = m.wq.shape[0]
    colors = m.gq.shape[1]
    half = rows // colors
    nh = m.q.shape[0]
    frames = m.x.shape[0]
    padded = m.xp.shape[0]
    tile = 128
    tiles = padded // tile
    width = m.x.shape[1]

    gq = Gather(cube, sems, lambda b, c: m.gq.at[b, c], colors)
    gv = Gather(cube, sems, lambda b, c: m.gv.at[b], 1)
    g1 = Gather(cube, sems, lambda b, c: m.g1.at[b, c], colors)
    g2 = Gather(cube, sems, lambda b, c: m.g2.at[b, c], colors)
    go = Gather(cube, sems, lambda b, c: m.go.at[:, b, c], colors)

    m.vec[...] = fill(m.vec.shape, 0)
    for row, ref in enumerate(m.shares):
        m.vec[row : row + 1, :rows] = ref[...].astype(F32)
    m.gv[r] = m.vec[:, :128]
    for c in range(colors):
        part = pl.ds(c * half, half)
        for h in range(nh):
            cols = slice(h * HEAD_DIM, (h + 1) * HEAD_DIM)
            m.gq[r, c, :, h * 128 : h * 128 + 64] = m.wk[part, cols]
            m.gq[r, c, :, h * 128 + 64 : (h + 1) * 128] = m.wv[part, cols]
        m.gq[r, c, :, nh * 128 : nh * 128 + nh * 64] = m.wq[part, :]
        spare = m.gq.shape[3] - nh * 192
        if spare:
            m.gq[r, c, :, nh * 192 :] = fill((half, spare), 0, BF16)
        m.g2[r, c] = m.w2[part, :]
        m.g1[r, c] = m.w1[part, :]

    entry_barrier(cube, nz)
    gv.start(0, 0)
    for c in range(colors):
        gq.start(0, c)

    wot = m.wo[...].T
    for c in range(colors):
        m.go[z, r, c] = wot[c * half : (c + 1) * half]
    out_sems = [sems.take() for _ in range(nz - 1)]

    def out_copies(arriving):
        for d in range(1, nz):
            origin = lax.rem(z + nz - d, nz) if arriving else z
            target = lax.rem(z + d, nz)
            piece = m.go.at[origin, r]
            yield remote(piece, piece, out_sems[d - 1], {"head": target})

    for copy in out_copies(False):
        copy.start()
    for c in range(1, colors):
        g1.start(0, c)
        g2.start(0, c)

    m.xp[0:frames] = m.x[...]
    m.xp[frames:padded] = fill((padded - frames, width), 0, BF16)

    def norm_tile(i, carry):
        at = pl.ds(pl.multiple_of(i * tile, tile), tile)
        xhat, _ = normalize(m.xp[at].astype(F32))
        m.xh2[at] = xhat
        return carry

    third = tiles // gq.steps
    for k in range(gq.steps):
        top = tiles if k == gq.steps - 1 else third * (k + 1)
        lax.fori_loop(third * k, top, norm_tile, 0)
        gv.advance(k, 0)
        for c in range(colors):
            gq.advance(k, c)
    for b in range(cube.size):
        m.vec[:, b * rows : (b + 1) * rows] = m.gv[b, :, :rows]
    gain, shift = m.vec[0:1, :], m.vec[1:2, :]
    m.bias[...] = fill(m.bias.shape, 0)
    bv = m.bv[...].astype(F32)[None, :]
    for h in range(nh):
        m.bias[0:1, h * 128 + 64 : (h + 1) * 128] = bv[:, h * HEAD_DIM : (h + 1) * HEAD_DIM]
    m.bias[0:1, nh * 128 : nh * 192] = m.bq[...].astype(F32)[None, :]
    bias = m.bias[0:1, :]
    scale = HEAD_DIM**-0.5

    def project(i, carry):
        at = pl.ds(pl.multiple_of(i * tile, tile), tile)
        n1 = (m.xh2[at] * gain + shift).astype(BF16)
        m.n1[at] = n1
        packed = dot(n1, m.gq[...].reshape(cube.size * rows, m.gq.shape[3])) + bias
        left = lane((tile, 128)) < 64
        for h in range(nh):
            m.kv[0, h, at] = packed[:, h * 128 : (h + 1) * 128].astype(BF16)
            base = nh * 128 + (h // 2) * 128
            pair = packed[:, base : base + 128]
            if h % 2:
                pair = pltpu.roll(pair, 64, 1)
            pair = pair.astype(BF16).astype(F32) * scale
            m.q[h, at] = jnp.where(left, pair, 0.0).astype(BF16)
        return carry

    lax.fori_loop(0, tiles, project, 0)

    kv_sems = [sems.take() for _ in range(nh)]
    other = {"seq": flip(lax.axis_index("seq"), 1)}
    kv_copies = [
        remote(m.kv.at[0, h], m.kv.at[1, h], kv_sems[h], other) for h in range(nh)
    ]
    for copy in out_copies(True):
        copy.wait_recv()
    for c in range(1, colors):
        go.start(0, c)
    kv_copies[0].start()
    for g in (g1, g2, go):
        g.start(0, 0)
    for copy in kv_copies[1:]:
        copy.start()

    left = lane((padded, 128)) < 64

    def prepare(part, h):
        block = m.kv[part, h]
        m.kvt[part, h] = block.T
        m.vo[part, h] = jnp.where(left, jnp.ones_like(block), block)

    for h in range(nh):
        prepare(0, h)

    line = Line(nz, sems, lambda origin, part: m.attz.at[origin, part], nh)
    block = 256
    valid = frames - (padded - 128)

    def attend(h):
        def one(b, carry):
            at = pl.ds(pl.multiple_of(b * block, block), block)
            query = m.q[h, at]
            keep = lane((block, 128)) < valid
            parts = []
            top = None
            for part in range(2):
                s = dot(query, m.kvt[part, h])
                body, tail = s[:, : padded - 128], s[:, padded - 128 :]
                tail = jnp.where(keep, tail, NEG)
                parts += [body, tail]
                high = jnp.maximum(jnp.max(body, axis=1, keepdims=True), jnp.max(tail, axis=1, keepdims=True))
                top = high if top is None else jnp.maximum(top, high)
            place = 0
            for s in parts:
                m.p[h, at, place : place + s.shape[1]] = jnp.exp(s - top).astype(BF16)
                place += s.shape[1]
            acc = dot(m.p[h, at, :padded], m.vo[0, h]) + dot(m.p[h, at, padded:], m.vo[1, h])
            inverse = 1.0 / pltpu.roll(acc, 64, 1)
            att = acc * inverse
            right = lane((block, 128)) >= 64
            m.il[h, at] = jnp.where(right, inverse, 0.0)
            m.atto[h, at] = jnp.where(right, att, 0.0).astype(BF16)
            turned = pltpu.roll(att, 64, 1)
            packed = jnp.where(right[: block // 2], att[block // 2 :], turned[: block // 2])
            to = pl.ds(pl.multiple_of(b * (block // 2), block // 2), block // 2)
            m.attz[z, h, to] = packed.astype(BF16)
            return carry

        lax.fori_loop(0, padded // block, one, 0)

    def weights(k, c):
        if c < colors and k < g1.steps:
            for g in (g1, g2, go):
                g.advance(k, c)

    for h in range(nh):
        kv_copies[h].wait_recv()
        prepare(1, h)
        attend(h)
        line.start(0, h)
        if h == 0:
            weights(0, 1)
        if h >= 1:
            line.arrive(0, h - 1)
            line.start(1, h - 1)
        if h == 1:
            weights(0, 0)
        if h >= 2:
            line.arrive(1, h - 2)
            line.start(2, h - 2)
    for hop in range(nz - 1):
        for h in range(nh):
            done = nh - 1 - h
            if hop >= done:
                if hop == nz - 2 and h == 1:
                    weights(1, 0)
                    weights(1, 1)
                line.arrive(hop, h)
                if hop + 1 < nz - 1:
                    line.start(hop + 1, h)
    for k in range(2, g1.steps):
        for c in range(colors):
            weights(k, c)

    for copy in kv_copies:
        copy.wait_send()
    for copy in out_copies(False):
        copy.wait_send()
    for g in (gv, gq, g1, g2, go):
        g.drain()
    for h in range(nh):
        line.drain(h)


class Scatter:
    def __init__(self, cube, sems, buffer, landing, rows, colors):
        self.cube, self.buffer, self.landing = cube, buffer, landing
        self.rows, self.colors, self.half = rows, colors, rows // colors
        self.steps = len(cube.orders[0])
        self.plan = [[[] for _ in range(self.steps)] for _ in range(colors)]
        for color in range(colors):
            masks, slot = [0], 0
            for k, step in enumerate(cube.orders[color]):
                for mask in masks:
                    copy = remote(
                        self.view(cube.block(mask ^ step[0]), color),
                        landing.at[color, slot],
                        sems.take(),
                        cube.peer(step),
                    )
                    self.plan[color][k].append((mask, slot, copy))
                    slot += 1
                masks = masks + [mask ^ step[0] for mask in masks]

    def view(self, block, color):
        start = block * self.rows + color * self.half
        return self.buffer.at[pl.ds(pl.multiple_of(start, 8), self.half)]

    def start(self):
        self.left = self.steps - 1
        self.send(self.left)

    def step(self):
        if self.left > 0:
            self.advance(self.left)
            self.left -= 1

    def send(self, k):
        for color in range(self.colors):
            for _, _, copy in self.plan[color][k]:
                copy.start()

    def advance(self, k):
        for color in range(self.colors):
            for mask, slot, copy in self.plan[color][k]:
                copy.wait_recv()
                view = self.view(self.cube.block(mask), color)
                total = view[...].astype(F32) + self.landing[color, slot].astype(F32)
                view[...] = total.astype(BF16)
            for _, _, copy in self.plan[color][k - 1]:
                copy.start()

    def finish(self):
        while self.left > 0:
            self.step()
        parts = []
        for color in range(self.colors):
            ((_, slot, copy),) = self.plan[color][0]
            copy.wait_recv()
            view = self.view(self.cube.block(0), color)
            parts.append(view[...].astype(F32) + self.landing[color, slot].astype(F32))
        return parts[0] if len(parts) == 1 else jnp.concatenate(parts, axis=0)

    def drain(self):
        for color in range(self.colors):
            for step in self.plan[color]:
                for _, _, copy in step:
                    copy.wait_send()


class LineSum:
    def __init__(self, nz, send, recv, base, chunks, rows, part, landed, crossed, total):
        z = lax.axis_index("head")
        self.inner = (z > 0) & (z < nz - 1)
        self.mate, self.cross = {"head": flip(z, 1)}, {"head": nz - 1 - z}
        self.send_sem, self.recv_sem, self.base = send, recv, base
        self.chunks, self.rows = chunks, rows
        self.part, self.landed, self.crossed, self.total = part, landed, crossed, total

    def at(self, ref, i):
        return ref.at[pl.ds(pl.multiple_of(i * self.rows, self.rows), self.rows)]

    def sems(self, kind, i):
        place = self.base + kind * self.chunks + i
        return self.send_sem.at[place], self.recv_sem.at[place]

    def first(self, i):
        return remote(self.at(self.part, i), self.at(self.landed, i), self.sems(0, i), self.mate)

    def second(self, i):
        return remote(self.at(self.part, i), self.at(self.crossed, i), self.sems(1, i), self.cross)

    def third(self, i):
        piece = self.at(self.total, i)
        return remote(piece, piece, self.sems(2, i), self.mate)

    def offer(self, i):
        @pl.when(jnp.logical_not(self.inner))
        def _():
            self.first(i).start()

    def relay(self, i):
        @pl.when(self.inner)
        def _():
            self.first(i).wait_recv()
            view = self.at(self.part, i)
            total = view[...].astype(F32) + self.at(self.landed, i)[...].astype(F32)
            view[...] = total.astype(BF16)
            self.second(i).start()

    def pump(self, i):
        @pl.when(i < self.chunks)
        def _():
            self.relay(i)

        @pl.when(i >= LAG)
        def _():
            self.close(i - LAG)

    def close(self, i):
        @pl.when(self.inner)
        def _():
            self.second(i).wait_recv()
            total = self.at(self.part, i)[...].astype(F32) + self.at(self.crossed, i)[...].astype(F32)
            self.at(self.total, i)[...] = total.astype(BF16)
            self.third(i).start()

    def accept(self, i):
        @pl.when(jnp.logical_not(self.inner))
        def _():
            self.third(i).wait_recv()

    def drain(self, i):
        @pl.when(self.inner)
        def _():
            self.second(i).wait_send()
            self.third(i).wait_send()

        @pl.when(jnp.logical_not(self.inner))
        def _():
            self.first(i).wait_send()


def loop(start, stop, step):
    lax.fori_loop(start, stop, lambda i, carry: (step(i), carry)[1], 0)


def rows_of(i, size):
    return pl.ds(pl.multiple_of(i * size, size), size)


def add_rows(m, row, values):
    count, width = values.shape
    m.acc[row, :, :width] += jnp.sum(values.reshape(count // 8, 8, width), axis=0)


B_FC_TWO, GAIN_TWO, SHIFT_TWO, B_OUT, GAIN_ONE, SHIFT_ONE, B_QKV, B_FC_ONE = range(8)
BLOCK = 256
CHUNK = 32
LAG = 4


def stage_two(m, cube, nz, sum_two, sum_out):
    padded, width = m.xp.shape
    rows = m.wq.shape[0]
    nh = m.q.shape[0]
    frames = m.cot.shape[0]
    hidden = m.w1.shape[1]
    m.gp[0:frames] = m.cot[...]
    m.gp[frames:padded] = fill((padded - frames, width), 0, BF16)
    m.acc[...] = fill(m.acc.shape, 0)
    gain, shift, b_out = m.vec[2:3, :], m.vec[3:4, :], m.vec[4:5, :]
    b_one = m.bf1[...].astype(F32)[None, :]
    per = BLOCK // CHUNK
    w_one = lambda: m.g1[...].reshape(cube.size * rows, hidden)
    w_two = lambda: m.g2[...].reshape(cube.size * rows, hidden)

    def block(b):
        at = rows_of(b, BLOCK)
        small = rows_of(b, BLOCK // 2)
        mid = m.xp[at].astype(F32) + b_out
        for zz in range(nz):
            pieces = [m.attz[zz, h, small] for h in range(nh)]
            top = jnp.concatenate([p[:, :64] for p in pieces], axis=1)
            low = jnp.concatenate([p[:, 64:] for p in pieces], axis=1)
            att = jnp.concatenate([top, low], axis=0)
            mid = mid + dot_nt(att, m.go[zz].reshape(cube.size * rows, nh * HEAD_DIM))
        xhat, inverse = normalize(mid)
        m.mid[at] = mid
        m.xh2[at] = xhat
        m.r2[at] = jnp.broadcast_to(inverse, (BLOCK, 128))
        n2 = (xhat * gain + shift).astype(BF16)
        m.n2[at] = n2
        pre = dot(n2, w_one()) + b_one
        cdf = 0.5 + 0.5 * lax.erf(pre * 0.7071067811865476)
        act = (pre * cdf).astype(BF16)
        m.act[at] = act
        slope = cdf + pre * jnp.exp(pre * pre * -0.5) * 0.3989422804014327
        g = m.gp[at]
        add_rows(m, B_FC_TWO, g.astype(F32))
        gpre = (dot(g, w_two()) * slope).astype(BF16)
        m.gpre[at] = gpre
        add_rows(m, B_FC_ONE, gpre.astype(F32))
        back = dot_nt(gpre, w_one())
        add_rows(m, GAIN_TWO, back * m.xh2[at])
        add_rows(m, SHIFT_TWO, back)
        m.part[at] = back.astype(BF16)
        loop(0, per, lambda j: sum_two.offer(b * per + j))
        m.opart[at] = dot_nt(m.act[at], w_two()).astype(BF16)

    loop(0, padded // BLOCK, block)
    loop(0, sum_out.chunks, sum_out.offer)


def stage_three(m, cube, nz, sems, sum_two, sum_out, sum_one):
    z = lax.axis_index("head")
    padded, width = m.xp.shape
    rows = m.wq.shape[0]
    nh = m.q.shape[0]
    local = nh * HEAD_DIM
    colors = m.gq.shape[1]
    chunks = padded // CHUNK
    blocks = padded // BLOCK
    per = BLOCK // CHUNK
    scale = HEAD_DIM**-0.5
    packed = m.gq.shape[3]
    s1 = Scatter(cube, sems, m.dw1, m.dl1, rows, colors)
    s2 = Scatter(cube, sems, m.dw2, m.dl2, rows, colors)
    so = Scatter(cube, sems, m.dwo, m.dlo, rows, colors)
    sq = Scatter(cube, sems, m.dwq, m.dlq, rows, colors)
    tile = 128
    tiles = width // tile

    def product(left, right, into, columns):
        def one(i):
            cols = pl.ds(pl.multiple_of(i * tile, tile), tile)
            into[rows_of(i, tile)] = dot_tn(left[:, cols], right())[:, :columns].astype(BF16)

        return one

    one = product(m.n2, lambda: m.gpre[...], m.dw1, m.dw1.shape[1])
    two = product(m.gp, lambda: m.act[...], m.dw2, m.dw2.shape[1])

    def first(i):
        one(i)
        sum_two.pump(i)

    def second(i):
        two(i)
        sum_two.pump(tiles + i)

    loop(0, tiles, first)
    s1.start()
    loop(0, tiles, second)
    s2.start()
    gain_two = m.vec[2:3, :]

    def middle(i):
        sum_two.accept(i)
        at = rows_of(i, CHUNK)
        n = m.total[at].astype(F32)
        e = n * gain_two
        xhat = m.xh2[at]
        r = m.r2[at][:, :1]
        mean = jnp.mean(e, axis=-1, keepdims=True)
        along = jnp.mean(e * xhat, axis=-1, keepdims=True)
        grad = m.gp[at].astype(F32) + r * (e - mean - xhat * along)
        m.xh2[at] = grad
        add_rows(m, B_OUT, grad)
        low = grad.astype(BF16)
        m.n2[at] = low
        da = dot(low, m.go[z].reshape(cube.size * rows, local)).astype(BF16).astype(F32)
        right = lane((CHUNK, 128)) >= 64
        for h in range(nh):
            base = (h // 2) * 128
            wide = da[:, base : min(base + 128, local)]
            if wide.shape[1] < 128:
                wide = jnp.concatenate([wide, jnp.zeros((CHUNK, 128 - wide.shape[1]), F32)], axis=1)
            if h % 2 == 0:
                wide = pltpu.roll(wide, 64, 1)
            m.act[at, h * 128 : (h + 1) * 128] = jnp.where(right, wide * m.il[h, at], 0.0).astype(BF16)
            m.at[at, h * 64 : (h + 1) * 64] = m.atto[h, at][:, 64:]

    ahead = 2 * tiles

    def pumped(i):
        sum_two.pump(i + ahead)
        middle(i)

    stop = chunks + LAG - ahead
    s1.step()
    fourth = stop // 4
    for part in range(4):
        loop(part * fourth, stop if part == 3 else (part + 1) * fourth, pumped)
        (s2, s1)[part % 2].step()
    loop(stop, chunks, middle)

    loop(0, tiles, product(m.n2, lambda: m.at[...], m.dwo, local))
    so.start()

    for h in range(nh):
        m.qt[h] = m.q[h].T
        m.dat[h] = m.act[:, h * 128 : (h + 1) * 128].T
    big = sum_out.chunks
    sum_out.relay(0)
    kv_sems = [sems.take() for _ in range(nh)]
    other = {"seq": flip(lax.axis_index("seq"), 1)}
    kv_copies = [remote(m.kvs.at[h], m.kvr.at[h], kv_sems[h], other) for h in range(nh)]
    for h in range(nh):
        m.dkv[0, h] = fill((128, padded), 0)
        m.dkv[1, h] = fill((128, padded), 0)

        def back(b, h=h):
            at = rows_of(b, BLOCK)
            da = m.act[at, h * 128 : (h + 1) * 128]
            inner = jnp.sum(da.astype(F32) * m.atto[h, at].astype(F32), axis=1, keepdims=True)
            for part in (1, 0):
                keys = slice(part * padded, (part + 1) * padded)
                dp = dot(da, m.kvt[part, h])
                p = m.p[h, at, keys]
                ds = (p.astype(F32) * (dp - inner)).astype(BF16)
                m.ds[:, keys] = ds
                m.dkv[part, h] += dot(m.qt[h, :, at], m.ds[:, keys]) + dot(m.dat[h, :, at], p)
            dq = dot(m.ds[:, :padded], m.kv[0, h]) + dot(m.ds[:, padded:], m.kv[1, h])
            dq = (dq * scale)[:, :64].astype(BF16)
            m.gpre[at, nh * 128 + h * 64 : nh * 128 + (h + 1) * 64] = dq
            point = h * blocks + b

            for i, (when, done) in enumerate(((2, None), (5, 0), (8, 1))):

                @pl.when(point == when)
                def _(i=i, done=done):
                    sum_out.relay(i + 1)
                    if done is not None:
                        sum_out.close(done)

        loop(0, blocks, back)
        m.kvs[h] = m.dkv[1, h].astype(BF16)
        kv_copies[h].start()
        if h < nh - 1:
            so.step()
    spare = packed - nh * 192
    if spare:
        m.gpre[:, nh * 192 : packed] = fill((padded, spare), 0, BF16)
    for h in range(nh):
        if h == nh - 1:
            sum_out.relay(4)
            sum_out.close(2)
        kv_copies[h].wait_recv()
        total = m.dkv[0, h] + m.kvr[h].astype(F32)
        m.gpre[:, h * 128 : (h + 1) * 128] = total.T.astype(BF16)

    def last(b):
        at = rows_of(b, BLOCK)
        grads = m.gpre[at, :packed]
        add_rows(m, B_QKV, grads.astype(F32))
        back = dot_nt(grads, m.gq[...].reshape(cube.size * rows, packed))
        xhat, _ = normalize(m.xp[at].astype(F32))
        add_rows(m, GAIN_ONE, back * xhat)
        add_rows(m, SHIFT_ONE, back)
        m.part[at] = back.astype(BF16)
        loop(0, per, lambda j: sum_one.offer(b * per + j))

    loop(0, chunks, sum_two.drain)
    loop(0, blocks, last)
    one_q = product(m.n1, lambda: m.gpre[:, :packed], m.dwq, packed)

    def qkv(i):
        one_q(i)
        sum_one.pump(i)

    sum_out.relay(5)
    sum_out.close(3)
    loop(0, tiles, qkv)
    sq.start()
    sum_out.close(4)
    sum_out.close(5)

    for row in range(8):
        m.vs[row : row + 1, :] = jnp.sum(m.acc[row], axis=0, keepdims=True)
    vec_steps = [(cube.peer(step), False) for step in cube.orders[0]]
    vec_steps += [({"head": flip(z, bit)}, True) for bit in powers(nz)]
    row_id = lax.broadcasted_iota(jnp.int32, m.vs.shape, 0)
    partial_rows = (row_id == GAIN_TWO) | (row_id == SHIFT_TWO) | (row_id == GAIN_ONE) | (row_id == SHIFT_ONE)
    vec_copies = []

    def vec_send(k):
        if k < len(vec_steps):
            m.vo_[k] = m.vs[...]
            copy = remote(m.vo_.at[k], m.vr.at[k], sems.take(), vec_steps[k][0])
            copy.start()
            vec_copies.append(copy)

    def vec_take(k):
        if k < len(vec_steps):
            vec_copies[k].wait_recv()
            arrived = m.vr[k]
            if vec_steps[k][1]:
                arrived = jnp.where(partial_rows, arrived, 0.0)
            m.vs[...] += arrived
            vec_send(k + 1)

    vec_send(0)
    b_two = m.vec[5:6, :]

    def output(i):
        sum_out.accept(i)
        at = rows_of(i, sum_out.rows)
        m.ototal[at] = (m.mid[at] + m.ototal[at].astype(F32) + b_two).astype(BF16)

    gain_one = m.vec[0:1, :]

    def final(i):
        sum_one.accept(i)
        at = rows_of(i, CHUNK)
        e = m.total[at].astype(F32) * gain_one
        xhat, r = normalize(m.xp[at].astype(F32))
        mean = jnp.mean(e, axis=-1, keepdims=True)
        along = jnp.mean(e * xhat, axis=-1, keepdims=True)
        m.igrad[at] = m.xh2[at] + r * (e - mean - xhat * along)

    def tail(i):
        sum_one.pump(i + tiles)
        final(i)

    def unpack():
        got = sq.finish()
        for h in range(nh):
            cols = slice(h * HEAD_DIM, (h + 1) * HEAD_DIM)
            m.owk[:, cols] = got[:, h * 128 : h * 128 + 64]
            m.owv[:, cols] = got[:, h * 128 + 64 : (h + 1) * 128]
        m.owq[...] = got[:, nh * 128 : nh * 128 + local]

    def vectors():
        for k in range(len(vec_steps) - 2, len(vec_steps)):
            vec_take(k)
        m.ovec[...] = fill(m.ovec.shape, 0)
        names = (GAIN_ONE, SHIFT_ONE, B_OUT, GAIN_TWO, SHIFT_TWO, B_FC_TWO)
        for b in range(cube.size):

            @pl.when(cube.rank() == b)
            def _(b=b):
                for place, row in enumerate(names):
                    m.ovec[place : place + 1, :rows] = m.vs[row : row + 1, b * rows : (b + 1) * rows]

        m.ovec[6:7, :local] = m.vs[B_QKV : B_QKV + 1, nh * 128 : nh * 192]
        for h in range(nh):
            m.ovec[7:8, h * 64 : (h + 1) * 64] = m.vs[B_QKV : B_QKV + 1, h * 128 + 64 : (h + 1) * 128]
        m.ovec[8:9, :] = m.vs[B_FC_ONE : B_FC_ONE + 1, :]

    def outputs():
        loop(0, big, sum_out.drain)
        loop(0, big, output)

    def early():
        m.ow1[...] = s1.finish()
        m.ow2[...] = s2.finish()
        m.owo[...] = so.finish().T

    def cubed():
        for k in range(1, len(vec_steps) - 2):
            vec_take(k)

    vec_take(0)
    stop = chunks + LAG - tiles
    jobs = (early, sq.step, cubed, sq.step, outputs, unpack, vectors)
    share = stop // len(jobs)
    for part, job in enumerate(jobs):
        loop(part * share, (part + 1) * share, tail)
        job()
    loop(len(jobs) * share, stop, tail)
    loop(stop, chunks, final)

    for copy in kv_copies + vec_copies:
        copy.wait_send()
    for s in (s1, s2, so, sq):
        s.drain()
    loop(0, chunks, sum_one.drain)


def layer(tokens, shares, biases, weights, mesh_shape):
    nz = mesh_shape["head"]
    cube = Cube(mesh_shape["clip"], mesh_shape["seq"])
    frames, width = tokens[0].shape
    rows, local = weights[0].shape
    hidden = weights[4].shape[1]
    nh = local // HEAD_DIM
    padded = -(-frames // BLOCK) * BLOCK
    colors = 2 if rows % 32 == 0 else 1
    half = rows // colors
    packed = -(-(nh * 192) // 128) * 128
    nb = cube.size
    steps = len(cube.all_bits) + len(powers(nz))
    token_names, bias_names = ("x", "cot"), ("bq", "bv", "bf1")
    weight_names = ("wq", "wk", "wv", "wo", "w1", "w2")
    share_names = tuple(f"share{i}" for i in range(len(shares)))
    names = token_names + share_names + bias_names + weight_names
    ins = dict(zip(names, (*tokens, *shares, *biases, *weights)))
    outs = dict(
        ototal=((padded, width), BF16),
        igrad=((padded, width), F32),
        ovec=((16, width), F32),
        owq=((rows, local), F32),
        owk=((rows, local), F32),
        owv=((rows, local), F32),
        owo=((local, rows), F32),
        ow1=((rows, hidden), F32),
        ow2=((rows, hidden), F32),
    )
    flat = (padded, width)
    scratch = dict(
        gq=((nb, colors, half, packed), BF16),
        go=((nz, nb, colors, half, local), BF16),
        g1=((nb, colors, half, hidden), BF16),
        g2=((nb, colors, half, hidden), BF16),
        gv=((nb, 8, 128), F32),
        vec=((8, width), F32),
        bias=((8, packed), F32),
        mid=(flat, F32),
        n1=(flat, BF16),
        q=((nh, padded, 128), BF16),
        kv=((2, nh, padded, 128), BF16),
        kvt=((2, nh, 128, padded), BF16),
        vo=((2, nh, padded, 128), BF16),
        p=((nh, padded, 2 * padded), BF16),
        il=((nh, padded, 128), F32),
        atto=((nh, padded, 128), BF16),
        attz=((nz, nh, padded // 2, 128), BF16),
        xp=(flat, BF16),
        gp=(flat, BF16),
        xh2=(flat, F32),
        r2=((padded, 128), F32),
        n2=(flat, BF16),
        act=((padded, hidden), BF16),
        gpre=((padded, hidden), BF16),
        acc=((8, 8, width), F32),
        vs=((8, width), F32),
        vo_=((steps, 8, width), F32),
        vr=((steps, 8, width), F32),
        part=(flat, BF16),
        landed=(flat, BF16),
        crossed=(flat, BF16),
        crossed_one=(flat, BF16),
        total=(flat, BF16),
        opart=(flat, BF16),
        olanded=(flat, BF16),
        ocrossed=(flat, BF16),
        at=((padded, local), BF16),
        qt=((nh, 128, padded), BF16),
        dat=((nh, 128, padded), BF16),
        dkv=((2, nh, 128, padded), F32),
        kvs=((nh, 128, padded), BF16),
        kvr=((nh, 128, padded), BF16),
        ds=((BLOCK, 2 * padded), BF16),
        dw1=((width, hidden), BF16),
        dl1=((colors, nb - 1, half, hidden), BF16),
        dw2=((width, hidden), BF16),
        dl2=((colors, nb - 1, half, hidden), BF16),
        dwo=((width, local), BF16),
        dlo=((colors, nb - 1, half, local), BF16),
        dwq=((width, packed), BF16),
        dlq=((colors, nb - 1, half, packed), BF16),
    )
    small, large = padded // CHUNK, 6
    lines = 3 * (2 * small + large)
    count = lines + 9 * colors * (nb - 1) + 60

    def body(*refs):
        names = list(ins) + list(outs) + list(scratch)
        m = types.SimpleNamespace(**dict(zip(names, refs)))
        send, recv = refs[len(names) :]
        m.shares = [getattr(m, name) for name in share_names]
        sems = Sems(send, recv)
        sems.used = lines
        sum_two = LineSum(nz, send, recv, 0, small, CHUNK, m.part, m.landed, m.crossed, m.total)
        sum_one = LineSum(nz, send, recv, 3 * small, small, CHUNK, m.part, m.landed, m.crossed_one, m.total)
        sum_out = LineSum(nz, send, recv, 6 * small, large, padded // large, m.opart, m.olanded, m.ocrossed, m.ototal)
        stage_one(m, cube, nz, sems)
        stage_two(m, cube, nz, sum_two, sum_out)
        stage_three(m, cube, nz, sems, sum_two, sum_out, sum_one)
        assert sems.used <= count, (sems.used, count)

    res = pl.pallas_call(
        body,
        out_shape=[jax.ShapeDtypeStruct(*v) for v in outs.values()],
        in_specs=[pl.BlockSpec(memory_space=pltpu.VMEM)] * len(ins),
        out_specs=[pl.BlockSpec(memory_space=pltpu.VMEM)] * len(outs),
        scratch_shapes=[pltpu.VMEM(*v) for v in scratch.values()] + [pltpu.SemaphoreType.DMA((count,))] * 2,
        compiler_params=pltpu.CompilerParams(
            collective_id=0, has_side_effects=True, vmem_limit_bytes=67_043_328
        ),
        name="layer",
    )(*ins.values())
    return types.SimpleNamespace(**dict(zip(outs, res)))


def finish(res, frames):
    padded, width = res.ototal.shape
    rows, local = res.owq.shape
    hidden = res.ow1.shape[1]
    tile = 256
    whole = lambda shape: pl.BlockSpec(shape, lambda i: (0,) * len(shape))
    sizes = [rows] * 6 + [local] * 2 + [hidden]
    passed = (res.owq, res.owk, res.owv, res.owo, res.ow1, res.ow2)

    def body(out_ref, grad_ref, vec_ref, *refs):
        ins, (to_out, to_grad, *rest) = refs[: len(passed)], refs[len(passed) :]
        to_out[...] = out_ref[...]
        to_grad[:, 0, :] = grad_ref[...]

        @pl.when(pl.program_id(0) == 0)
        def _():
            for source, target in zip(ins, rest):
                target[...] = source[...]
            *vectors, last = rest[len(passed) :]
            for i, target in enumerate(vectors):
                target[...] = vec_ref[i : i + 1, : sizes[i]]
            for i in range(hidden // 128):
                last[i : i + 1, :] = vec_ref[len(vectors) : len(vectors) + 1, i * 128 : (i + 1) * 128]

    row_tile = pl.BlockSpec((tile, width), lambda i: (i, 0))
    vectors = [jax.ShapeDtypeStruct((1, size), F32) for size in sizes[:-1]]
    vectors.append(jax.ShapeDtypeStruct((hidden // 128, 128), F32))
    kept = [jax.ShapeDtypeStruct(a.shape, a.dtype) for a in passed]
    return pl.pallas_call(
        body,
        grid=(padded // tile,),
        out_shape=[
            jax.ShapeDtypeStruct((frames, width), BF16),
            jax.ShapeDtypeStruct((frames, 1, width), F32),
            *kept,
            *vectors,
        ],
        in_specs=[row_tile, row_tile, whole(res.ovec.shape)] + [whole(a.shape) for a in passed],
        out_specs=[
            row_tile,
            pl.BlockSpec((tile, 1, width), lambda i: (i, 0, 0)),
            *[whole(a.shape) for a in kept + vectors],
        ],
        name="finish",
    )(res.ototal, res.igrad, res.ovec, *passed)


def on_device(
    inputs,
    gain_one,
    shift_one,
    w_query,
    b_query,
    w_key,
    w_value,
    b_value,
    w_out,
    b_out,
    gain_two,
    shift_two,
    w_fc_one,
    b_fc_one,
    w_fc_two,
    b_fc_two,
    cotangent,
    mesh_shape,
):
    clips, frames, width = inputs.shape
    count = clips * frames
    row = lambda v: v.reshape(1, -1)
    res = layer(
        (inputs.reshape(count, width), cotangent.reshape(count, width)),
        tuple(row(v) for v in (gain_one, shift_one, gain_two, shift_two, b_out, b_fc_two)),
        (b_query, b_value, b_fc_one),
        (w_query, w_key, w_value, w_out, w_fc_one, w_fc_two.T),
        mesh_shape,
    )
    outputs, grad, g_query, g_key, g_value, g_out, g_one, g_two, *vectors = finish(res, count)
    g1, s1, b_o, g2, s2, b_two, b_q, b_v, b_one = (v.reshape(-1) for v in vectors)
    return (
        outputs.reshape(clips, frames, width),
        grad.transpose(1, 0, 2).reshape(clips, frames, width),
        g1,
        s1,
        g_query,
        b_q,
        g_key,
        g_value,
        b_v,
        g_out,
        b_o,
        g2,
        s2,
        g_one,
        b_one,
        g_two.T,
        b_two,
    )


def solution(mesh):
    group = ("clip", "seq")
    rows, columns, own, heads = P(group, "head"), P("head", group), P(group), P("head")
    tokens = P("clip", "seq", None)
    return jax.shard_map(
        partial(on_device, mesh_shape=dict(mesh.shape)),
        mesh=mesh,
        in_specs=(
            tokens, own, own, rows, heads, rows, rows, heads, columns,
            own, own, own, rows, heads, columns, own, tokens,
        ),
        out_specs=(
            tokens, tokens, own, own, rows, heads, rows, rows, heads,
            columns, own, own, own, rows, heads, columns, own,
        ),
        check_vma=False,
    )
```

```python
from functools import partial
import types

import jax
import jax.numpy as jnp
from jax import lax
from jax.experimental import pallas as pl
from jax.experimental.pallas import tpu as pltpu
from jax.sharding import PartitionSpec as P

HEAD_DIM = 64
EPS = 1e-05
F32 = jnp.float32
BF16 = jnp.bfloat16
MESH = pl.DeviceIdType.MESH


def flip(value, bit):
    return value + bit * (1 - 2 * lax.rem(lax.div(value, bit), 2))


def flips(value, mask, bits):
    for bit in bits:
        if mask & bit:
            value = flip(value, bit)
    return value


def powers(size):
    bits, bit = [], 1
    while bit < size:
        bits.append(bit)
        bit *= 2
    return bits


class Cube:
    def __init__(self, clips, seqs):
        self.clips, self.seqs, self.size = clips, seqs, clips * seqs
        self.seq_bits = [(bit, "seq", bit) for bit in powers(seqs)]
        self.clip_bits = [(bit * seqs, "clip", bit) for bit in powers(clips)]
        core, rest = self.clip_bits[:1], self.clip_bits[1:]
        self.orders = (
            self.seq_bits + rest + core,
            rest[:1] + self.seq_bits + rest[1:] + core,
        )
        self.all_bits = [bit for bit, _, _ in self.seq_bits + self.clip_bits]

    def rank(self):
        return lax.axis_index("clip") * self.seqs + lax.axis_index("seq")

    def block(self, mask):
        return flips(self.rank(), mask, self.all_bits)

    @staticmethod
    def peer(step):
        _, axis, bit = step
        return {axis: flip(lax.axis_index(axis), bit)}


class Sems:
    def __init__(self, send, recv):
        self.send, self.recv, self.used = send, recv, 0

    def take(self):
        self.used += 1
        return self.send.at[self.used - 1], self.recv.at[self.used - 1]


def remote(src, dst, sems, device):
    return pltpu.make_async_remote_copy(
        src_ref=src,
        dst_ref=dst,
        send_sem=sems[0],
        recv_sem=sems[1],
        device_id=device,
        device_id_type=MESH,
    )


class Gather:
    def __init__(self, cube, sems, view, colors):
        self.cube, self.view, self.colors = cube, view, colors
        self.steps = len(cube.orders[0])
        self.copies = [[[] for _ in range(self.steps)] for _ in range(colors)]
        for color in range(colors):
            masks = [0]
            for k, step in enumerate(cube.orders[color]):
                for mask in masks:
                    block = cube.block(mask)
                    piece = view(block, color)
                    self.copies[color][k].append(
                        remote(piece, piece, sems.take(), cube.peer(step))
                    )
                masks = masks + [mask ^ step[0] for mask in masks]

    def start(self, k, color):
        for copy in self.copies[color][k]:
            copy.start()

    def advance(self, k, color):
        for copy in self.copies[color][k]:
            copy.wait_recv()
        if k + 1 < self.steps:
            self.start(k + 1, color)

    def drain(self):
        for color in range(self.colors):
            for step in self.copies[color]:
                for copy in step:
                    copy.wait_send()


def normalize(rows):
    mean = jnp.mean(rows, axis=-1, keepdims=True)
    centered = rows - mean
    spread = jnp.mean(centered * centered, axis=-1, keepdims=True)
    inverse = lax.rsqrt(spread + EPS)
    return centered * inverse, inverse


def dot(a, b):
    return jnp.dot(a, b, preferred_element_type=F32)


def dot_nt(a, b):
    return lax.dot_general(a, b, (((1,), (1,)), ((), ())), preferred_element_type=F32)


def dot_tn(a, b):
    return lax.dot_general(a, b, (((0,), (0,)), ((), ())), preferred_element_type=F32)


NEG = -1e30
LINE_LAG = 3


def fill(shape, value, dtype=F32):
    return jnp.full(shape, value, dtype)


def lane(shape):
    return lax.broadcasted_iota(jnp.int32, shape, len(shape) - 1)


class Line:
    def __init__(self, nodes, send, recv, base, view, parts):
        self.n, self.z = nodes, lax.axis_index("head")
        self.send_sem, self.recv_sem, self.base = send, recv, base
        self.view, self.parts = view, parts

    @staticmethod
    def count(nodes, parts):
        return 2 * (nodes - 1) * parts

    def moves(self, hop, part):
        z, n = self.z, self.n

        def copy(origin, way, target):
            piece = self.view(origin, part)
            place = self.base + (way * (n - 1) + hop) * self.parts + part
            sems = self.send_sem.at[place], self.recv_sem.at[place]
            return remote(piece, piece, sems, {"head": target})

        sends = (
            ((z >= hop) & (z < n - 1), lambda: copy(z - hop, 0, z + 1)),
            ((n - 1 - z >= hop) & (z > 0), lambda: copy(z + hop, 1, z - 1)),
        )
        arrivals = (
            (z > hop, lambda: copy(z - 1 - hop, 0, z - 1)),
            (n - 1 - z > hop, lambda: copy(z + 1 + hop, 1, z + 1)),
        )
        return sends, arrivals

    def start(self, hop, part):
        for condition, copy in self.moves(hop, part)[0]:
            pl.when(condition)(lambda copy=copy: copy().start())

    def arrive(self, hop, part):
        for condition, copy in self.moves(hop, part)[1]:
            pl.when(condition)(lambda copy=copy: copy().wait_recv())

    def pump(self, step):
        @pl.when(step < self.parts)
        def _():
            self.start(0, step)

        for hop in range(self.n - 1):
            part = step - LINE_LAG * (hop + 1)

            @pl.when((part >= 0) & (part < self.parts))
            def _(hop=hop, part=part):
                self.arrive(hop, part)
                if hop + 1 < self.n - 1:
                    self.start(hop + 1, part)

    def drain(self, part):
        for hop in range(self.n - 1):
            for condition, copy in self.moves(hop, part)[0]:
                pl.when(condition)(lambda copy=copy: copy().wait_send())


def entry_peers(cube, heads):
    z = lax.axis_index("head")
    peers = [cube.peer(step) for step in cube.orders[0]]
    return peers + [{"head": lax.rem(z + d, heads)} for d in range(1, heads)]


def greet(peers):
    for peer in peers:
        pl.semaphore_signal(pltpu.get_barrier_semaphore(), inc=1, device_id=peer, device_id_type=MESH)


def stage_one(m, cube, nz, sems, line):
    z = lax.axis_index("head")
    r = cube.rank()
    rows = m.wq.shape[0]
    colors = m.gq.shape[1]
    half = rows // colors
    nh = m.q.shape[0]
    frames = m.x.shape[0]
    padded = m.xp.shape[0]
    tile = 128
    tiles = padded // tile
    width = m.x.shape[1]

    peers = entry_peers(cube, nz)
    greet(peers)
    gk = Gather(cube, sems, lambda b, c: m.gk.at[b, c], colors)
    gq = Gather(cube, sems, lambda b, c: m.gq.at[b, c], colors)
    gv = Gather(cube, sems, lambda b, c: m.gv.at[b], 1)
    g1 = Gather(cube, sems, lambda b, c: m.g1.at[b, c], colors)
    g2 = Gather(cube, sems, lambda b, c: m.g2.at[b, c], colors)
    go = Gather(cube, sems, lambda b, c: m.go.at[:, b, c], colors)

    m.vec[...] = fill(m.vec.shape, 0)
    for name in m.first_loads:
        m.load[name].wait()
    for row, ref in enumerate(m.shares):
        m.vec[row : row + 1, :rows] = ref[...].astype(F32)
    m.gv[r] = m.vec[:, :128]
    for c in range(colors):
        part = pl.ds(c * half, half)
        for h in range(nh):
            cols = slice(h * HEAD_DIM, (h + 1) * HEAD_DIM)
            m.gk[r, c, :, h * 128 : h * 128 + 64] = m.wk[part, cols]
            m.gk[r, c, :, h * 128 + 64 : (h + 1) * 128] = m.wv[part, cols]
        m.gq[r, c, :, : nh * 64] = m.wq[part, :]
        spare = m.gq.shape[3] - nh * 64
        if spare:
            m.gq[r, c, :, nh * 64 :] = fill((half, spare), 0, BF16)

    pl.semaphore_wait(pltpu.get_barrier_semaphore(), len(peers))
    gv.start(0, 0)
    for g in (gk, gq):
        for c in range(colors):
            g.start(0, c)

    for name in m.next_loads:
        m.load[name].wait()
    wot = m.wo[...].T
    for c in range(colors):
        part = slice(c * half, (c + 1) * half)
        m.go[z, r, c] = wot[part]
        m.g2[r, c] = m.w2[part, :]
        m.g1[r, c] = m.w1[part, :]
    out_sems = [sems.take() for _ in range(nz - 1)]

    def out_copies(arriving):
        for d in range(1, nz):
            origin = lax.rem(z + nz - d, nz) if arriving else z
            target = lax.rem(z + d, nz)
            piece = m.go.at[origin, r]
            yield remote(piece, piece, out_sems[d - 1], {"head": target})

    for copy in out_copies(False):
        copy.start()
    m.xp[0:frames] = m.x[...]
    m.xp[frames:padded] = fill((padded - frames, width), 0, BF16)

    def norm_tile(i, carry):
        at = pl.ds(pl.multiple_of(i * tile, tile), tile)
        xhat, _ = normalize(m.xp[at].astype(F32))
        m.xh2[at] = xhat
        return carry

    third = tiles // gq.steps
    for k in range(gq.steps):
        top = tiles if k == gq.steps - 1 else third * (k + 1)
        lax.fori_loop(third * k, top, norm_tile, 0)
        gv.advance(k, 0)
        for c in range(colors):
            gk.advance(k, c)
        if k < gq.steps - 1:
            for c in range(colors):
                gq.advance(k, c)
        if k == 0:
            for g in (g1, g2):
                for c in range(colors):
                    g.start(0, c)
    for b in range(cube.size):
        m.vec[:, b * rows : (b + 1) * rows] = m.gv[b, :, :rows]
    gain, shift = m.vec[0:1, :], m.vec[1:2, :]
    m.bias[...] = fill(m.bias.shape, 0)
    bv = m.bv[...].astype(F32)[None, :]
    for h in range(nh):
        m.bias[0:1, h * 128 + 64 : (h + 1) * 128] = bv[:, h * HEAD_DIM : (h + 1) * HEAD_DIM]
    m.bias[1:2, : nh * 64] = m.bq[...].astype(F32)[None, :]
    scale = HEAD_DIM**-0.5

    def project(i, carry):
        at = pl.ds(pl.multiple_of(i * tile, tile), tile)
        n1 = (m.xh2[at] * gain + shift).astype(BF16)
        m.n1[at] = n1
        packed = dot(n1, m.gk[...].reshape(cube.size * rows, nh * 128)) + m.bias[0:1, : nh * 128]
        for h in range(nh):
            m.kv[0, h, at] = packed[:, h * 128 : (h + 1) * 128].astype(BF16)
        return carry

    lax.fori_loop(0, tiles, project, 0)

    kv_sems = [sems.take() for _ in range(nh)]
    other = {"seq": flip(lax.axis_index("seq"), 1)}
    kv_copies = [
        remote(m.kv.at[0, h], m.kv.at[1, h], kv_sems[h], other) for h in range(nh)
    ]
    kv_copies[0].start()
    for copy in out_copies(True):
        copy.wait_recv()
    for c in range(colors):
        go.start(0, c)
    for copy in kv_copies[1:]:
        copy.start()
    for c in range(colors):
        gq.advance(gq.steps - 1, c)

    def project_query(i, carry):
        at = pl.ds(pl.multiple_of(i * tile, tile), tile)
        wide = m.gq.shape[3]
        packed = dot(m.n1[at], m.gq[...].reshape(cube.size * rows, wide)) + m.bias[1:2, :wide]
        left = lane((tile, 128)) < 64
        for h in range(nh):
            pair = packed[:, (h // 2) * 128 : (h // 2) * 128 + 128]
            if h % 2:
                pair = pltpu.roll(pair, 64, 1)
            pair = pair.astype(BF16).astype(F32) * scale
            m.q[h, at] = jnp.where(left, pair, 0.0).astype(BF16)
        return carry

    lax.fori_loop(0, tiles, project_query, 0)

    left = lane((padded, 128)) < 64

    def prepare(part, h):
        block = m.kv[part, h]
        m.kvt[part, h] = block.T
        m.vo[part, h] = jnp.where(left, jnp.ones_like(block), block)

    for h in range(nh):
        prepare(0, h)

    block = 256
    valid = frames - (padded - 128)

    def attend(h):
        def one(b, carry):
            at = pl.ds(pl.multiple_of(b * block, block), block)
            query = m.q[h, at]
            keep = lane((block, 128)) < valid
            parts = []
            top = None
            for part in range(2):
                s = dot(query, m.kvt[part, h])
                body, tail = s[:, : padded - 128], s[:, padded - 128 :]
                tail = jnp.where(keep, tail, NEG)
                parts += [body, tail]
                high = jnp.maximum(jnp.max(body, axis=1, keepdims=True), jnp.max(tail, axis=1, keepdims=True))
                top = high if top is None else jnp.maximum(top, high)
            place = 0
            for s in parts:
                m.p[h, at, place : place + s.shape[1]] = jnp.exp(s - top).astype(BF16)
                place += s.shape[1]
            acc = dot(m.p[h, at, :padded], m.vo[0, h]) + dot(m.p[h, at, padded:], m.vo[1, h])
            inverse = 1.0 / pltpu.roll(acc, 64, 1)
            att = acc * inverse
            right = lane((block, 128)) >= 64
            m.il[h, at] = jnp.where(right, inverse, 0.0)
            m.atto[h, at] = jnp.where(right, att, 0.0).astype(BF16)
            turned = pltpu.roll(att, 64, 1)
            pieces = [
                jnp.where(right[:64], att[g + 64 : g + 128], turned[g : g + 64])
                for g in range(0, block, 128)
            ]
            part = h * (padded // block) + b
            m.attz[z, part] = jnp.concatenate(pieces, axis=0).astype(BF16)
            line.pump(part)
            return carry

        lax.fori_loop(0, padded // block, one, 0)

    def weights(gathers, k, c):
        if c < colors and k < g1.steps - 1:
            for g in gathers:
                g.advance(k, c)

    feed = (g1, g2)
    plan = {0: ((feed, 0, 0), (feed, 0, 1)), 1: (((go,), 0, 0), ((go,), 0, 1))}
    plan[nh - 1] = ((feed, 1, 0),)
    for h in range(nh):
        kv_copies[h].wait_recv()
        prepare(1, h)
        attend(h)
        for job in plan.get(h, ()):
            weights(*job)
    parts = line.parts
    stop = parts + LINE_LAG * (nz - 1)
    loop(parts, parts + 3, line.pump)
    weights((go,), 1, 0)
    weights(feed, 1, 1)
    loop(parts + 3, stop - 2, line.pump)
    weights((go,), 1, 1)
    loop(stop - 2, stop, line.pump)
    for k in range(2, g1.steps):
        for g in (go, g1, g2):
            for c in range(colors):
                g.advance(k, c)

    for copy in kv_copies:
        copy.wait_send()
    for copy in out_copies(False):
        copy.wait_send()
    for g in (gv, gk, gq, g1, g2, go):
        g.drain()
    loop(0, line.parts, line.drain)


class Scatter:
    def __init__(self, cube, sems, buffer, landing, rows, colors):
        self.cube, self.buffer, self.landing = cube, buffer, landing
        self.rows, self.colors, self.half = rows, colors, rows // colors
        self.steps = len(cube.orders[0])
        self.plan = [[[] for _ in range(self.steps)] for _ in range(colors)]
        for color in range(colors):
            masks, slot = [0], 0
            for k, step in enumerate(cube.orders[color]):
                for mask in masks:
                    copy = remote(
                        self.view(cube.block(mask ^ step[0]), color),
                        landing.at[color, slot],
                        sems.take(),
                        cube.peer(step),
                    )
                    self.plan[color][k].append((mask, slot, copy))
                    slot += 1
                masks = masks + [mask ^ step[0] for mask in masks]

    def view(self, block, color):
        start = block * self.rows + color * self.half
        return self.buffer.at[pl.ds(pl.multiple_of(start, 8), self.half)]

    def start(self):
        self.left = self.steps - 1
        self.send(self.left)

    def step(self):
        if self.left > 0:
            self.advance(self.left)
            self.left -= 1

    def send(self, k):
        for color in range(self.colors):
            for _, _, copy in self.plan[color][k]:
                copy.start()

    def advance(self, k):
        for color in range(self.colors):
            for mask, slot, copy in self.plan[color][k]:
                copy.wait_recv()
                view = self.view(self.cube.block(mask), color)
                total = view[...].astype(F32) + self.landing[color, slot].astype(F32)
                view[...] = total.astype(BF16)
            for _, _, copy in self.plan[color][k - 1]:
                copy.start()

    def finish(self):
        while self.left > 0:
            self.step()
        parts = []
        for color in range(self.colors):
            ((_, slot, copy),) = self.plan[color][0]
            copy.wait_recv()
            view = self.view(self.cube.block(0), color)
            parts.append(view[...].astype(F32) + self.landing[color, slot].astype(F32))
        return parts[0] if len(parts) == 1 else jnp.concatenate(parts, axis=0)

    def drain(self):
        for color in range(self.colors):
            for step in self.plan[color]:
                for _, _, copy in step:
                    copy.wait_send()


class LineSum:
    def __init__(self, nz, send, recv, ends, middle, chunks, rows, part, landed, crossed, total):
        z = lax.axis_index("head")
        self.inner = (z > 0) & (z < nz - 1)
        self.mate, self.cross = {"head": flip(z, 1)}, {"head": nz - 1 - z}
        self.send_sem, self.recv_sem, self.bases = send, recv, (ends, middle, ends)
        self.chunks, self.rows = chunks, rows
        self.part, self.landed, self.crossed, self.total = part, landed, crossed, total

    def at(self, ref, i):
        return ref.at[pl.ds(pl.multiple_of(i * self.rows, self.rows), self.rows)]

    def sems(self, kind, i):
        place = self.bases[kind] + i
        return self.send_sem.at[place], self.recv_sem.at[place]

    def first(self, i):
        return remote(self.at(self.part, i), self.at(self.landed, i), self.sems(0, i), self.mate)

    def second(self, i):
        return remote(self.at(self.part, i), self.at(self.crossed, i), self.sems(1, i), self.cross)

    def third(self, i):
        piece = self.at(self.total, i)
        return remote(piece, piece, self.sems(2, i), self.mate)

    def offer(self, i):
        @pl.when(jnp.logical_not(self.inner))
        def _():
            self.first(i).start()

    def relay(self, i):
        @pl.when(self.inner)
        def _():
            self.first(i).wait_recv()
            view = self.at(self.part, i)
            total = view[...].astype(F32) + self.at(self.landed, i)[...].astype(F32)
            view[...] = total.astype(BF16)
            self.second(i).start()

    def pump(self, i):
        @pl.when(i < self.chunks)
        def _():
            self.relay(i)

        @pl.when(i >= LAG)
        def _():
            self.close(i - LAG)

    def close(self, i):
        @pl.when(self.inner)
        def _():
            self.second(i).wait_recv()
            total = self.at(self.part, i)[...].astype(F32) + self.at(self.crossed, i)[...].astype(F32)
            self.at(self.total, i)[...] = total.astype(BF16)
            self.third(i).start()

    def accept(self, i):
        @pl.when(jnp.logical_not(self.inner))
        def _():
            self.third(i).wait_recv()

    def drain(self, i):
        @pl.when(self.inner)
        def _():
            self.second(i).wait_send()
            self.third(i).wait_send()

        @pl.when(jnp.logical_not(self.inner))
        def _():
            self.first(i).wait_send()


def loop(start, stop, step):
    lax.fori_loop(start, stop, lambda i, carry: (step(i), carry)[1], 0)


def rows_of(i, size):
    return pl.ds(pl.multiple_of(i * size, size), size)


def add_rows(m, row, values):
    count, width = values.shape
    m.acc[row, :, :width] += jnp.sum(values.reshape(count // 8, 8, width), axis=0)


B_FC_TWO, GAIN_TWO, SHIFT_TWO, B_OUT, GAIN_ONE, SHIFT_ONE, B_QKV, B_FC_ONE = range(8)
BLOCK = 256
STEP = 128
CHUNK = 32
LAG = 4


def stage_two(m, cube, nz, sum_two, sum_out):
    padded, width = m.xp.shape
    rows = m.wq.shape[0]
    nh = m.q.shape[0]
    frames = m.cot.shape[0]
    hidden = m.w1.shape[1]
    m.load["cot"].wait()
    m.gp[0:frames] = m.cot[...]
    m.gp[frames:padded] = fill((padded - frames, width), 0, BF16)
    m.acc[...] = fill(m.acc.shape, 0)
    gain, shift, b_out = m.vec[2:3, :], m.vec[3:4, :], m.vec[4:5, :]
    b_one = m.bf1[...].astype(F32)[None, :]
    per = STEP // CHUNK
    w_one = lambda: m.g1[...].reshape(cube.size * rows, hidden)
    w_two = lambda: m.g2[...].reshape(cube.size * rows, hidden)

    def block(b):
        at = rows_of(b, STEP)
        packed = rows_of(lax.rem(b, 2), STEP // 2)
        mid = m.xp[at].astype(F32) + b_out
        for zz in range(nz):
            pieces = [m.attz[zz, h * (padded // BLOCK) + lax.div(b, 2), packed] for h in range(nh)]
            top = jnp.concatenate([p[:, :64] for p in pieces], axis=1)
            low = jnp.concatenate([p[:, 64:] for p in pieces], axis=1)
            att = jnp.concatenate([top, low], axis=0)
            mid = mid + dot_nt(att, m.go[zz].reshape(cube.size * rows, nh * HEAD_DIM))
        xhat, inverse = normalize(mid)
        m.mid[at] = mid
        m.xh2[at] = xhat
        m.r2[at] = jnp.broadcast_to(inverse, (STEP, 128))
        n2 = (xhat * gain + shift).astype(BF16)
        m.n2[at] = n2
        pre = dot(n2, w_one()) + b_one
        cdf = 0.5 + 0.5 * lax.erf(pre * 0.7071067811865476)
        act = (pre * cdf).astype(BF16)
        m.act[at] = act
        slope = cdf + pre * jnp.exp(pre * pre * -0.5) * 0.3989422804014327
        g = m.gp[at]
        add_rows(m, B_FC_TWO, g.astype(F32))
        gpre = (dot(g, w_two()) * slope).astype(BF16)
        m.gpre[at] = gpre
        add_rows(m, B_FC_ONE, gpre.astype(F32))
        back = dot_nt(gpre, w_one())
        add_rows(m, GAIN_TWO, back * m.xh2[at])
        add_rows(m, SHIFT_TWO, back)
        m.part[at] = back.astype(BF16)
        loop(0, per, lambda j: sum_two.offer(b * per + j))

        @pl.when(b >= 2)
        def _():
            sum_two.pump(2 * b - 4)
            sum_two.pump(2 * b - 3)

        m.opart[at] = dot_nt(m.act[at], w_two()).astype(BF16)

    loop(0, padded // STEP, block)
    loop(0, sum_out.chunks, sum_out.offer)


def stage_three(m, cube, nz, sems, sum_two, sum_out, sum_one):
    z = lax.axis_index("head")
    padded, width = m.xp.shape
    rows = m.wq.shape[0]
    nh = m.q.shape[0]
    local = nh * HEAD_DIM
    colors = m.gq.shape[1]
    chunks = padded // CHUNK
    blocks = padded // BLOCK
    per = STEP // CHUNK
    scale = HEAD_DIM**-0.5
    packed = m.gk.shape[3] + m.gq.shape[3]
    s1 = Scatter(cube, sems, m.dw1, m.dl1, rows, colors)
    s2 = Scatter(cube, sems, m.dw2, m.dl2, rows, colors)
    so = Scatter(cube, sems, m.dwo, m.dlo, rows, colors)
    sq = Scatter(cube, sems, m.dwq, m.dlq, rows, colors)
    tile = 128
    tiles = width // tile

    def product(left, right, into, columns):
        def one(i):
            cols = pl.ds(pl.multiple_of(i * tile, tile), tile)
            into[rows_of(i, tile)] = dot_tn(left[:, cols], right())[:, :columns].astype(BF16)

        return one

    one = product(m.n2, lambda: m.gpre[...], m.dw1, m.dw1.shape[1])
    two = product(m.gp, lambda: m.act[...], m.dw2, m.dw2.shape[1])

    def first(i):
        one(i)
        sum_two.pump(early + i)

    def second(i):
        two(i)
        sum_two.pump(early + tiles + i)

    early = 2 * (padded // STEP - 2)

    loop(0, tiles, first)
    s1.start()
    loop(0, tiles, second)
    s2.start()
    gain_two = m.vec[2:3, :]

    def middle(i):
        sum_two.accept(i)
        at = rows_of(i, CHUNK)
        n = m.total[at].astype(F32)
        e = n * gain_two
        xhat = m.xh2[at]
        r = m.r2[at][:, :1]
        mean = jnp.mean(e, axis=-1, keepdims=True)
        along = jnp.mean(e * xhat, axis=-1, keepdims=True)
        grad = m.gp[at].astype(F32) + r * (e - mean - xhat * along)
        m.xh2[at] = grad
        add_rows(m, B_OUT, grad)
        low = grad.astype(BF16)
        m.n2[at] = low
        da = dot(low, m.go[z].reshape(cube.size * rows, local)).astype(BF16).astype(F32)
        right = lane((CHUNK, 128)) >= 64
        for h in range(nh):
            base = (h // 2) * 128
            wide = da[:, base : min(base + 128, local)]
            if wide.shape[1] < 128:
                wide = jnp.concatenate([wide, jnp.zeros((CHUNK, 128 - wide.shape[1]), F32)], axis=1)
            if h % 2 == 0:
                wide = pltpu.roll(wide, 64, 1)
            m.act[at, h * 128 : (h + 1) * 128] = jnp.where(right, wide * m.il[h, at], 0.0).astype(BF16)
            m.at[at, h * 64 : (h + 1) * 64] = m.atto[h, at][:, 64:]

    ahead = early + 2 * tiles
    stop = chunks + LAG - ahead
    each = chunks // stop

    def pumped(i):
        sum_two.pump(i + ahead)
        loop(i * each, (i + 1) * each, middle)

    s1.step()
    fourth = stop // 4
    for part in range(4):
        loop(part * fourth, stop if part == 3 else (part + 1) * fourth, pumped)
        (s2, s1)[part % 2].step()
    loop(stop * each, chunks, middle)

    loop(0, tiles, product(m.n2, lambda: m.at[...], m.dwo, local))
    so.start()

    for h in range(nh):
        m.qt[h] = m.q[h].T
        m.dat[h] = m.act[:, h * 128 : (h + 1) * 128].T
    big = sum_out.chunks
    sum_out.relay(0)
    kv_sems = [sems.take() for _ in range(nh)]
    other = {"seq": flip(lax.axis_index("seq"), 1)}
    kv_copies = [remote(m.kvs.at[h], m.kvr.at[h], kv_sems[h], other) for h in range(nh)]
    for h in range(nh):
        m.dkv[0, h] = fill((128, padded), 0)
        m.dkv[1, h] = fill((128, padded), 0)

        def back(b, h=h):
            at = rows_of(b, BLOCK)
            da = m.act[at, h * 128 : (h + 1) * 128]
            inner = jnp.sum(da.astype(F32) * m.atto[h, at].astype(F32), axis=1, keepdims=True)
            for part in (1, 0):
                keys = slice(part * padded, (part + 1) * padded)
                dp = dot(da, m.kvt[part, h])
                p = m.p[h, at, keys]
                ds = (p.astype(F32) * (dp - inner)).astype(BF16)
                m.ds[:, keys] = ds
                m.dkv[part, h] += dot(m.qt[h, :, at], m.ds[:, keys]) + dot(m.dat[h, :, at], p)
            dq = dot(m.ds[:, :padded], m.kv[0, h]) + dot(m.ds[:, padded:], m.kv[1, h])
            dq = (dq * scale)[:, :64].astype(BF16)
            m.gpre[at, nh * 128 + h * 64 : nh * 128 + (h + 1) * 64] = dq
            point = h * blocks + b

            for i, (when, done) in enumerate(((2, None), (5, 0), (8, 1))):

                @pl.when(point == when)
                def _(i=i, done=done):
                    sum_out.relay(i + 1)
                    if done is not None:
                        sum_out.close(done)

        loop(0, blocks, back)
        m.kvs[h] = m.dkv[1, h].astype(BF16)
        kv_copies[h].start()
        if h < nh - 1:
            so.step()
    spare = packed - nh * 192
    if spare:
        m.gpre[:, nh * 192 : packed] = fill((padded, spare), 0, BF16)
    for h in range(nh):
        if h == nh - 1:
            sum_out.relay(4)
            sum_out.close(2)
        kv_copies[h].wait_recv()
        total = m.dkv[0, h] + m.kvr[h].astype(F32)
        m.gpre[:, h * 128 : (h + 1) * 128] = total.T.astype(BF16)

    def last(b):
        at = rows_of(b, STEP)
        grads = m.gpre[at, :packed]
        add_rows(m, B_QKV, grads.astype(F32))
        keys = nh * 128
        back = dot_nt(grads[:, :keys], m.gk[...].reshape(cube.size * rows, keys))
        back = back + dot_nt(grads[:, keys:], m.gq[...].reshape(cube.size * rows, packed - keys))
        xhat, _ = normalize(m.xp[at].astype(F32))
        add_rows(m, GAIN_ONE, back * xhat)
        add_rows(m, SHIFT_ONE, back)
        m.part[at] = back.astype(BF16)
        loop(0, per, lambda j: sum_one.offer(b * per + j))

    loop(0, chunks, sum_two.drain)
    loop(0, padded // STEP, last)
    one_q = product(m.n1, lambda: m.gpre[:, :packed], m.dwq, packed)

    def qkv(i):
        one_q(i)
        sum_one.pump(i)

    sum_out.relay(5)
    sum_out.close(3)
    loop(0, tiles, qkv)
    sq.start()
    sum_out.close(4)
    sum_out.close(5)

    for row in range(8):
        m.vs[row : row + 1, :] = jnp.sum(m.acc[row], axis=0, keepdims=True)
    vec_steps = [(cube.peer(step), False) for step in cube.orders[0]]
    vec_steps += [({"head": flip(z, bit)}, True) for bit in powers(nz)]
    row_id = lax.broadcasted_iota(jnp.int32, m.vs.shape, 0)
    partial_rows = (row_id == GAIN_TWO) | (row_id == SHIFT_TWO) | (row_id == GAIN_ONE) | (row_id == SHIFT_ONE)
    vec_copies = []

    def vec_send(k):
        if k < len(vec_steps):
            m.vo_[k] = m.vs[...]
            copy = remote(m.vo_.at[k], m.vr.at[k], sems.take(), vec_steps[k][0])
            copy.start()
            vec_copies.append(copy)

    def vec_take(k):
        if k < len(vec_steps):
            vec_copies[k].wait_recv()
            arrived = m.vr[k]
            if vec_steps[k][1]:
                arrived = jnp.where(partial_rows, arrived, 0.0)
            m.vs[...] += arrived
            vec_send(k + 1)

    vec_send(0)
    b_two = m.vec[5:6, :]

    def output(i):
        sum_out.accept(i)
        at = rows_of(i, sum_out.rows)
        m.ototal[at] = (m.mid[at] + m.ototal[at].astype(F32) + b_two).astype(BF16)

    gain_one = m.vec[0:1, :]

    def final(i):
        sum_one.accept(i)
        at = rows_of(i, CHUNK)
        e = m.total[at].astype(F32) * gain_one
        xhat, r = normalize(m.xp[at].astype(F32))
        mean = jnp.mean(e, axis=-1, keepdims=True)
        along = jnp.mean(e * xhat, axis=-1, keepdims=True)
        m.igrad[at] = m.xh2[at] + r * (e - mean - xhat * along)

    def tail(i):
        sum_one.pump(i + tiles)
        final(i)

    def unpack():
        got = sq.finish()
        for h in range(nh):
            cols = slice(h * HEAD_DIM, (h + 1) * HEAD_DIM)
            m.owk[:, cols] = got[:, h * 128 : h * 128 + 64]
            m.owv[:, cols] = got[:, h * 128 + 64 : (h + 1) * 128]
        m.owq[...] = got[:, nh * 128 : nh * 128 + local]
        for name in ("owk", "owv", "owq"):
            m.save[name].start()

    def vectors():
        for k in range(len(vec_steps) - 2, len(vec_steps)):
            vec_take(k)
        m.ovec[...] = fill(m.ovec.shape, 0)
        names = (GAIN_ONE, SHIFT_ONE, B_OUT, GAIN_TWO, SHIFT_TWO, B_FC_TWO)
        for b in range(cube.size):

            @pl.when(cube.rank() == b)
            def _(b=b):
                for place, row in enumerate(names):
                    m.ovec[place : place + 1, :rows] = m.vs[row : row + 1, b * rows : (b + 1) * rows]

        m.ovec[6:7, :local] = m.vs[B_QKV : B_QKV + 1, nh * 128 : nh * 192]
        for h in range(nh):
            m.ovec[7:8, h * 64 : (h + 1) * 64] = m.vs[B_QKV : B_QKV + 1, h * 128 + 64 : (h + 1) * 128]
        m.ovec[8:9, :] = m.vs[B_FC_ONE : B_FC_ONE + 1, :]
        m.save["ovec"].start()

    def outputs():
        loop(0, big, sum_out.drain)
        loop(0, big, output)
        m.save["ototal"].start()

    def early():
        m.ow1[...] = s1.finish()
        m.save["ow1"].start()
        m.ow2[...] = s2.finish()
        m.save["ow2"].start()
        m.owo[...] = so.finish().T
        m.save["owo"].start()

    def cubed():
        for k in range(1, len(vec_steps) - 2):
            vec_take(k)

    vec_take(0)
    stop = chunks + LAG - tiles
    jobs = (early, sq.step, cubed, sq.step, outputs, unpack, vectors)
    share = stop // len(jobs)
    for part, job in enumerate(jobs):
        loop(part * share, (part + 1) * share, tail)
        job()
    loop(len(jobs) * share, stop, tail)
    loop(stop, chunks, final)
    m.save["igrad"].start()

    for copy in kv_copies + vec_copies:
        copy.wait_send()
    for s in (s1, s2, so, sq):
        s.drain()
    loop(0, chunks, sum_one.drain)


def layer(tokens, shares, biases, weights, mesh_shape):
    nz = mesh_shape["head"]
    cube = Cube(mesh_shape["clip"], mesh_shape["seq"])
    frames, width = tokens[0].shape
    rows, local = weights[0].shape
    hidden = weights[4].shape[1]
    nh = local // HEAD_DIM
    padded = -(-frames // BLOCK) * BLOCK
    colors = 2 if rows % 32 == 0 else 1
    half = rows // colors
    packed = -(-(nh * 192) // 128) * 128
    nb = cube.size
    steps = len(cube.all_bits) + len(powers(nz))
    token_names, bias_names = ("x", "cot"), ("bq", "bv", "bf1")
    weight_names = ("wq", "wk", "wv", "wo", "w1", "w2")
    share_names = tuple(f"share{i}" for i in range(len(shares)))
    names = token_names + share_names + bias_names + weight_names
    parts = nh * (padded // BLOCK)
    ins = dict(zip(names, (*tokens, *shares, *biases, *weights)))
    outs = dict(
        ototal=((padded, width), BF16),
        igrad=((padded, width), F32),
        ovec=((16, width), F32),
        owq=((rows, local), F32),
        owk=((rows, local), F32),
        owv=((rows, local), F32),
        owo=((local, rows), F32),
        ow1=((rows, hidden), F32),
        ow2=((rows, hidden), F32),
    )
    flat = (padded, width)
    scratch = dict(
        gk=((nb, colors, half, nh * 128), BF16),
        gq=((nb, colors, half, packed - nh * 128), BF16),
        go=((nz, nb, colors, half, local), BF16),
        g1=((nb, colors, half, hidden), BF16),
        g2=((nb, colors, half, hidden), BF16),
        gv=((nb, 8, 128), F32),
        vec=((8, width), F32),
        bias=((8, packed), F32),
        mid=(flat, F32),
        n1=(flat, BF16),
        q=((nh, padded, 128), BF16),
        kv=((2, nh, padded, 128), BF16),
        kvt=((2, nh, 128, padded), BF16),
        vo=((2, nh, padded, 128), BF16),
        p=((nh, padded, 2 * padded), BF16),
        il=((nh, padded, 128), F32),
        atto=((nh, padded, 128), BF16),
        attz=((nz, parts, BLOCK // 2, 128), BF16),
        xp=(flat, BF16),
        gp=(flat, BF16),
        xh2=(flat, F32),
        r2=((padded, 128), F32),
        n2=(flat, BF16),
        act=((padded, hidden), BF16),
        gpre=((padded, hidden), BF16),
        acc=((8, 8, width), F32),
        vs=((8, width), F32),
        vo_=((steps, 8, width), F32),
        vr=((steps, 8, width), F32),
        part=(flat, BF16),
        landed=(flat, BF16),
        crossed=(flat, BF16),
        crossed_one=(flat, BF16),
        total=(flat, BF16),
        opart=(flat, BF16),
        olanded=(flat, BF16),
        ocrossed=(flat, BF16),
        at=((padded, local), BF16),
        qt=((nh, 128, padded), BF16),
        dat=((nh, 128, padded), BF16),
        dkv=((2, nh, 128, padded), F32),
        kvs=((nh, 128, padded), BF16),
        kvr=((nh, 128, padded), BF16),
        ds=((BLOCK, 2 * padded), BF16),
        dw1=((width, hidden), BF16),
        dl1=((colors, nb - 1, half, hidden), BF16),
        dw2=((width, hidden), BF16),
        dl2=((colors, nb - 1, half, hidden), BF16),
        dwo=((width, local), BF16),
        dlo=((colors, nb - 1, half, local), BF16),
        dwq=((width, packed), BF16),
        dlq=((colors, nb - 1, half, packed), BF16),
    )
    small, large = padded // CHUNK, 6
    sums = 3 * small + 2 * large
    lines = sums + Line.count(nz, parts)
    count = lines + (9 * colors + 1) * (nb - 1) + (nz - 1) + 2 * nh + steps

    def body(*refs):
        far_in, far_out = refs[: len(ins)], refs[len(ins) : len(ins) + len(outs)]
        names = list(ins) + list(outs) + list(scratch)
        refs = refs[len(ins) + len(outs) :]
        m = types.SimpleNamespace(**dict(zip(names, refs)))
        send, recv, move = refs[len(names) :]
        m.load = {
            name: pltpu.make_async_copy(far, getattr(m, name), move.at[i])
            for i, (name, far) in enumerate(zip(ins, far_in))
        }
        m.save = {
            name: pltpu.make_async_copy(getattr(m, name), far, move.at[len(ins) + i])
            for i, (name, far) in enumerate(zip(outs, far_out))
        }
        m.first_loads = share_names + ("wk", "wv", "wq")
        m.next_loads = ("wo", "w1", "w2", "x", *bias_names)
        for name in (*m.first_loads, *m.next_loads, "cot"):
            m.load[name].start()
        m.shares = [getattr(m, name) for name in share_names]
        sems = Sems(send, recv)
        sems.used = lines
        sum_two = LineSum(nz, send, recv, 0, small, small, CHUNK, m.part, m.landed, m.crossed, m.total)
        sum_one = LineSum(nz, send, recv, 0, 2 * small, small, CHUNK, m.part, m.landed, m.crossed_one, m.total)
        sum_out = LineSum(
            nz, send, recv, 3 * small, 3 * small + large, large, padded // large, m.opart, m.olanded, m.ocrossed, m.ototal
        )
        line = Line(nz, send, recv, sums, lambda origin, part: m.attz.at[origin, part], parts)
        stage_one(m, cube, nz, sems, line)
        stage_two(m, cube, nz, sum_two, sum_out)
        stage_three(m, cube, nz, sems, sum_two, sum_out, sum_one)
        assert sems.used == count, (sems.used, count)
        for copy in m.save.values():
            copy.wait()

    res = pl.pallas_call(
        body,
        out_shape=[jax.ShapeDtypeStruct(*v) for v in outs.values()],
        in_specs=[pl.BlockSpec(memory_space=pl.ANY)] * len(ins),
        out_specs=[pl.BlockSpec(memory_space=pl.ANY)] * len(outs),
        scratch_shapes=[pltpu.VMEM(a.shape, a.dtype) for a in ins.values()]
        + [pltpu.VMEM(*v) for v in (outs | scratch).values()]
        + [pltpu.SemaphoreType.DMA((count,))] * 2
        + [pltpu.SemaphoreType.DMA((len(ins) + len(outs),))],
        compiler_params=pltpu.CompilerParams(
            collective_id=0, has_side_effects=True, vmem_limit_bytes=67_043_328
        ),
        name="layer",
    )(*ins.values())
    return types.SimpleNamespace(**dict(zip(outs, res)))


def finish(res, frames):
    padded, width = res.ototal.shape
    rows, local = res.owq.shape
    hidden = res.ow1.shape[1]
    tile = 256
    sizes = [rows] * 6 + [local] * 2
    passed = (res.owq, res.owk, res.owv, res.owo, res.ow1, res.ow2)
    n = len(passed)

    def body(out_far, grad_far, vec_far, *refs):
        far, (to_out, to_grad, *to) = refs[:n], refs[n : 2 * n + 2 + 9]
        out_near, grad_near, vec_near, *near = refs[2 * n + 11 : 3 * n + 14]
        grad_flat, *flat = refs[3 * n + 14 : -1]
        sem = refs[-1]
        copy = lambda i, a, b: pltpu.make_async_copy(a, b, sem.at[i])
        pieces = [(t, min(tile, padded - t)) for t in range(0, padded, tile)]
        loads = [
            copy(i, grad_far.at[pl.ds(t, size)], grad_near.at[pl.ds(t, size)]) for i, (t, size) in enumerate(pieces)
        ]
        k = len(pieces)
        others = [copy(k + i, a, b) for i, (a, b) in enumerate(zip((vec_far, out_far, *far), (vec_near, out_near, *near)))]
        for c in loads + others:
            c.start()
        k += len(others)
        saves = []

        def save(a, b):
            saves.append(copy(k + len(saves), a, b))
            saves[-1].start()

        for c, (t, size) in zip(loads, pieces):
            c.wait()
            size = min(size, frames - t)
            grad_flat[t : t + size, 0, :] = grad_near[t : t + size]
            save(grad_flat.at[pl.ds(t, size)], to_grad.at[pl.ds(t, size)])
        others[0].wait()
        for i in range(8):
            flat[i][...] = vec_near[i : i + 1, : sizes[i]]
        for i in range(hidden // 128):
            flat[8][i : i + 1, :] = vec_near[8:9, i * 128 : (i + 1) * 128]
        others[1].wait()
        flat[9][...] = out_near[0:frames]
        save(flat[9], to_out)
        for i in range(9):
            save(flat[i], to[n + i])
        for c, a, b in zip(others[2:], near, to):
            c.wait()
            save(a, b)
        for c in saves:
            c.wait()

    vectors = [jax.ShapeDtypeStruct((1, size), F32) for size in sizes]
    vectors.append(jax.ShapeDtypeStruct((hidden // 128, 128), F32))
    kept = [jax.ShapeDtypeStruct(a.shape, a.dtype) for a in passed]
    final = jax.ShapeDtypeStruct((frames, width), BF16)
    grads = jax.ShapeDtypeStruct((frames, 1, width), F32)
    given = (res.ototal, res.igrad, res.ovec, *passed)
    near = [*given, grads, *vectors, final]
    return pl.pallas_call(
        body,
        out_shape=[final, grads, *kept, *vectors],
        in_specs=[pl.BlockSpec(memory_space=pl.ANY)] * len(given),
        out_specs=[pl.BlockSpec(memory_space=pl.ANY)] * (2 + n + 9),
        scratch_shapes=[pltpu.VMEM(a.shape, a.dtype) for a in near] + [pltpu.SemaphoreType.DMA((-(-padded // tile) * 2 + 2 * n + 12,))],
        compiler_params=pltpu.CompilerParams(vmem_limit_bytes=67_043_328),
        name="finish",
    )(*given)


def on_device(
    inputs,
    gain_one,
    shift_one,
    w_query,
    b_query,
    w_key,
    w_value,
    b_value,
    w_out,
    b_out,
    gain_two,
    shift_two,
    w_fc_one,
    b_fc_one,
    w_fc_two,
    b_fc_two,
    cotangent,
    mesh_shape,
):
    clips, frames, width = inputs.shape
    count = clips * frames
    row = lambda v: v.reshape(1, -1)
    res = layer(
        (inputs.reshape(count, width), cotangent.reshape(count, width)),
        tuple(row(v) for v in (gain_one, shift_one, gain_two, shift_two, b_out, b_fc_two)),
        (b_query, b_value, b_fc_one),
        (w_query, w_key, w_value, w_out, w_fc_one, w_fc_two.T),
        mesh_shape,
    )
    outputs, grad, g_query, g_key, g_value, g_out, g_one, g_two, *vectors = finish(res, count)
    g1, s1, b_o, g2, s2, b_two, b_q, b_v, b_one = (v.reshape(-1) for v in vectors)
    return (
        outputs.reshape(clips, frames, width),
        grad.transpose(1, 0, 2).reshape(clips, frames, width),
        g1,
        s1,
        g_query,
        b_q,
        g_key,
        g_value,
        b_v,
        g_out,
        b_o,
        g2,
        s2,
        g_one,
        b_one,
        g_two.T,
        b_two,
    )


def solution(mesh):
    group = ("clip", "seq")
    rows, columns, own, heads = P(group, "head"), P("head", group), P(group), P("head")
    tokens = P("clip", "seq", None)
    return jax.shard_map(
        partial(on_device, mesh_shape=dict(mesh.shape)),
        mesh=mesh,
        in_specs=(
            tokens, own, own, rows, heads, rows, rows, heads, columns,
            own, own, own, rows, heads, columns, own, tokens,
        ),
        out_specs=(
            tokens, tokens, own, own, rows, heads, rows, rows, heads,
            columns, own, own, own, rows, heads, columns, own,
        ),
        check_vma=False,
    )
```

```python
from functools import partial
import types

import jax
import jax.numpy as jnp
from jax import lax
from jax.experimental import pallas as pl
from jax.experimental.pallas import tpu as pltpu
from jax.sharding import PartitionSpec as P

HEAD_DIM = 64
EPS = 1e-05
F32 = jnp.float32
BF16 = jnp.bfloat16
MESH = pl.DeviceIdType.MESH


def flip(value, bit):
    return value + bit * (1 - 2 * lax.rem(lax.div(value, bit), 2))


def flips(value, mask, bits):
    for bit in bits:
        if mask & bit:
            value = flip(value, bit)
    return value


def powers(size):
    bits, bit = [], 1
    while bit < size:
        bits.append(bit)
        bit *= 2
    return bits


class Cube:
    def __init__(self, clips, seqs):
        self.clips, self.seqs, self.size = clips, seqs, clips * seqs
        self.seq_bits = [(bit, "seq", bit) for bit in powers(seqs)]
        self.clip_bits = [(bit * seqs, "clip", bit) for bit in powers(clips)]
        core, rest = self.clip_bits[:1], self.clip_bits[1:]
        self.orders = (
            self.seq_bits + rest + core,
            rest[:1] + self.seq_bits + rest[1:] + core,
        )
        self.all_bits = [bit for bit, _, _ in self.seq_bits + self.clip_bits]

    def rank(self):
        return lax.axis_index("clip") * self.seqs + lax.axis_index("seq")

    def block(self, mask):
        return flips(self.rank(), mask, self.all_bits)

    @staticmethod
    def peer(step):
        _, axis, bit = step
        return {axis: flip(lax.axis_index(axis), bit)}


class Sems:
    def __init__(self, send, recv):
        self.send, self.recv, self.used = send, recv, 0

    def take(self):
        self.used += 1
        return self.send.at[self.used - 1], self.recv.at[self.used - 1]


def remote(src, dst, sems, device):
    return pltpu.make_async_remote_copy(
        src_ref=src,
        dst_ref=dst,
        send_sem=sems[0],
        recv_sem=sems[1],
        device_id=device,
        device_id_type=MESH,
    )


class Gather:
    def __init__(self, cube, sems, view, colors):
        self.cube, self.view, self.colors = cube, view, colors
        self.steps = len(cube.orders[0])
        self.copies = [[[] for _ in range(self.steps)] for _ in range(colors)]
        for color in range(colors):
            masks = [0]
            for k, step in enumerate(cube.orders[color]):
                for mask in masks:
                    block = cube.block(mask)
                    piece = view(block, color)
                    self.copies[color][k].append(
                        remote(piece, piece, sems.take(), cube.peer(step))
                    )
                masks = masks + [mask ^ step[0] for mask in masks]

    def start(self, k, color):
        for copy in self.copies[color][k]:
            copy.start()

    def advance(self, k, color):
        for copy in self.copies[color][k]:
            copy.wait_recv()
        if k + 1 < self.steps:
            self.start(k + 1, color)

    def drain(self):
        for color in range(self.colors):
            for step in self.copies[color]:
                for copy in step:
                    copy.wait_send()


def normalize(rows):
    mean = jnp.mean(rows, axis=-1, keepdims=True)
    centered = rows - mean
    spread = jnp.mean(centered * centered, axis=-1, keepdims=True)
    inverse = lax.rsqrt(spread + EPS)
    return centered * inverse, inverse


def dot(a, b):
    return jnp.dot(a, b, preferred_element_type=F32)


def dot_nt(a, b):
    return lax.dot_general(a, b, (((1,), (1,)), ((), ())), preferred_element_type=F32)


def dot_tn(a, b):
    return lax.dot_general(a, b, (((0,), (0,)), ((), ())), preferred_element_type=F32)


NEG = -1e30
LINE_LAG = 3


def fill(shape, value, dtype=F32):
    return jnp.full(shape, value, dtype)


def lane(shape):
    return lax.broadcasted_iota(jnp.int32, shape, len(shape) - 1)


class Line:
    def __init__(self, nodes, send, recv, base, view, parts):
        self.n, self.z = nodes, lax.axis_index("head")
        self.send_sem, self.recv_sem, self.base = send, recv, base
        self.view, self.parts = view, parts

    @staticmethod
    def count(nodes, parts):
        return 2 * (nodes - 1) * parts

    def moves(self, hop, part):
        z, n = self.z, self.n

        def copy(origin, way, target):
            piece = self.view(origin, part)
            place = self.base + (way * (n - 1) + hop) * self.parts + part
            sems = self.send_sem.at[place], self.recv_sem.at[place]
            return remote(piece, piece, sems, {"head": target})

        sends = (
            ((z >= hop) & (z < n - 1), lambda: copy(z - hop, 0, z + 1)),
            ((n - 1 - z >= hop) & (z > 0), lambda: copy(z + hop, 1, z - 1)),
        )
        arrivals = (
            (z > hop, lambda: copy(z - 1 - hop, 0, z - 1)),
            (n - 1 - z > hop, lambda: copy(z + 1 + hop, 1, z + 1)),
        )
        return sends, arrivals

    def start(self, hop, part):
        for condition, copy in self.moves(hop, part)[0]:
            pl.when(condition)(lambda copy=copy: copy().start())

    def arrive(self, hop, part):
        for condition, copy in self.moves(hop, part)[1]:
            pl.when(condition)(lambda copy=copy: copy().wait_recv())

    def pump(self, step):
        @pl.when(step < self.parts)
        def _():
            self.start(0, step)

        for hop in range(self.n - 1):
            part = step - LINE_LAG * (hop + 1)

            @pl.when((part >= 0) & (part < self.parts))
            def _(hop=hop, part=part):
                self.arrive(hop, part)
                if hop + 1 < self.n - 1:
                    self.start(hop + 1, part)

    def drain(self, part):
        for hop in range(self.n - 1):
            for condition, copy in self.moves(hop, part)[0]:
                pl.when(condition)(lambda copy=copy: copy().wait_send())


def entry_peers(cube, heads):
    z = lax.axis_index("head")
    peers = [cube.peer(step) for step in cube.orders[0]]
    return peers + [{"head": lax.rem(z + d, heads)} for d in range(1, heads)]


def greet(peers):
    for peer in peers:
        pl.semaphore_signal(pltpu.get_barrier_semaphore(), inc=1, device_id=peer, device_id_type=MESH)


def stage_one(m, cube, nz, sems, line):
    z = lax.axis_index("head")
    r = cube.rank()
    rows = m.wq.shape[0]
    colors = m.gq.shape[1]
    half = rows // colors
    nh = m.q.shape[0]
    frames = m.x.shape[0]
    padded = m.xp.shape[0]
    tile = 128
    tiles = padded // tile
    width = m.x.shape[1]

    peers = entry_peers(cube, nz)
    greet(peers)
    gk = Gather(cube, sems, lambda b, c: m.gk.at[b, c], colors)
    gq = Gather(cube, sems, lambda b, c: m.gq.at[b, c], colors)
    gv = Gather(cube, sems, lambda b, c: m.gv.at[b], 1)
    g1 = Gather(cube, sems, lambda b, c: m.g1.at[b, c], colors)
    g2 = Gather(cube, sems, lambda b, c: m.g2.at[b, c], colors)
    go = Gather(cube, sems, lambda b, c: m.go.at[:, b, c], colors)

    m.vec[...] = fill(m.vec.shape, 0)
    for name in m.first_loads:
        m.load[name].wait()
    for row, ref in enumerate(m.shares):
        m.vec[row : row + 1, :rows] = ref[...].astype(F32)
    m.gv[r] = m.vec[:, :128]
    for c in range(colors):
        part = pl.ds(c * half, half)
        for h in range(nh):
            cols = slice(h * HEAD_DIM, (h + 1) * HEAD_DIM)
            m.gk[r, c, :, h * 128 : h * 128 + 64] = m.wk[part, cols]
            m.gk[r, c, :, h * 128 + 64 : (h + 1) * 128] = m.wv[part, cols]
        m.gq[r, c, :, : nh * 64] = m.wq[part, :]
        spare = m.gq.shape[3] - nh * 64
        if spare:
            m.gq[r, c, :, nh * 64 :] = fill((half, spare), 0, BF16)

    pl.semaphore_wait(pltpu.get_barrier_semaphore(), len(peers))
    gv.start(0, 0)
    for g in (gk, gq):
        for c in range(colors):
            g.start(0, c)

    for name in m.next_loads:
        m.load[name].wait()
    wot = m.wo[...].T
    for c in range(colors):
        part = slice(c * half, (c + 1) * half)
        m.go[z, r, c] = wot[part]
        m.g2[r, c] = m.w2[part, :]
        m.g1[r, c] = m.w1[part, :]
    out_sems = [sems.take() for _ in range(nz - 1)]

    def out_copies(arriving):
        for d in range(1, nz):
            origin = lax.rem(z + nz - d, nz) if arriving else z
            target = lax.rem(z + d, nz)
            piece = m.go.at[origin, r]
            yield remote(piece, piece, out_sems[d - 1], {"head": target})

    for copy in out_copies(False):
        copy.start()
    m.xp[0:frames] = m.x[...]
    m.xp[frames:padded] = fill((padded - frames, width), 0, BF16)

    def norm_tile(i, carry):
        at = pl.ds(pl.multiple_of(i * tile, tile), tile)
        xhat, _ = normalize(m.xp[at].astype(F32))
        m.xh2[at] = xhat
        return carry

    third = tiles // gq.steps
    for k in range(gq.steps):
        top = tiles if k == gq.steps - 1 else third * (k + 1)
        lax.fori_loop(third * k, top, norm_tile, 0)
        gv.advance(k, 0)
        for c in range(colors):
            gk.advance(k, c)
        if k < gq.steps - 1:
            for c in range(colors):
                gq.advance(k, c)
        if k == 0:
            for g in (g1, g2):
                for c in range(colors):
                    g.start(0, c)
    for b in range(cube.size):
        m.vec[:, b * rows : (b + 1) * rows] = m.gv[b, :, :rows]
    gain, shift = m.vec[0:1, :], m.vec[1:2, :]
    m.bias[...] = fill(m.bias.shape, 0)
    bv = m.bv[...].astype(F32)[None, :]
    for h in range(nh):
        m.bias[0:1, h * 128 + 64 : (h + 1) * 128] = bv[:, h * HEAD_DIM : (h + 1) * HEAD_DIM]
    m.bias[1:2, : nh * 64] = m.bq[...].astype(F32)[None, :]
    scale = HEAD_DIM**-0.5

    def project(i, carry):
        at = pl.ds(pl.multiple_of(i * tile, tile), tile)
        n1 = (m.xh2[at] * gain + shift).astype(BF16)
        m.n1[at] = n1
        packed = dot(n1, m.gk[...].reshape(cube.size * rows, nh * 128)) + m.bias[0:1, : nh * 128]
        for h in range(nh):
            m.kv[0, h, at] = packed[:, h * 128 : (h + 1) * 128].astype(BF16)
        return carry

    lax.fori_loop(0, tiles, project, 0)

    kv_sems = [sems.take() for _ in range(nh)]
    other = {"seq": flip(lax.axis_index("seq"), 1)}
    kv_copies = [
        remote(m.kv.at[0, h], m.kv.at[1, h], kv_sems[h], other) for h in range(nh)
    ]
    kv_copies[0].start()
    for copy in out_copies(True):
        copy.wait_recv()
    for c in range(colors):
        go.start(0, c)
    for copy in kv_copies[1:]:
        copy.start()
    for c in range(colors):
        gq.advance(gq.steps - 1, c)

    def project_query(i, carry):
        at = pl.ds(pl.multiple_of(i * tile, tile), tile)
        wide = m.gq.shape[3]
        packed = dot(m.n1[at], m.gq[...].reshape(cube.size * rows, wide)) + m.bias[1:2, :wide]
        left = lane((tile, 128)) < 64
        for h in range(nh):
            pair = packed[:, (h // 2) * 128 : (h // 2) * 128 + 128]
            if h % 2:
                pair = pltpu.roll(pair, 64, 1)
            pair = pair.astype(BF16).astype(F32) * scale
            m.q[h, at] = jnp.where(left, pair, 0.0).astype(BF16)
        return carry

    lax.fori_loop(0, tiles, project_query, 0)

    left = lane((padded, 128)) < 64

    def prepare(part, h):
        block = m.kv[part, h]
        m.kvt[part, h] = block.T
        m.vo[part, h] = jnp.where(left, jnp.ones_like(block), block)

    for h in range(nh):
        prepare(0, h)

    block = 256
    valid = frames - (padded - 128)

    def attend(h):
        def one(b, carry):
            at = pl.ds(pl.multiple_of(b * block, block), block)
            query = m.q[h, at]
            keep = lane((block, 128)) < valid
            parts = []
            top = None
            for part in range(2):
                s = dot(query, m.kvt[part, h])
                body, tail = s[:, : padded - 128], s[:, padded - 128 :]
                tail = jnp.where(keep, tail, NEG)
                parts += [body, tail]
                high = jnp.maximum(jnp.max(body, axis=1, keepdims=True), jnp.max(tail, axis=1, keepdims=True))
                top = high if top is None else jnp.maximum(top, high)
            place = 0
            for s in parts:
                m.p[h, at, place : place + s.shape[1]] = jnp.exp(s - top).astype(BF16)
                place += s.shape[1]
            acc = dot(m.p[h, at, :padded], m.vo[0, h]) + dot(m.p[h, at, padded:], m.vo[1, h])
            inverse = 1.0 / pltpu.roll(acc, 64, 1)
            att = acc * inverse
            right = lane((block, 128)) >= 64
            m.il[h, at] = jnp.where(right, inverse, 0.0)
            m.atto[h, at] = jnp.where(right, att, 0.0).astype(BF16)
            turned = pltpu.roll(att, 64, 1)
            pieces = [
                jnp.where(right[:64], att[g + 64 : g + 128], turned[g : g + 64])
                for g in range(0, block, 128)
            ]
            part = h * (padded // block) + b
            m.attz[z, part] = jnp.concatenate(pieces, axis=0).astype(BF16)
            line.pump(part)
            return carry

        lax.fori_loop(0, padded // block, one, 0)

    def weights(gathers, k, c):
        if c < colors and k < g1.steps - 1:
            for g in gathers:
                g.advance(k, c)

    feed = (g1, g2)
    plan = {0: ((feed, 0, 0), (feed, 0, 1)), 1: (((go,), 0, 0), ((go,), 0, 1))}
    plan[nh - 1] = ((feed, 1, 0),)
    for h in range(nh):
        kv_copies[h].wait_recv()
        prepare(1, h)
        attend(h)
        for job in plan.get(h, ()):
            weights(*job)
    parts = line.parts
    stop = parts + LINE_LAG * (nz - 1)
    loop(parts, parts + 3, line.pump)
    weights((go,), 1, 0)
    weights(feed, 1, 1)
    loop(parts + 3, stop - 2, line.pump)
    weights((go,), 1, 1)
    loop(stop - 2, stop, line.pump)
    for k in range(2, g1.steps):
        for g in (go, g1, g2):
            for c in range(colors):
                g.advance(k, c)

    for copy in kv_copies:
        copy.wait_send()
    for copy in out_copies(False):
        copy.wait_send()
    for g in (gv, gk, gq, g1, g2, go):
        g.drain()
    loop(0, line.parts, line.drain)


class Scatter:
    def __init__(self, cube, sems, buffer, landing, rows, colors):
        self.cube, self.buffer, self.landing = cube, buffer, landing
        self.rows, self.colors, self.half = rows, colors, rows // colors
        self.steps = len(cube.orders[0])
        self.plan = [[[] for _ in range(self.steps)] for _ in range(colors)]
        for color in range(colors):
            masks, slot = [0], 0
            for k, step in enumerate(cube.orders[color]):
                for mask in masks:
                    copy = remote(
                        self.view(cube.block(mask ^ step[0]), color),
                        landing.at[color, slot],
                        sems.take(),
                        cube.peer(step),
                    )
                    self.plan[color][k].append((mask, slot, copy))
                    slot += 1
                masks = masks + [mask ^ step[0] for mask in masks]

    def view(self, block, color):
        start = block * self.rows + color * self.half
        return self.buffer.at[pl.ds(pl.multiple_of(start, 8), self.half)]

    def start(self):
        self.left = self.steps - 1
        self.send(self.left)

    def step(self):
        if self.left > 0:
            self.advance(self.left)
            self.left -= 1

    def send(self, k):
        for color in range(self.colors):
            for _, _, copy in self.plan[color][k]:
                copy.start()

    def advance(self, k):
        for color in range(self.colors):
            for mask, slot, copy in self.plan[color][k]:
                copy.wait_recv()
                view = self.view(self.cube.block(mask), color)
                total = view[...].astype(F32) + self.landing[color, slot].astype(F32)
                view[...] = total.astype(BF16)
            for _, _, copy in self.plan[color][k - 1]:
                copy.start()

    def finish(self):
        while self.left > 0:
            self.step()
        parts = []
        for color in range(self.colors):
            ((_, slot, copy),) = self.plan[color][0]
            copy.wait_recv()
            view = self.view(self.cube.block(0), color)
            parts.append(view[...].astype(F32) + self.landing[color, slot].astype(F32))
        return parts[0] if len(parts) == 1 else jnp.concatenate(parts, axis=0)

    def drain(self):
        for color in range(self.colors):
            for step in self.plan[color]:
                for _, _, copy in step:
                    copy.wait_send()


class LineSum:
    def __init__(self, nz, send, recv, ends, middle, chunks, rows, part, landed, crossed, total):
        z = lax.axis_index("head")
        self.inner = (z > 0) & (z < nz - 1)
        self.mate, self.cross = {"head": flip(z, 1)}, {"head": nz - 1 - z}
        self.send_sem, self.recv_sem, self.bases = send, recv, (ends, middle, ends)
        self.chunks, self.rows = chunks, rows
        self.part, self.landed, self.crossed, self.total = part, landed, crossed, total

    def at(self, ref, i):
        return ref.at[pl.ds(pl.multiple_of(i * self.rows, self.rows), self.rows)]

    def sems(self, kind, i):
        place = self.bases[kind] + i
        return self.send_sem.at[place], self.recv_sem.at[place]

    def first(self, i):
        return remote(self.at(self.part, i), self.at(self.landed, i), self.sems(0, i), self.mate)

    def second(self, i):
        return remote(self.at(self.part, i), self.at(self.crossed, i), self.sems(1, i), self.cross)

    def third(self, i):
        piece = self.at(self.total, i)
        return remote(piece, piece, self.sems(2, i), self.mate)

    def offer(self, i):
        @pl.when(jnp.logical_not(self.inner))
        def _():
            self.first(i).start()

    def relay(self, i):
        @pl.when(self.inner)
        def _():
            self.first(i).wait_recv()
            view = self.at(self.part, i)
            total = view[...].astype(F32) + self.at(self.landed, i)[...].astype(F32)
            view[...] = total.astype(BF16)
            self.second(i).start()

    def pump(self, i):
        @pl.when(i < self.chunks)
        def _():
            self.relay(i)

        @pl.when(i >= LAG)
        def _():
            self.close(i - LAG)

    def step(self, i, lag):
        if i < self.chunks:
            self.relay(i)
        if i >= lag:
            self.close(i - lag)

    def close(self, i):
        @pl.when(self.inner)
        def _():
            self.second(i).wait_recv()
            total = self.at(self.part, i)[...].astype(F32) + self.at(self.crossed, i)[...].astype(F32)
            self.at(self.total, i)[...] = total.astype(BF16)
            self.third(i).start()

    def accept(self, i):
        @pl.when(jnp.logical_not(self.inner))
        def _():
            self.third(i).wait_recv()

    def drain(self, i):
        @pl.when(self.inner)
        def _():
            self.second(i).wait_send()
            self.third(i).wait_send()

        @pl.when(jnp.logical_not(self.inner))
        def _():
            self.first(i).wait_send()


def loop(start, stop, step):
    lax.fori_loop(start, stop, lambda i, carry: (step(i), carry)[1], 0)


def rows_of(i, size):
    return pl.ds(pl.multiple_of(i * size, size), size)


def add_rows(m, row, values):
    count, width = values.shape
    m.acc[row, :, :width] += jnp.sum(values.reshape(count // 8, 8, width), axis=0)


B_FC_TWO, GAIN_TWO, SHIFT_TWO, B_OUT, GAIN_ONE, SHIFT_ONE, B_QKV, B_FC_ONE = range(8)
BLOCK = 256
STEP = 128
CHUNK = 32
LAG = 4
OUT_LAG = 3


def stage_two(m, cube, nz, sum_two, sum_out):
    padded, width = m.xp.shape
    rows = m.wq.shape[0]
    nh = m.q.shape[0]
    frames = m.cot.shape[0]
    hidden = m.w1.shape[1]
    m.load["cot"].wait()
    m.gp[0:frames] = m.cot[...]
    m.gp[frames:padded] = fill((padded - frames, width), 0, BF16)
    m.acc[...] = fill(m.acc.shape, 0)
    gain, shift, b_out = m.vec[2:3, :], m.vec[3:4, :], m.vec[4:5, :]
    b_one = m.bf1[...].astype(F32)[None, :]
    per = STEP // CHUNK
    w_one = lambda: m.g1[...].reshape(cube.size * rows, hidden)
    w_two = lambda: m.g2[...].reshape(cube.size * rows, hidden)

    def block(b):
        at = rows_of(b, STEP)
        packed = rows_of(lax.rem(b, 2), STEP // 2)
        mid = m.xp[at].astype(F32) + b_out
        for zz in range(nz):
            pieces = [m.attz[zz, h * (padded // BLOCK) + lax.div(b, 2), packed] for h in range(nh)]
            top = jnp.concatenate([p[:, :64] for p in pieces], axis=1)
            low = jnp.concatenate([p[:, 64:] for p in pieces], axis=1)
            att = jnp.concatenate([top, low], axis=0)
            mid = mid + dot_nt(att, m.go[zz].reshape(cube.size * rows, nh * HEAD_DIM))
        xhat, inverse = normalize(mid)
        m.mid[at] = mid
        m.xh2[at] = xhat
        m.r2[at] = jnp.broadcast_to(inverse, (STEP, 128))
        n2 = (xhat * gain + shift).astype(BF16)
        m.n2[at] = n2
        pre = dot(n2, w_one()) + b_one
        cdf = 0.5 + 0.5 * lax.erf(pre * 0.7071067811865476)
        act = (pre * cdf).astype(BF16)
        m.act[at] = act
        slope = cdf + pre * jnp.exp(pre * pre * -0.5) * 0.3989422804014327
        g = m.gp[at]
        add_rows(m, B_FC_TWO, g.astype(F32))
        gpre = (dot(g, w_two()) * slope).astype(BF16)
        m.gpre[at] = gpre
        add_rows(m, B_FC_ONE, gpre.astype(F32))
        back = dot_nt(gpre, w_one())
        add_rows(m, GAIN_TWO, back * m.xh2[at])
        add_rows(m, SHIFT_TWO, back)
        m.part[at] = back.astype(BF16)
        loop(0, per, lambda j: sum_two.offer(b * per + j))

        @pl.when(b >= 2)
        def _():
            sum_two.pump(2 * b - 4)
            sum_two.pump(2 * b - 3)

        m.opart[at] = dot_nt(m.act[at], w_two()).astype(BF16)

    loop(0, padded // STEP, block)
    loop(0, sum_out.chunks, sum_out.offer)


def stage_three(m, cube, nz, sems, sum_two, sum_out, sum_one):
    z = lax.axis_index("head")
    padded, width = m.xp.shape
    rows = m.wq.shape[0]
    nh = m.q.shape[0]
    local = nh * HEAD_DIM
    colors = m.gq.shape[1]
    chunks = padded // CHUNK
    blocks = padded // BLOCK
    per = STEP // CHUNK
    scale = HEAD_DIM**-0.5
    packed = m.gk.shape[3] + m.gq.shape[3]
    s1 = Scatter(cube, sems, m.dw1, m.dl1, rows, colors)
    s2 = Scatter(cube, sems, m.dw2, m.dl2, rows, colors)
    so = Scatter(cube, sems, m.dwo, m.dlo, rows, colors)
    sq = Scatter(cube, sems, m.dwq, m.dlq, rows, colors)
    tile = 128
    tiles = width // tile

    def product(left, right, into, columns):
        def one(i):
            cols = pl.ds(pl.multiple_of(i * tile, tile), tile)
            into[rows_of(i, tile)] = dot_tn(left[:, cols], right())[:, :columns].astype(BF16)

        return one

    one = product(m.n2, lambda: m.gpre[...], m.dw1, m.dw1.shape[1])
    two = product(m.gp, lambda: m.act[...], m.dw2, m.dw2.shape[1])

    def first(i):
        one(i)
        sum_two.pump(early + i)

    def second(i):
        two(i)
        sum_two.pump(early + tiles + i)

    early = 2 * (padded // STEP - 2)

    loop(0, tiles, first)
    s1.start()
    loop(0, tiles, second)
    s2.start()
    for h in range(nh):
        m.qt[h] = m.q[h].T
    gain_two = m.vec[2:3, :]

    def middle(i):
        sum_two.accept(i)
        at = rows_of(i, CHUNK)
        n = m.total[at].astype(F32)
        e = n * gain_two
        xhat = m.xh2[at]
        r = m.r2[at][:, :1]
        mean = jnp.mean(e, axis=-1, keepdims=True)
        along = jnp.mean(e * xhat, axis=-1, keepdims=True)
        grad = m.gp[at].astype(F32) + r * (e - mean - xhat * along)
        m.xh2[at] = grad
        add_rows(m, B_OUT, grad)
        low = grad.astype(BF16)
        m.n2[at] = low
        da = dot(low, m.go[z].reshape(cube.size * rows, local)).astype(BF16).astype(F32)
        right = lane((CHUNK, 128)) >= 64
        for h in range(nh):
            base = (h // 2) * 128
            wide = da[:, base : min(base + 128, local)]
            if wide.shape[1] < 128:
                wide = jnp.concatenate([wide, jnp.zeros((CHUNK, 128 - wide.shape[1]), F32)], axis=1)
            if h % 2 == 0:
                wide = pltpu.roll(wide, 64, 1)
            m.act[at, h * 128 : (h + 1) * 128] = jnp.where(right, wide * m.il[h, at], 0.0).astype(BF16)
            m.at[at, h * 64 : (h + 1) * 64] = m.atto[h, at][:, 64:]

    ahead = early + 2 * tiles
    stop = chunks + LAG - ahead
    each = chunks // stop

    def pumped(i):
        sum_two.pump(i + ahead)
        loop(i * each, (i + 1) * each, middle)

    s1.step()
    fourth = stop // 4
    for part in range(4):
        loop(part * fourth, stop if part == 3 else (part + 1) * fourth, pumped)
        (s2, s1)[part % 2].step()
    taken = []

    def out_step():
        if len(taken) < sum_out.chunks + OUT_LAG:
            sum_out.step(len(taken), OUT_LAG)
            taken.append(None)

    out_step()
    loop(stop * each, chunks, middle)
    out_step()

    for h in range(nh):
        m.dat[h] = m.act[:, h * 128 : (h + 1) * 128].T
    big = sum_out.chunks
    out_step()
    kv_sems = [sems.take() for _ in range(nh)]
    other = {"seq": flip(lax.axis_index("seq"), 1)}
    kv_copies = [remote(m.kvs.at[h], m.kvr.at[h], kv_sems[h], other) for h in range(nh)]
    for h in range(nh):

        def back(b, h=h):
            at = rows_of(b, BLOCK)
            da = m.act[at, h * 128 : (h + 1) * 128]
            inner = jnp.sum(da.astype(F32) * m.atto[h, at].astype(F32), axis=1, keepdims=True)
            for part in (1, 0):
                keys = slice(part * padded, (part + 1) * padded)
                dp = dot(da, m.kvt[part, h])
                m.ds[at, keys] = (m.p[h, at, keys].astype(F32) * (dp - inner)).astype(BF16)
            dq = dot(m.ds[at, :padded], m.kv[0, h]) + dot(m.ds[at, padded:], m.kv[1, h])
            dq = (dq * scale)[:, :64].astype(BF16)
            m.gpre[at, nh * 128 + h * 64 : nh * 128 + (h + 1) * 64] = dq

        loop(0, blocks, back)
        out_step()
        far, own = slice(padded, 2 * padded), slice(0, padded)
        m.kvs[h] = (dot(m.qt[h], m.ds[:, far]) + dot(m.dat[h], m.p[h, :, far])).astype(BF16)
        kv_copies[h].start()
        m.dkv[h] = dot(m.qt[h], m.ds[:, own]) + dot(m.dat[h], m.p[h, :, own])
        out_step()
    spare = packed - nh * 192
    if spare:
        m.gpre[:, nh * 192 : packed] = fill((padded, spare), 0, BF16)
    for h in range(nh):
        kv_copies[h].wait_recv()
        total = m.dkv[h] + m.kvr[h].astype(F32)
        m.gpre[:, h * 128 : (h + 1) * 128] = total.T.astype(BF16)

    out_step()
    def last(b):
        at = rows_of(b, STEP)
        grads = m.gpre[at, :packed]
        add_rows(m, B_QKV, grads.astype(F32))
        keys = nh * 128
        back = dot_nt(grads[:, :keys], m.gk[...].reshape(cube.size * rows, keys))
        back = back + dot_nt(grads[:, keys:], m.gq[...].reshape(cube.size * rows, packed - keys))
        xhat, _ = normalize(m.xp[at].astype(F32))
        add_rows(m, GAIN_ONE, back * xhat)
        add_rows(m, SHIFT_ONE, back)
        m.part[at] = back.astype(BF16)
        loop(0, per, lambda j: sum_one.offer(b * per + j))

    loop(0, chunks, sum_two.drain)
    loop(0, padded // STEP, last)
    out_step()
    for row in range(8):
        m.vs[row : row + 1, :] = jnp.sum(m.acc[row], axis=0, keepdims=True)
    cube_peers = [cube.peer(step) for step in cube.orders[0]]
    vec_copies = []

    def vec_send(k):
        if k < len(cube_peers):
            m.vo_[k] = m.vs[...]
            vec_copies.append(remote(m.vo_.at[k], m.vr.at[k], sems.take(), cube_peers[k]))
            vec_copies[-1].start()
            return
        m.vo_[k] = m.vs[...]
        for d in range(1, nz):
            target = {"head": lax.rem(z + d, nz)}
            vec_copies.append(remote(m.vo_.at[k], m.vr.at[k + d - 1], sems.take(), target))
            vec_copies[-1].start()

    def vec_take(k):
        if k < len(cube_peers):
            vec_copies[k].wait_recv()
            m.vs[...] += m.vr[k]
            vec_send(k + 1)

    vec_send(0)
    one_q = product(m.n1, lambda: m.gpre[:, :packed], m.dwq, packed)
    one_o = product(m.n2, lambda: m.at[...], m.dwo, local)

    def qkv(i):
        one_q(i)
        sum_one.pump(i)

    def out(i):
        one_o(i)
        sum_one.pump(tiles + i)

    half = tiles // 2
    loop(0, half, qkv)
    out_step()
    loop(half, tiles, qkv)
    sq.start()
    out_step()
    vec_take(0)
    loop(0, half, out)
    out_step()
    loop(half, tiles, out)
    so.start()
    while len(taken) < sum_out.chunks + OUT_LAG:
        out_step()
    vec_take(1)

    b_two = m.vec[5:6, :]

    def output(i):
        sum_out.accept(i)
        at = rows_of(i, sum_out.rows)
        m.ototal[at] = (m.mid[at] + m.ototal[at].astype(F32) + b_two).astype(BF16)

    gain_one = m.vec[0:1, :]

    def final(i):
        sum_one.accept(i)
        at = rows_of(i, CHUNK)
        e = m.total[at].astype(F32) * gain_one
        xhat, r = normalize(m.xp[at].astype(F32))
        mean = jnp.mean(e, axis=-1, keepdims=True)
        along = jnp.mean(e * xhat, axis=-1, keepdims=True)
        m.igrad[at] = m.xh2[at] + r * (e - mean - xhat * along)

    ahead = 2 * tiles
    stop = chunks + LAG - ahead
    turn = 2 * stop - chunks

    def tail(i):
        sum_one.pump(i + ahead)
        final(i)

    def faster(i):
        sum_one.pump(i + ahead)
        final(2 * i - turn)
        final(2 * i - turn + 1)

    def unpack():
        got = sq.finish()
        for h in range(nh):
            cols = slice(h * HEAD_DIM, (h + 1) * HEAD_DIM)
            m.owk[:, cols] = got[:, h * 128 : h * 128 + 64]
            m.owv[:, cols] = got[:, h * 128 + 64 : (h + 1) * 128]
        m.owq[...] = got[:, nh * 128 : nh * 128 + local]
        for name in ("owk", "owv", "owq"):
            m.save[name].start()

    def vectors():
        row_id = lax.broadcasted_iota(jnp.int32, m.vs.shape, 0)
        summed = (row_id == GAIN_TWO) | (row_id == SHIFT_TWO) | (row_id == GAIN_ONE) | (row_id == SHIFT_ONE)
        base = len(cube_peers)
        for d in range(1, nz):
            vec_copies[base + d - 1].wait_recv()
        rest = sum(m.vr[base + d - 1] for d in range(1, nz))
        m.vs[...] += jnp.where(summed, rest, 0.0)
        m.ovec[...] = fill(m.ovec.shape, 0)
        names = (GAIN_ONE, SHIFT_ONE, B_OUT, GAIN_TWO, SHIFT_TWO, B_FC_TWO)
        for b in range(cube.size):

            @pl.when(cube.rank() == b)
            def _(b=b):
                for place, row in enumerate(names):
                    m.ovec[place : place + 1, :rows] = m.vs[row : row + 1, b * rows : (b + 1) * rows]

        m.ovec[6:7, :local] = m.vs[B_QKV : B_QKV + 1, nh * 128 : nh * 192]
        for h in range(nh):
            m.ovec[7:8, h * 64 : (h + 1) * 64] = m.vs[B_QKV : B_QKV + 1, h * 128 + 64 : (h + 1) * 128]
        m.ovec[8:9, :] = m.vs[B_FC_ONE : B_FC_ONE + 1, :]
        m.save["ovec"].start()

    def outputs():
        loop(0, big, sum_out.drain)
        loop(0, big, output)
        m.save["ototal"].start()

    def early():
        m.ow1[...] = s1.finish()
        m.save["ow1"].start()
        m.ow2[...] = s2.finish()
        m.save["ow2"].start()

    def first_job():
        sq.step()

    def second_job():
        for k in range(2, len(cube_peers)):
            vec_take(k)

    def third_job():
        sq.step()
        so.step()

    def sixth_job():
        unpack()
        m.owo[...] = so.finish().T
        m.save["owo"].start()

    def fourth_job():
        outputs()
        so.step()

    jobs = (first_job, second_job, third_job, fourth_job, early, sixth_job)
    near = turn // 3
    ends = [near, 2 * near, turn]
    far = (stop - turn) // 4
    ends += [turn + far, turn + 2 * far, turn + 3 * far, stop]
    begin = 0
    saved = 0
    for place, end in enumerate(ends):
        loop(begin, end, tail if end <= turn else faster)
        begin = end
        done = (end if end <= turn else 2 * end - turn) * CHUNK
        m.save_rows(saved, done - saved).start()
        saved = done
        if place < len(jobs):
            jobs[place]()
    assert saved == padded
    vectors()

    for copy in kv_copies + vec_copies:
        copy.wait_send()
    for s in (s1, s2, so, sq):
        s.drain()
    loop(0, chunks, sum_one.drain)


def layer(tokens, shares, biases, weights, mesh_shape):
    nz = mesh_shape["head"]
    cube = Cube(mesh_shape["clip"], mesh_shape["seq"])
    frames, width = tokens[0].shape
    rows, local = weights[0].shape
    hidden = weights[4].shape[1]
    nh = local // HEAD_DIM
    padded = -(-frames // BLOCK) * BLOCK
    colors = 2 if rows % 32 == 0 else 1
    half = rows // colors
    packed = -(-(nh * 192) // 128) * 128
    nb = cube.size
    steps = len(cube.all_bits) + nz - 1
    token_names, bias_names = ("x", "cot"), ("bq", "bv", "bf1")
    weight_names = ("wq", "wk", "wv", "wo", "w1", "w2")
    share_names = tuple(f"share{i}" for i in range(len(shares)))
    names = token_names + share_names + bias_names + weight_names
    parts = nh * (padded // BLOCK)
    ins = dict(zip(names, (*tokens, *shares, *biases, *weights)))
    outs = dict(
        ototal=((padded, width), BF16),
        igrad=((padded, width), F32),
        ovec=((16, width), F32),
        owq=((rows, local), F32),
        owk=((rows, local), F32),
        owv=((rows, local), F32),
        owo=((local, rows), F32),
        ow1=((rows, hidden), F32),
        ow2=((rows, hidden), F32),
    )
    flat = (padded, width)
    scratch = dict(
        gk=((nb, colors, half, nh * 128), BF16),
        gq=((nb, colors, half, packed - nh * 128), BF16),
        go=((nz, nb, colors, half, local), BF16),
        g1=((nb, colors, half, hidden), BF16),
        g2=((nb, colors, half, hidden), BF16),
        gv=((nb, 8, 128), F32),
        vec=((8, width), F32),
        bias=((8, packed), F32),
        mid=(flat, F32),
        n1=(flat, BF16),
        q=((nh, padded, 128), BF16),
        kv=((2, nh, padded, 128), BF16),
        kvt=((2, nh, 128, padded), BF16),
        vo=((2, nh, padded, 128), BF16),
        p=((nh, padded, 2 * padded), BF16),
        il=((nh, padded, 128), F32),
        atto=((nh, padded, 128), BF16),
        attz=((nz, parts, BLOCK // 2, 128), BF16),
        xp=(flat, BF16),
        gp=(flat, BF16),
        xh2=(flat, F32),
        r2=((padded, 128), F32),
        n2=(flat, BF16),
        act=((padded, hidden), BF16),
        gpre=((padded, hidden), BF16),
        acc=((8, 8, width), F32),
        vs=((8, width), F32),
        vo_=((steps, 8, width), F32),
        vr=((steps, 8, width), F32),
        part=(flat, BF16),
        landed=(flat, BF16),
        crossed=(flat, BF16),
        crossed_one=(flat, BF16),
        total=(flat, BF16),
        opart=(flat, BF16),
        olanded=(flat, BF16),
        ocrossed=(flat, BF16),
        at=((padded, local), BF16),
        qt=((nh, 128, padded), BF16),
        dat=((nh, 128, padded), BF16),
        dkv=((nh, 128, padded), F32),
        kvs=((nh, 128, padded), BF16),
        kvr=((nh, 128, padded), BF16),
        ds=((padded, 2 * padded), BF16),
        dw1=((width, hidden), BF16),
        dl1=((colors, nb - 1, half, hidden), BF16),
        dw2=((width, hidden), BF16),
        dl2=((colors, nb - 1, half, hidden), BF16),
        dwo=((width, local), BF16),
        dlo=((colors, nb - 1, half, local), BF16),
        dwq=((width, packed), BF16),
        dlq=((colors, nb - 1, half, packed), BF16),
    )
    small, large = padded // CHUNK, 12
    sums = 3 * small + 2 * large
    lines = sums + Line.count(nz, parts)
    count = lines + (9 * colors + 1) * (nb - 1) + (nz - 1) + 2 * nh + steps

    def body(*refs):
        far_in, far_out = refs[: len(ins)], refs[len(ins) : len(ins) + len(outs)]
        names = list(ins) + list(outs) + list(scratch)
        refs = refs[len(ins) + len(outs) :]
        m = types.SimpleNamespace(**dict(zip(names, refs)))
        send, recv, move = refs[len(names) :]
        m.load = {
            name: pltpu.make_async_copy(far, getattr(m, name), move.at[i])
            for i, (name, far) in enumerate(zip(ins, far_in))
        }
        m.save = {
            name: pltpu.make_async_copy(getattr(m, name), far, move.at[len(ins) + i])
            for i, (name, far) in enumerate(zip(outs, far_out))
            if name != "igrad"
        }
        rows_far = far_out[list(outs).index("igrad")]

        def save_rows(start, size):
            part = pl.ds(start, size)
            at = len(ins) + len(outs) + len(m.saved)
            m.saved.append(pltpu.make_async_copy(m.igrad.at[part], rows_far.at[part], move.at[at]))
            return m.saved[-1]

        m.saved, m.save_rows = [], save_rows
        m.first_loads = share_names + ("wk", "wv", "wq")
        m.next_loads = ("wo", "w1", "w2", "x", *bias_names)
        for name in (*m.first_loads, *m.next_loads, "cot"):
            m.load[name].start()
        m.shares = [getattr(m, name) for name in share_names]
        sems = Sems(send, recv)
        sems.used = lines
        sum_two = LineSum(nz, send, recv, 0, small, small, CHUNK, m.part, m.landed, m.crossed, m.total)
        sum_one = LineSum(nz, send, recv, 0, 2 * small, small, CHUNK, m.part, m.landed, m.crossed_one, m.total)
        sum_out = LineSum(
            nz, send, recv, 3 * small, 3 * small + large, large, padded // large, m.opart, m.olanded, m.ocrossed, m.ototal
        )
        line = Line(nz, send, recv, sums, lambda origin, part: m.attz.at[origin, part], parts)
        stage_one(m, cube, nz, sems, line)
        stage_two(m, cube, nz, sum_two, sum_out)
        stage_three(m, cube, nz, sems, sum_two, sum_out, sum_one)
        assert sems.used == count, (sems.used, count)
        for copy in (*m.save.values(), *m.saved):
            copy.wait()

    res = pl.pallas_call(
        body,
        out_shape=[jax.ShapeDtypeStruct(*v) for v in outs.values()],
        in_specs=[pl.BlockSpec(memory_space=pl.ANY)] * len(ins),
        out_specs=[pl.BlockSpec(memory_space=pl.ANY)] * len(outs),
        scratch_shapes=[pltpu.VMEM(a.shape, a.dtype) for a in ins.values()]
        + [pltpu.VMEM(*v) for v in (outs | scratch).values()]
        + [pltpu.SemaphoreType.DMA((count,))] * 2
        + [pltpu.SemaphoreType.DMA((len(ins) + len(outs) + 7,))],
        compiler_params=pltpu.CompilerParams(
            collective_id=0, has_side_effects=True, vmem_limit_bytes=67_043_328
        ),
        name="layer",
    )(*ins.values())
    return types.SimpleNamespace(**dict(zip(outs, res)))


def finish(res, frames):
    padded, width = res.ototal.shape
    rows, local = res.owq.shape
    hidden = res.ow1.shape[1]
    tile = 256
    sizes = [rows] * 6 + [local] * 2
    passed = (res.owq, res.owk, res.owv, res.owo, res.ow1, res.ow2)
    n = len(passed)

    def body(out_far, grad_far, vec_far, *refs):
        far, (to_out, to_grad, *to) = refs[:n], refs[n : 2 * n + 2 + 9]
        out_near, grad_near, vec_near, *near = refs[2 * n + 11 : 3 * n + 14]
        grad_flat, *flat = refs[3 * n + 14 : -1]
        sem = refs[-1]
        copy = lambda i, a, b: pltpu.make_async_copy(a, b, sem.at[i])
        pieces = [(t, min(tile, padded - t)) for t in range(0, padded, tile)]
        loads = [
            copy(i, grad_far.at[pl.ds(t, size)], grad_near.at[pl.ds(t, size)]) for i, (t, size) in enumerate(pieces)
        ]
        k = len(pieces)
        others = [copy(k + i, a, b) for i, (a, b) in enumerate(zip((vec_far, out_far, *far), (vec_near, out_near, *near)))]
        for c in loads + others:
            c.start()
        k += len(others)
        saves = []

        def save(a, b):
            saves.append(copy(k + len(saves), a, b))
            saves[-1].start()

        for c, (t, size) in zip(loads, pieces):
            c.wait()
            size = min(size, frames - t)
            grad_flat[t : t + size, 0, :] = grad_near[t : t + size]
            save(grad_flat.at[pl.ds(t, size)], to_grad.at[pl.ds(t, size)])
        others[0].wait()
        for i in range(8):
            flat[i][...] = vec_near[i : i + 1, : sizes[i]]
        for i in range(hidden // 128):
            flat[8][i : i + 1, :] = vec_near[8:9, i * 128 : (i + 1) * 128]
        others[1].wait()
        flat[9][...] = out_near[0:frames]
        save(flat[9], to_out)
        for i in range(9):
            save(flat[i], to[n + i])
        for c, a, b in zip(others[2:], near, to):
            c.wait()
            save(a, b)
        for c in saves:
            c.wait()

    vectors = [jax.ShapeDtypeStruct((1, size), F32) for size in sizes]
    vectors.append(jax.ShapeDtypeStruct((hidden // 128, 128), F32))
    kept = [jax.ShapeDtypeStruct(a.shape, a.dtype) for a in passed]
    final = jax.ShapeDtypeStruct((frames, width), BF16)
    grads = jax.ShapeDtypeStruct((frames, 1, width), F32)
    given = (res.ototal, res.igrad, res.ovec, *passed)
    near = [*given, grads, *vectors, final]
    return pl.pallas_call(
        body,
        out_shape=[final, grads, *kept, *vectors],
        in_specs=[pl.BlockSpec(memory_space=pl.ANY)] * len(given),
        out_specs=[pl.BlockSpec(memory_space=pl.ANY)] * (2 + n + 9),
        scratch_shapes=[pltpu.VMEM(a.shape, a.dtype) for a in near] + [pltpu.SemaphoreType.DMA((-(-padded // tile) * 2 + 2 * n + 12,))],
        compiler_params=pltpu.CompilerParams(vmem_limit_bytes=67_043_328),
        name="finish",
    )(*given)


def on_device(
    inputs,
    gain_one,
    shift_one,
    w_query,
    b_query,
    w_key,
    w_value,
    b_value,
    w_out,
    b_out,
    gain_two,
    shift_two,
    w_fc_one,
    b_fc_one,
    w_fc_two,
    b_fc_two,
    cotangent,
    mesh_shape,
):
    clips, frames, width = inputs.shape
    count = clips * frames
    row = lambda v: v.reshape(1, -1)
    res = layer(
        (inputs.reshape(count, width), cotangent.reshape(count, width)),
        tuple(row(v) for v in (gain_one, shift_one, gain_two, shift_two, b_out, b_fc_two)),
        (b_query, b_value, b_fc_one),
        (w_query, w_key, w_value, w_out, w_fc_one, w_fc_two.T),
        mesh_shape,
    )
    outputs, grad, g_query, g_key, g_value, g_out, g_one, g_two, *vectors = finish(res, count)
    g1, s1, b_o, g2, s2, b_two, b_q, b_v, b_one = (v.reshape(-1) for v in vectors)
    return (
        outputs.reshape(clips, frames, width),
        grad.transpose(1, 0, 2).reshape(clips, frames, width),
        g1,
        s1,
        g_query,
        b_q,
        g_key,
        g_value,
        b_v,
        g_out,
        b_o,
        g2,
        s2,
        g_one,
        b_one,
        g_two.T,
        b_two,
    )


def solution(mesh):
    group = ("clip", "seq")
    rows, columns, own, heads = P(group, "head"), P("head", group), P(group), P("head")
    tokens = P("clip", "seq", None)
    return jax.shard_map(
        partial(on_device, mesh_shape=dict(mesh.shape)),
        mesh=mesh,
        in_specs=(
            tokens, own, own, rows, heads, rows, rows, heads, columns,
            own, own, own, rows, heads, columns, own, tokens,
        ),
        out_specs=(
            tokens, tokens, own, own, rows, heads, rows, rows, heads,
            columns, own, own, own, rows, heads, columns, own,
        ),
        check_vma=False,
    )
```

```python
from functools import partial
import types

import jax
import jax.numpy as jnp
from jax import lax
from jax.experimental import pallas as pl
from jax.experimental.pallas import tpu as pltpu
from jax.sharding import PartitionSpec as P

HEAD_DIM = 64
EPS = 1e-05
F32 = jnp.float32
BF16 = jnp.bfloat16
MESH = pl.DeviceIdType.MESH


def flip(value, bit):
    return value + bit * (1 - 2 * lax.rem(lax.div(value, bit), 2))


def flips(value, mask, bits):
    for bit in bits:
        if mask & bit:
            value = flip(value, bit)
    return value


def powers(size):
    bits, bit = [], 1
    while bit < size:
        bits.append(bit)
        bit *= 2
    return bits


class Cube:
    def __init__(self, clips, seqs):
        self.clips, self.seqs, self.size = clips, seqs, clips * seqs
        self.seq_bits = [(bit, "seq", bit) for bit in powers(seqs)]
        self.clip_bits = [(bit * seqs, "clip", bit) for bit in powers(clips)]
        core, rest = self.clip_bits[:1], self.clip_bits[1:]
        self.orders = (
            self.seq_bits + rest + core,
            rest[:1] + self.seq_bits + rest[1:] + core,
        )
        self.all_bits = [bit for bit, _, _ in self.seq_bits + self.clip_bits]

    def rank(self):
        return lax.axis_index("clip") * self.seqs + lax.axis_index("seq")

    def block(self, mask):
        return flips(self.rank(), mask, self.all_bits)

    @staticmethod
    def peer(step):
        _, axis, bit = step
        return {axis: flip(lax.axis_index(axis), bit)}


class Sems:
    def __init__(self, send, recv):
        self.send, self.recv, self.used = send, recv, 0

    def take(self):
        self.used += 1
        return self.send.at[self.used - 1], self.recv.at[self.used - 1]


def remote(src, dst, sems, device):
    return pltpu.make_async_remote_copy(
        src_ref=src,
        dst_ref=dst,
        send_sem=sems[0],
        recv_sem=sems[1],
        device_id=device,
        device_id_type=MESH,
    )


class Gather:
    def __init__(self, cube, sems, view, colors):
        self.cube, self.view, self.colors = cube, view, colors
        self.steps = len(cube.orders[0])
        self.copies = [[[] for _ in range(self.steps)] for _ in range(colors)]
        for color in range(colors):
            masks = [0]
            for k, step in enumerate(cube.orders[color]):
                for mask in masks:
                    block = cube.block(mask)
                    piece = view(block, color)
                    self.copies[color][k].append(
                        remote(piece, piece, sems.take(), cube.peer(step))
                    )
                masks = masks + [mask ^ step[0] for mask in masks]

    def start(self, k, color):
        for copy in self.copies[color][k]:
            copy.start()

    def advance(self, k, color):
        for copy in self.copies[color][k]:
            copy.wait_recv()
        if k + 1 < self.steps:
            self.start(k + 1, color)

    def drain(self):
        for color in range(self.colors):
            for step in self.copies[color]:
                for copy in step:
                    copy.wait_send()


def normalize(rows):
    mean = jnp.mean(rows, axis=-1, keepdims=True)
    centered = rows - mean
    spread = jnp.mean(centered * centered, axis=-1, keepdims=True)
    inverse = lax.rsqrt(spread + EPS)
    return centered * inverse, inverse


def dot(a, b):
    return jnp.dot(a, b, preferred_element_type=F32)


def dot_nt(a, b):
    return lax.dot_general(a, b, (((1,), (1,)), ((), ())), preferred_element_type=F32)


def dot_tn(a, b):
    return lax.dot_general(a, b, (((0,), (0,)), ((), ())), preferred_element_type=F32)


NEG = -1e30
LINE_LAG = 2


def fill(shape, value, dtype=F32):
    return jnp.full(shape, value, dtype)


def lane(shape):
    return lax.broadcasted_iota(jnp.int32, shape, len(shape) - 1)


class Line:
    def __init__(self, nodes, send, recv, base, view, parts):
        self.n, self.z = nodes, lax.axis_index("head")
        self.send_sem, self.recv_sem, self.base = send, recv, base
        self.view, self.parts = view, parts

    @staticmethod
    def count(nodes, parts):
        return 2 * (nodes - 1) * parts

    def moves(self, hop, part):
        z, n = self.z, self.n

        def copy(origin, way, target):
            piece = self.view(origin, part)
            place = self.base + (way * (n - 1) + hop) * self.parts + part
            sems = self.send_sem.at[place], self.recv_sem.at[place]
            return remote(piece, piece, sems, {"head": target})

        sends = (
            ((z >= hop) & (z < n - 1), lambda: copy(z - hop, 0, z + 1)),
            ((n - 1 - z >= hop) & (z > 0), lambda: copy(z + hop, 1, z - 1)),
        )
        arrivals = (
            (z > hop, lambda: copy(z - 1 - hop, 0, z - 1)),
            (n - 1 - z > hop, lambda: copy(z + 1 + hop, 1, z + 1)),
        )
        return sends, arrivals

    def start(self, hop, part):
        for condition, copy in self.moves(hop, part)[0]:
            pl.when(condition)(lambda copy=copy: copy().start())

    def arrive(self, hop, part):
        for condition, copy in self.moves(hop, part)[1]:
            pl.when(condition)(lambda copy=copy: copy().wait_recv())

    def pump(self, step):
        @pl.when(step < self.parts)
        def _():
            self.start(0, step)

        for hop in range(self.n - 1):
            part = step - LINE_LAG * (hop + 1)

            @pl.when((part >= 0) & (part < self.parts))
            def _(hop=hop, part=part):
                self.arrive(hop, part)
                if hop + 1 < self.n - 1:
                    self.start(hop + 1, part)

    def drain(self, part):
        for hop in range(self.n - 1):
            for condition, copy in self.moves(hop, part)[0]:
                pl.when(condition)(lambda copy=copy: copy().wait_send())


def entry_peers(cube, heads):
    z = lax.axis_index("head")
    peers = [cube.peer(step) for step in cube.orders[0]]
    return peers + [{"head": lax.rem(z + d, heads)} for d in range(1, heads)]


def greet(peers):
    for peer in peers:
        pl.semaphore_signal(pltpu.get_barrier_semaphore(), inc=1, device_id=peer, device_id_type=MESH)


def stage_one(m, cube, nz, sems, line):
    z = lax.axis_index("head")
    r = cube.rank()
    rows = m.wq.shape[0]
    colors = m.gq.shape[1]
    half = rows // colors
    nh = m.q.shape[0]
    frames = m.x.shape[0]
    padded = m.xp.shape[0]
    tile = 128
    tiles = padded // tile
    width = m.x.shape[1]

    peers = entry_peers(cube, nz)
    greet(peers)
    gk = Gather(cube, sems, lambda b, c: m.gk.at[b, c], colors)
    gq = Gather(cube, sems, lambda b, c: m.gq.at[b, c], colors)
    gv = Gather(cube, sems, lambda b, c: m.gv.at[b], 1)
    g1 = Gather(cube, sems, lambda b, c: m.g1.at[b, c], colors)
    g2 = Gather(cube, sems, lambda b, c: m.g2.at[b, c], colors)
    go = Gather(cube, sems, lambda b, c: m.go.at[:, b, c], colors)

    m.vec[...] = fill(m.vec.shape, 0)
    for name in m.first_loads:
        m.load[name].wait()
    for row, ref in enumerate(m.shares):
        m.vec[row : row + 1, :rows] = ref[...].astype(F32)
    m.gv[r] = m.vec[:, :128]
    for c in range(colors):
        part = pl.ds(c * half, half)
        for h in range(nh):
            cols = slice(h * HEAD_DIM, (h + 1) * HEAD_DIM)
            m.gk[r, c, :, h * 128 : h * 128 + 64] = m.wk[part, cols]
            m.gk[r, c, :, h * 128 + 64 : (h + 1) * 128] = m.wv[part, cols]
        m.gq[r, c, :, : nh * 64] = m.wq[part, :]
        spare = m.gq.shape[3] - nh * 64
        if spare:
            m.gq[r, c, :, nh * 64 :] = fill((half, spare), 0, BF16)

    pl.semaphore_wait(pltpu.get_barrier_semaphore(), len(peers))
    gv.start(0, 0)
    for g in (gk, gq):
        for c in range(colors):
            g.start(0, c)

    for name in m.next_loads:
        m.load[name].wait()
    wot = m.wo[...].T
    for c in range(colors):
        part = slice(c * half, (c + 1) * half)
        m.go[z, r, c] = wot[part]
        m.g2[r, c] = m.w2[part, :]
        m.g1[r, c] = m.w1[part, :]
    out_sems = [sems.take() for _ in range(nz - 1)]

    def out_copies(arriving):
        for d in range(1, nz):
            origin = lax.rem(z + nz - d, nz) if arriving else z
            target = lax.rem(z + d, nz)
            piece = m.go.at[origin, r]
            yield remote(piece, piece, out_sems[d - 1], {"head": target})

    for copy in out_copies(False):
        copy.start()
    m.xp[0:frames] = m.x[...]
    m.xp[frames:padded] = fill((padded - frames, width), 0, BF16)

    def norm_tile(i, carry):
        at = pl.ds(pl.multiple_of(i * tile, tile), tile)
        xhat, _ = normalize(m.xp[at].astype(F32))
        m.xh2[at] = xhat
        return carry

    third = tiles // gq.steps
    for k in range(gq.steps):
        top = tiles if k == gq.steps - 1 else third * (k + 1)
        lax.fori_loop(third * k, top, norm_tile, 0)
        gv.advance(k, 0)
        for c in range(colors):
            gk.advance(k, c)
        if k < gq.steps - 1:
            for c in range(colors):
                gq.advance(k, c)
        if k == 0:
            for g in (g1, g2):
                for c in range(colors):
                    g.start(0, c)
    for b in range(cube.size):
        m.vec[:, b * rows : (b + 1) * rows] = m.gv[b, :, :rows]
    gain, shift = m.vec[0:1, :], m.vec[1:2, :]
    m.bias[...] = fill(m.bias.shape, 0)
    bv = m.bv[...].astype(F32)[None, :]
    for h in range(nh):
        m.bias[0:1, h * 128 + 64 : (h + 1) * 128] = bv[:, h * HEAD_DIM : (h + 1) * HEAD_DIM]
    m.bias[1:2, : nh * 64] = m.bq[...].astype(F32)[None, :]
    scale = HEAD_DIM**-0.5

    def project(i, carry):
        at = pl.ds(pl.multiple_of(i * tile, tile), tile)
        n1 = (m.xh2[at] * gain + shift).astype(BF16)
        m.n1[at] = n1
        packed = dot(n1, m.gk[...].reshape(cube.size * rows, nh * 128)) + m.bias[0:1, : nh * 128]
        for h in range(nh):
            m.kv[0, h, at] = packed[:, h * 128 : (h + 1) * 128].astype(BF16)
        return carry

    lax.fori_loop(0, tiles, project, 0)

    kv_sems = [sems.take() for _ in range(nh)]
    other = {"seq": flip(lax.axis_index("seq"), 1)}
    kv_copies = [
        remote(m.kv.at[0, h], m.kv.at[1, h], kv_sems[h], other) for h in range(nh)
    ]
    kv_copies[0].start()
    for copy in out_copies(True):
        copy.wait_recv()
    for c in range(colors):
        go.start(0, c)
    for copy in kv_copies[1:]:
        copy.start()
    for c in range(colors):
        gq.advance(gq.steps - 1, c)

    def project_query(i, carry):
        at = pl.ds(pl.multiple_of(i * tile, tile), tile)
        wide = m.gq.shape[3]
        packed = dot(m.n1[at], m.gq[...].reshape(cube.size * rows, wide)) + m.bias[1:2, :wide]
        left = lane((tile, 128)) < 64
        for h in range(nh):
            pair = packed[:, (h // 2) * 128 : (h // 2) * 128 + 128]
            if h % 2:
                pair = pltpu.roll(pair, 64, 1)
            pair = pair.astype(BF16).astype(F32) * scale
            m.q[h, at] = jnp.where(left, pair, 0.0).astype(BF16)
        return carry

    lax.fori_loop(0, tiles, project_query, 0)

    left = lane((padded, 128)) < 64

    def prepare(part, h):
        block = m.kv[part, h]
        m.kvt[part, h] = block.T
        m.vo[part, h] = jnp.where(left, jnp.ones_like(block), block)

    for h in range(nh):
        prepare(0, h)
    m.load["cot"].wait()
    m.gp[0:frames] = m.cot[...]
    m.gp[frames:padded] = fill((padded - frames, width), 0, BF16)
    m.acc[...] = fill(m.acc.shape, 0)

    block = 256
    valid = frames - (padded - 128)

    def attend(h):
        def one(b, carry):
            at = pl.ds(pl.multiple_of(b * block, block), block)
            query = m.q[h, at]
            keep = lane((block, 128)) < valid
            parts = []
            top = None
            for part in range(2):
                s = dot(query, m.kvt[part, h])
                body, tail = s[:, : padded - 128], s[:, padded - 128 :]
                tail = jnp.where(keep, tail, NEG)
                parts += [body, tail]
                high = jnp.maximum(jnp.max(body, axis=1, keepdims=True), jnp.max(tail, axis=1, keepdims=True))
                top = high if top is None else jnp.maximum(top, high)
            place = 0
            for s in parts:
                m.p[h, at, place : place + s.shape[1]] = jnp.exp(s - top).astype(BF16)
                place += s.shape[1]
            acc = dot(m.p[h, at, :padded], m.vo[0, h]) + dot(m.p[h, at, padded:], m.vo[1, h])
            inverse = 1.0 / pltpu.roll(acc, 64, 1)
            att = acc * inverse
            right = lane((block, 128)) >= 64
            m.il[h, at] = jnp.where(right, inverse, 0.0)
            m.atto[h, at] = jnp.where(right, att, 0.0).astype(BF16)
            turned = pltpu.roll(att, 64, 1)
            pieces = [
                jnp.where(right[:64], att[g + 64 : g + 128], turned[g : g + 64])
                for g in range(0, block, 128)
            ]
            part = h * (padded // block) + b
            m.attz[z, part] = jnp.concatenate(pieces, axis=0).astype(BF16)
            line.pump(part)
            return carry

        lax.fori_loop(0, padded // block, one, 0)

    def weights(gathers, k, c):
        if c < colors and k < g1.steps - 1:
            for g in gathers:
                g.advance(k, c)

    feed = (g1, g2)
    plan = {0: ((feed, 0, 0), (feed, 0, 1)), 1: (((go,), 0, 0), ((go,), 0, 1))}
    plan[nh - 1] = ((feed, 1, 0),)
    for h in range(nh):
        kv_copies[h].wait_recv()
        prepare(1, h)
        attend(h)
        for job in plan.get(h, ()):
            weights(*job)
    parts = line.parts
    stop = parts + LINE_LAG * (nz - 1)
    loop(parts, parts + 3, line.pump)
    weights((go,), 1, 0)
    weights(feed, 1, 1)
    loop(parts + 3, stop - 2, line.pump)
    weights((go,), 1, 1)
    loop(stop - 2, stop, line.pump)
    for k in range(2, g1.steps):
        for g in (go, g1, g2):
            for c in range(colors):
                g.advance(k, c)

    def drain():
        for copy in kv_copies:
            copy.wait_send()
        for copy in out_copies(False):
            copy.wait_send()
        for g in (gv, gk, gq, g1, g2, go):
            g.drain()
        loop(0, line.parts, line.drain)

    return drain


class Scatter:
    def __init__(self, cube, sems, buffer, landing, rows, colors):
        self.cube, self.buffer, self.landing = cube, buffer, landing
        self.rows, self.colors, self.half = rows, colors, rows // colors
        self.steps = len(cube.orders[0])
        self.plan = [[[] for _ in range(self.steps)] for _ in range(colors)]
        for color in range(colors):
            masks, slot = [0], 0
            for k, step in enumerate(cube.orders[color]):
                for mask in masks:
                    copy = remote(
                        self.view(cube.block(mask ^ step[0]), color),
                        landing.at[color, slot],
                        sems.take(),
                        cube.peer(step),
                    )
                    self.plan[color][k].append((mask, slot, copy))
                    slot += 1
                masks = masks + [mask ^ step[0] for mask in masks]

    def view(self, block, color):
        start = block * self.rows + color * self.half
        return self.buffer.at[pl.ds(pl.multiple_of(start, 8), self.half)]

    def start(self):
        self.left = self.steps - 1
        self.send(self.left)

    def step(self):
        if self.left > 0:
            self.advance(self.left)
            self.left -= 1

    def send(self, k):
        for color in range(self.colors):
            for _, _, copy in self.plan[color][k]:
                copy.start()

    def advance(self, k):
        for color in range(self.colors):
            for mask, slot, copy in self.plan[color][k]:
                copy.wait_recv()
                view = self.view(self.cube.block(mask), color)
                total = view[...].astype(F32) + self.landing[color, slot].astype(F32)
                view[...] = total.astype(BF16)
            for _, _, copy in self.plan[color][k - 1]:
                copy.start()

    def finish(self):
        while self.left > 0:
            self.step()
        parts = []
        for color in range(self.colors):
            ((_, slot, copy),) = self.plan[color][0]
            copy.wait_recv()
            view = self.view(self.cube.block(0), color)
            parts.append(view[...].astype(F32) + self.landing[color, slot].astype(F32))
        return parts[0] if len(parts) == 1 else jnp.concatenate(parts, axis=0)

    def drain(self):
        for color in range(self.colors):
            for step in self.plan[color]:
                for _, _, copy in step:
                    copy.wait_send()


class LineSum:
    def __init__(self, nz, send, recv, ends, middle, chunks, rows, part, landed, crossed, total):
        z = lax.axis_index("head")
        self.inner = (z > 0) & (z < nz - 1)
        self.mate, self.cross = {"head": flip(z, 1)}, {"head": nz - 1 - z}
        self.send_sem, self.recv_sem, self.bases = send, recv, (ends, middle, ends)
        self.chunks, self.rows = chunks, rows
        self.part, self.landed, self.crossed, self.total = part, landed, crossed, total

    def at(self, ref, i):
        return ref.at[pl.ds(pl.multiple_of(i * self.rows, self.rows), self.rows)]

    def sems(self, kind, i):
        place = self.bases[kind] + i
        return self.send_sem.at[place], self.recv_sem.at[place]

    def first(self, i):
        return remote(self.at(self.part, i), self.at(self.landed, i), self.sems(0, i), self.mate)

    def second(self, i):
        return remote(self.at(self.part, i), self.at(self.crossed, i), self.sems(1, i), self.cross)

    def third(self, i):
        piece = self.at(self.total, i)
        return remote(piece, piece, self.sems(2, i), self.mate)

    def offer(self, i):
        @pl.when(jnp.logical_not(self.inner))
        def _():
            self.first(i).start()

    def relay(self, i):
        @pl.when(self.inner)
        def _():
            self.first(i).wait_recv()
            view = self.at(self.part, i)
            total = view[...].astype(F32) + self.at(self.landed, i)[...].astype(F32)
            view[...] = total.astype(BF16)
            self.second(i).start()

    def pump(self, i):
        @pl.when(i < self.chunks)
        def _():
            self.relay(i)

        @pl.when(i >= LAG)
        def _():
            self.close(i - LAG)

    def step(self, i, lag):
        if i < self.chunks:
            self.relay(i)
        if i >= lag:
            self.close(i - lag)

    def close(self, i):
        @pl.when(self.inner)
        def _():
            self.second(i).wait_recv()
            total = self.at(self.part, i)[...].astype(F32) + self.at(self.crossed, i)[...].astype(F32)
            self.at(self.total, i)[...] = total.astype(BF16)
            self.third(i).start()

    def accept(self, i):
        @pl.when(jnp.logical_not(self.inner))
        def _():
            self.third(i).wait_recv()

    def drain(self, i):
        @pl.when(self.inner)
        def _():
            self.second(i).wait_send()
            self.third(i).wait_send()

        @pl.when(jnp.logical_not(self.inner))
        def _():
            self.first(i).wait_send()


def loop(start, stop, step):
    lax.fori_loop(start, stop, lambda i, carry: (step(i), carry)[1], 0)


def rows_of(i, size):
    return pl.ds(pl.multiple_of(i * size, size), size)


def add_rows(m, row, values):
    count, width = values.shape
    m.acc[row, :, :width] += jnp.sum(values.reshape(count // 8, 8, width), axis=0)


B_FC_TWO, GAIN_TWO, SHIFT_TWO, B_OUT, GAIN_ONE, SHIFT_ONE, B_QKV, B_FC_ONE = range(8)
BLOCK = 256
STEP = 128
CHUNK = 32
LAG = 4
OUT_LAG = 2


def stage_two(m, cube, nz, sum_two, sum_out):
    padded, width = m.xp.shape
    rows = m.wq.shape[0]
    nh = m.q.shape[0]
    frames = m.cot.shape[0]
    hidden = m.w1.shape[1]
    gain, shift, b_out = m.vec[2:3, :], m.vec[3:4, :], m.vec[4:5, :]
    b_one = m.bf1[...].astype(F32)[None, :]
    per = STEP // CHUNK
    w_one = lambda: m.g1[...].reshape(cube.size * rows, hidden)
    w_two = lambda: m.g2[...].reshape(cube.size * rows, hidden)

    def block(b):
        at = rows_of(b, STEP)
        packed = rows_of(lax.rem(b, 2), STEP // 2)
        mid = m.xp[at].astype(F32) + b_out
        for zz in range(nz):
            pieces = [m.attz[zz, h * (padded // BLOCK) + lax.div(b, 2), packed] for h in range(nh)]
            top = jnp.concatenate([p[:, :64] for p in pieces], axis=1)
            low = jnp.concatenate([p[:, 64:] for p in pieces], axis=1)
            att = jnp.concatenate([top, low], axis=0)
            mid = mid + dot_nt(att, m.go[zz].reshape(cube.size * rows, nh * HEAD_DIM))
        xhat, inverse = normalize(mid)
        m.mid[at] = mid
        m.xh2[at] = xhat
        m.r2[at] = jnp.broadcast_to(inverse, (STEP, 128))
        n2 = (xhat * gain + shift).astype(BF16)
        m.n2[at] = n2
        pre = dot(n2, w_one()) + b_one
        cdf = 0.5 + 0.5 * lax.erf(pre * 0.7071067811865476)
        act = (pre * cdf).astype(BF16)
        m.act[at] = act
        slope = cdf + pre * jnp.exp(pre * pre * -0.5) * 0.3989422804014327
        g = m.gp[at]
        add_rows(m, B_FC_TWO, g.astype(F32))
        gpre = (dot(g, w_two()) * slope).astype(BF16)
        m.gpre[at] = gpre
        add_rows(m, B_FC_ONE, gpre.astype(F32))
        back = dot_nt(gpre, w_one())
        m.part[at] = back.astype(BF16)
        loop(0, per, lambda j: sum_two.offer(b * per + j))
        add_rows(m, GAIN_TWO, back * m.xh2[at])
        add_rows(m, SHIFT_TWO, back)

        @pl.when(b >= 2)
        def _():
            sum_two.pump(2 * b - 4)
            sum_two.pump(2 * b - 3)

        m.opart[at] = dot_nt(m.act[at], w_two()).astype(BF16)

    loop(0, padded // STEP, block)
    loop(0, sum_out.chunks, sum_out.offer)


def stage_three(m, cube, nz, sems, sum_two, sum_out, sum_one, drain):
    z = lax.axis_index("head")
    padded, width = m.xp.shape
    rows = m.wq.shape[0]
    nh = m.q.shape[0]
    local = nh * HEAD_DIM
    colors = m.gq.shape[1]
    chunks = padded // CHUNK
    blocks = padded // BLOCK
    per = STEP // CHUNK
    scale = HEAD_DIM**-0.5
    packed = m.gk.shape[3] + m.gq.shape[3]
    s1 = Scatter(cube, sems, m.dw1, m.dl1, rows, colors)
    s2 = Scatter(cube, sems, m.dw2, m.dl2, rows, colors)
    so = Scatter(cube, sems, m.dwo, m.dlo, rows, colors)
    sq = Scatter(cube, sems, m.dwq, m.dlq, rows, colors)
    tile = 128
    tiles = width // tile

    def product(left, right, into, columns):
        def one(i):
            cols = pl.ds(pl.multiple_of(i * tile, tile), tile)
            into[rows_of(i, tile)] = dot_tn(left[:, cols], right())[:, :columns].astype(BF16)

        return one

    one = product(m.n2, lambda: m.gpre[...], m.dw1, m.dw1.shape[1])
    two = product(m.gp, lambda: m.act[...], m.dw2, m.dw2.shape[1])

    def first(i):
        one(i)
        sum_two.pump(early + i)

    def second(i):
        two(i)
        sum_two.pump(early + tiles + i)

    early = 2 * (padded // STEP - 2)

    loop(0, tiles, first)
    s1.start()
    loop(0, tiles, second)
    s2.start()
    for h in range(nh):
        m.qt[h] = m.q[h].T
    gain_two = m.vec[2:3, :]

    def middle(i):
        sum_two.accept(i)
        at = rows_of(i, CHUNK)
        n = m.total[at].astype(F32)
        e = n * gain_two
        xhat = m.xh2[at]
        r = m.r2[at][:, :1]
        mean = jnp.mean(e, axis=-1, keepdims=True)
        along = jnp.mean(e * xhat, axis=-1, keepdims=True)
        grad = m.gp[at].astype(F32) + r * (e - mean - xhat * along)
        m.xh2[at] = grad
        add_rows(m, B_OUT, grad)
        low = grad.astype(BF16)
        m.n2[at] = low
        da = dot(low, m.go[z].reshape(cube.size * rows, local)).astype(BF16).astype(F32)
        right = lane((CHUNK, 128)) >= 64
        for h in range(nh):
            base = (h // 2) * 128
            wide = da[:, base : min(base + 128, local)]
            if wide.shape[1] < 128:
                wide = jnp.concatenate([wide, jnp.zeros((CHUNK, 128 - wide.shape[1]), F32)], axis=1)
            if h % 2 == 0:
                wide = pltpu.roll(wide, 64, 1)
            m.act[at, h * 128 : (h + 1) * 128] = jnp.where(right, wide * m.il[h, at], 0.0).astype(BF16)
            m.at[at, h * 64 : (h + 1) * 64] = m.atto[h, at][:, 64:]

    ahead = early + 2 * tiles
    stop = chunks + LAG - ahead
    each = chunks // stop

    def pumped(i):
        sum_two.pump(i + ahead)
        loop(i * each, (i + 1) * each, middle)

    taken = []

    def out_step():
        if len(taken) < sum_out.chunks + OUT_LAG:
            sum_out.step(len(taken), OUT_LAG)
            taken.append(None)

    s1.step()
    fourth = stop // 4
    for part in range(4):
        loop(part * fourth, stop if part == 3 else (part + 1) * fourth, pumped)
        (s2, s1)[part % 2].step()
        if part >= 2:
            out_step()
    loop(stop * each, chunks, middle)
    out_step()

    for h in range(nh):
        m.dat[h] = m.act[:, h * 128 : (h + 1) * 128].T
    big = sum_out.chunks
    out_step()
    kv_sems = [sems.take() for _ in range(nh)]
    other = {"seq": flip(lax.axis_index("seq"), 1)}
    kv_copies = [remote(m.kvs.at[h], m.kvr.at[h], kv_sems[h], other) for h in range(nh)]
    for h in range(nh):

        def back(b, h=h):
            at = rows_of(b, BLOCK)
            da = m.act[at, h * 128 : (h + 1) * 128]
            inner = jnp.sum(da.astype(F32) * m.atto[h, at].astype(F32), axis=1, keepdims=True)
            for part in (1, 0):
                keys = slice(part * padded, (part + 1) * padded)
                dp = dot(da, m.kvt[part, h])
                m.ds[at, keys] = (m.p[h, at, keys].astype(F32) * (dp - inner)).astype(BF16)
            dq = dot(m.ds[at, :padded], m.kv[0, h]) + dot(m.ds[at, padded:], m.kv[1, h])
            dq = (dq * scale)[:, :64].astype(BF16)
            m.gpre[at, nh * 128 + h * 64 : nh * 128 + (h + 1) * 64] = dq

        loop(0, blocks, back)
        out_step()
        far, own = slice(padded, 2 * padded), slice(0, padded)
        m.kvs[h] = (dot(m.qt[h], m.ds[:, far]) + dot(m.dat[h], m.p[h, :, far])).astype(BF16)
        kv_copies[h].start()
        m.dkv[h] = dot(m.qt[h], m.ds[:, own]) + dot(m.dat[h], m.p[h, :, own])
        out_step()
    spare = packed - nh * 192
    if spare:
        m.gpre[:, nh * 192 : packed] = fill((padded, spare), 0, BF16)
    for h in range(nh):
        kv_copies[h].wait_recv()
        total = m.dkv[h] + m.kvr[h].astype(F32)
        m.gpre[:, h * 128 : (h + 1) * 128] = total.T.astype(BF16)

    out_step()
    def last(b):
        at = rows_of(b, STEP)
        grads = m.gpre[at, :packed]
        add_rows(m, B_QKV, grads.astype(F32))
        keys = nh * 128
        back = dot_nt(grads[:, :keys], m.gk[...].reshape(cube.size * rows, keys))
        back = back + dot_nt(grads[:, keys:], m.gq[...].reshape(cube.size * rows, packed - keys))
        m.part[at] = back.astype(BF16)
        loop(0, per, lambda j: sum_one.offer(b * per + j))
        xhat, _ = normalize(m.xp[at].astype(F32))
        add_rows(m, GAIN_ONE, back * xhat)
        add_rows(m, SHIFT_ONE, back)

    loop(0, chunks, sum_two.drain)
    loop(0, padded // STEP, last)
    out_step()
    for row in range(8):
        m.vs[row : row + 1, :] = jnp.sum(m.acc[row], axis=0, keepdims=True)
    cube_peers = [cube.peer(step) for step in cube.orders[0]]
    vec_copies = []

    def vec_send(k):
        if k < len(cube_peers):
            m.vo_[k] = m.vs[...]
            vec_copies.append(remote(m.vo_.at[k], m.vr.at[k], sems.take(), cube_peers[k]))
            vec_copies[-1].start()
            return
        m.vo_[k] = m.vs[...]
        for d in range(1, nz):
            target = {"head": lax.rem(z + d, nz)}
            vec_copies.append(remote(m.vo_.at[k], m.vr.at[k + d - 1], sems.take(), target))
            vec_copies[-1].start()

    def vec_take(k):
        if k < len(cube_peers):
            vec_copies[k].wait_recv()
            m.vs[...] += m.vr[k]
            vec_send(k + 1)

    vec_send(0)
    one_q = product(m.n1, lambda: m.gpre[:, :packed], m.dwq, packed)
    one_o = product(m.n2, lambda: m.at[...], m.dwo, local)

    def qkv(i):
        one_q(i)
        sum_one.pump(i)

    def out(i):
        one_o(i)
        sum_one.pump(tiles + i)

    half = tiles // 2
    loop(0, half, qkv)
    out_step()
    loop(half, tiles, qkv)
    sq.start()
    out_step()
    vec_take(0)
    loop(0, half, out)
    out_step()
    loop(half, tiles, out)
    so.start()
    while len(taken) < sum_out.chunks + OUT_LAG:
        out_step()
    vec_take(1)

    b_two = m.vec[5:6, :]

    def output(i):
        sum_out.accept(i)
        at = rows_of(i, sum_out.rows)
        m.ototal[at] = (m.mid[at] + m.ototal[at].astype(F32) + b_two).astype(BF16)

    gain_one = m.vec[0:1, :]

    def final(i):
        sum_one.accept(i)
        at = rows_of(i, CHUNK)
        e = m.total[at].astype(F32) * gain_one
        xhat, r = normalize(m.xp[at].astype(F32))
        mean = jnp.mean(e, axis=-1, keepdims=True)
        along = jnp.mean(e * xhat, axis=-1, keepdims=True)
        m.igrad[at] = m.xh2[at] + r * (e - mean - xhat * along)

    ahead = 2 * tiles
    stop = chunks + LAG - ahead
    turn = 2 * stop - chunks

    def tail(i):
        sum_one.pump(i + ahead)
        final(i)

    def faster(i):
        sum_one.pump(i + ahead)
        final(2 * i - turn)
        final(2 * i - turn + 1)

    def unpack():
        got = sq.finish()
        for h in range(nh):
            cols = slice(h * HEAD_DIM, (h + 1) * HEAD_DIM)
            m.owk[:, cols] = got[:, h * 128 : h * 128 + 64]
            m.owv[:, cols] = got[:, h * 128 + 64 : (h + 1) * 128]
        m.owq[...] = got[:, nh * 128 : nh * 128 + local]
        for name in ("owk", "owv", "owq"):
            m.save[name].start()

    def vectors():
        row_id = lax.broadcasted_iota(jnp.int32, m.vs.shape, 0)
        summed = (row_id == GAIN_TWO) | (row_id == SHIFT_TWO) | (row_id == GAIN_ONE) | (row_id == SHIFT_ONE)
        base = len(cube_peers)
        for d in range(1, nz):
            vec_copies[base + d - 1].wait_recv()
        rest = sum(m.vr[base + d - 1] for d in range(1, nz))
        m.vs[...] += jnp.where(summed, rest, 0.0)
        m.ovec[...] = fill(m.ovec.shape, 0)
        names = (GAIN_ONE, SHIFT_ONE, B_OUT, GAIN_TWO, SHIFT_TWO, B_FC_TWO)
        for b in range(cube.size):

            @pl.when(cube.rank() == b)
            def _(b=b):
                for place, row in enumerate(names):
                    m.ovec[place : place + 1, :rows] = m.vs[row : row + 1, b * rows : (b + 1) * rows]

        m.ovec[6:7, :local] = m.vs[B_QKV : B_QKV + 1, nh * 128 : nh * 192]
        for h in range(nh):
            m.ovec[7:8, h * 64 : (h + 1) * 64] = m.vs[B_QKV : B_QKV + 1, h * 128 + 64 : (h + 1) * 128]
        m.ovec[8:9, :] = m.vs[B_FC_ONE : B_FC_ONE + 1, :]
        m.save["ovec"].start()

    def outputs():
        loop(0, big, sum_out.drain)
        loop(0, big, output)
        m.save["ototal"].start()

    def early():
        m.ow1[...] = s1.finish()
        m.save["ow1"].start()
        m.ow2[...] = s2.finish()
        m.save["ow2"].start()

    def first_job():
        sq.step()

    def second_job():
        for k in range(2, len(cube_peers)):
            vec_take(k)

    def third_job():
        drain()
        sq.step()
        so.step()

    def sixth_job():
        unpack()
        m.owo[...] = so.finish().T
        m.save["owo"].start()
        for scatter in (s1, s2, so, sq):
            scatter.drain()

    def fourth_job():
        outputs()
        so.step()

    jobs = (first_job, second_job, third_job, fourth_job, early, sixth_job)
    near = turn // 3
    ends = [near, 2 * near, turn]
    far = (stop - turn) // 4
    ends += [turn + far, turn + 2 * far, turn + 3 * far, stop]
    begin = 0
    saved = 0
    for place, end in enumerate(ends):
        loop(begin, end, tail if end <= turn else faster)
        begin = end
        done = (end if end <= turn else 2 * end - turn) * CHUNK
        m.save_rows(saved, done - saved).start()
        saved = done
        if place < len(jobs):
            jobs[place]()
    assert saved == padded
    vectors()

    for copy in kv_copies + vec_copies:
        copy.wait_send()
    loop(0, chunks, sum_one.drain)


def layer(tokens, shares, biases, weights, mesh_shape):
    nz = mesh_shape["head"]
    cube = Cube(mesh_shape["clip"], mesh_shape["seq"])
    frames, width = tokens[0].shape
    rows, local = weights[0].shape
    hidden = weights[4].shape[1]
    nh = local // HEAD_DIM
    padded = -(-frames // BLOCK) * BLOCK
    colors = 2 if rows % 32 == 0 else 1
    half = rows // colors
    packed = -(-(nh * 192) // 128) * 128
    nb = cube.size
    steps = len(cube.all_bits) + nz - 1
    token_names, bias_names = ("x", "cot"), ("bq", "bv", "bf1")
    weight_names = ("wq", "wk", "wv", "wo", "w1", "w2")
    share_names = tuple(f"share{i}" for i in range(len(shares)))
    names = token_names + share_names + bias_names + weight_names
    parts = nh * (padded // BLOCK)
    ins = dict(zip(names, (*tokens, *shares, *biases, *weights)))
    outs = dict(
        ototal=((padded, width), BF16),
        igrad=((padded, width), F32),
        ovec=((16, width), F32),
        owq=((rows, local), F32),
        owk=((rows, local), F32),
        owv=((rows, local), F32),
        owo=((local, rows), F32),
        ow1=((rows, hidden), F32),
        ow2=((rows, hidden), F32),
    )
    flat = (padded, width)
    scratch = dict(
        gk=((nb, colors, half, nh * 128), BF16),
        gq=((nb, colors, half, packed - nh * 128), BF16),
        go=((nz, nb, colors, half, local), BF16),
        g1=((nb, colors, half, hidden), BF16),
        g2=((nb, colors, half, hidden), BF16),
        gv=((nb, 8, 128), F32),
        vec=((8, width), F32),
        bias=((8, packed), F32),
        mid=(flat, F32),
        n1=(flat, BF16),
        q=((nh, padded, 128), BF16),
        kv=((2, nh, padded, 128), BF16),
        kvt=((2, nh, 128, padded), BF16),
        vo=((2, nh, padded, 128), BF16),
        p=((nh, padded, 2 * padded), BF16),
        il=((nh, padded, 128), F32),
        atto=((nh, padded, 128), BF16),
        attz=((nz, parts, BLOCK // 2, 128), BF16),
        xp=(flat, BF16),
        gp=(flat, BF16),
        xh2=(flat, F32),
        r2=((padded, 128), F32),
        n2=(flat, BF16),
        act=((padded, hidden), BF16),
        gpre=((padded, hidden), BF16),
        acc=((8, 8, width), F32),
        vs=((8, width), F32),
        vo_=((steps, 8, width), F32),
        vr=((steps, 8, width), F32),
        part=(flat, BF16),
        landed=(flat, BF16),
        crossed=(flat, BF16),
        crossed_one=(flat, BF16),
        total=(flat, BF16),
        opart=(flat, BF16),
        olanded=(flat, BF16),
        ocrossed=(flat, BF16),
        at=((padded, local), BF16),
        qt=((nh, 128, padded), BF16),
        dat=((nh, 128, padded), BF16),
        dkv=((nh, 128, padded), F32),
        kvs=((nh, 128, padded), BF16),
        kvr=((nh, 128, padded), BF16),
        ds=((padded, 2 * padded), BF16),
        dw1=((width, hidden), BF16),
        dl1=((colors, nb - 1, half, hidden), BF16),
        dw2=((width, hidden), BF16),
        dl2=((colors, nb - 1, half, hidden), BF16),
        dwo=((width, local), BF16),
        dlo=((colors, nb - 1, half, local), BF16),
        dwq=((width, packed), BF16),
        dlq=((colors, nb - 1, half, packed), BF16),
    )
    small, large = padded // CHUNK, 12
    sums = 3 * small + 2 * large
    lines = sums + Line.count(nz, parts)
    count = lines + (9 * colors + 1) * (nb - 1) + (nz - 1) + 2 * nh + steps

    def body(*refs):
        far_in, far_out = refs[: len(ins)], refs[len(ins) : len(ins) + len(outs)]
        names = list(ins) + list(outs) + list(scratch)
        refs = refs[len(ins) + len(outs) :]
        m = types.SimpleNamespace(**dict(zip(names, refs)))
        send, recv, move = refs[len(names) :]
        m.load = {
            name: pltpu.make_async_copy(far, getattr(m, name), move.at[i])
            for i, (name, far) in enumerate(zip(ins, far_in))
        }
        m.save = {
            name: pltpu.make_async_copy(getattr(m, name), far, move.at[len(ins) + i])
            for i, (name, far) in enumerate(zip(outs, far_out))
            if name != "igrad"
        }
        rows_far = far_out[list(outs).index("igrad")]

        def save_rows(start, size):
            part = pl.ds(start, size)
            at = len(ins) + len(outs) + len(m.saved)
            m.saved.append(pltpu.make_async_copy(m.igrad.at[part], rows_far.at[part], move.at[at]))
            return m.saved[-1]

        m.saved, m.save_rows = [], save_rows
        m.first_loads = share_names + ("wk", "wv", "wq")
        m.next_loads = ("wo", "w1", "w2", "x", *bias_names)
        for name in (*m.first_loads, *m.next_loads, "cot"):
            m.load[name].start()
        m.shares = [getattr(m, name) for name in share_names]
        sems = Sems(send, recv)
        sems.used = lines
        sum_two = LineSum(nz, send, recv, 0, small, small, CHUNK, m.part, m.landed, m.crossed, m.total)
        sum_one = LineSum(nz, send, recv, 0, 2 * small, small, CHUNK, m.part, m.landed, m.crossed_one, m.total)
        sum_out = LineSum(
            nz, send, recv, 3 * small, 3 * small + large, large, padded // large, m.opart, m.olanded, m.ocrossed, m.ototal
        )
        line = Line(nz, send, recv, sums, lambda origin, part: m.attz.at[origin, part], parts)
        drain = stage_one(m, cube, nz, sems, line)
        stage_two(m, cube, nz, sum_two, sum_out)
        stage_three(m, cube, nz, sems, sum_two, sum_out, sum_one, drain)
        assert sems.used == count, (sems.used, count)
        for copy in (*m.save.values(), *m.saved):
            copy.wait()

    res = pl.pallas_call(
        body,
        out_shape=[jax.ShapeDtypeStruct(*v) for v in outs.values()],
        in_specs=[pl.BlockSpec(memory_space=pl.ANY)] * len(ins),
        out_specs=[pl.BlockSpec(memory_space=pl.ANY)] * len(outs),
        scratch_shapes=[pltpu.VMEM(a.shape, a.dtype) for a in ins.values()]
        + [pltpu.VMEM(*v) for v in (outs | scratch).values()]
        + [pltpu.SemaphoreType.DMA((count,))] * 2
        + [pltpu.SemaphoreType.DMA((len(ins) + len(outs) + 7,))],
        compiler_params=pltpu.CompilerParams(
            collective_id=0, has_side_effects=True, vmem_limit_bytes=67_043_328
        ),
        name="layer",
    )(*ins.values())
    return types.SimpleNamespace(**dict(zip(outs, res)))


def finish(res, frames):
    padded, width = res.ototal.shape
    rows, local = res.owq.shape
    hidden = res.ow1.shape[1]
    tile = 256
    sizes = [rows] * 6 + [local] * 2
    passed = (res.owq, res.owk, res.owv, res.owo, res.ow1, res.ow2)
    n = len(passed)

    def body(out_far, grad_far, vec_far, *refs):
        far, (to_out, to_grad, *to) = refs[:n], refs[n : 2 * n + 2 + 9]
        out_near, grad_near, vec_near, *near = refs[2 * n + 11 : 3 * n + 14]
        grad_flat, *flat = refs[3 * n + 14 : -1]
        sem = refs[-1]
        copy = lambda i, a, b: pltpu.make_async_copy(a, b, sem.at[i])
        pieces = [(t, min(tile, padded - t)) for t in range(0, padded, tile)]
        loads = [
            copy(i, grad_far.at[pl.ds(t, size)], grad_near.at[pl.ds(t, size)]) for i, (t, size) in enumerate(pieces)
        ]
        k = len(pieces)
        others = [copy(k + i, a, b) for i, (a, b) in enumerate(zip((vec_far, out_far, *far), (vec_near, out_near, *near)))]
        for c in loads + others:
            c.start()
        k += len(others)
        saves = []

        def save(a, b):
            saves.append(copy(k + len(saves), a, b))
            saves[-1].start()

        for c, (t, size) in zip(loads, pieces):
            c.wait()
            size = min(size, frames - t)
            grad_flat[t : t + size, 0, :] = grad_near[t : t + size]
            save(grad_flat.at[pl.ds(t, size)], to_grad.at[pl.ds(t, size)])
        others[0].wait()
        for i in range(8):
            flat[i][...] = vec_near[i : i + 1, : sizes[i]]
        for i in range(hidden // 128):
            flat[8][i : i + 1, :] = vec_near[8:9, i * 128 : (i + 1) * 128]
        others[1].wait()
        flat[9][...] = out_near[0:frames]
        save(flat[9], to_out)
        for i in range(9):
            save(flat[i], to[n + i])
        for c, a, b in zip(others[2:], near, to):
            c.wait()
            save(a, b)
        for c in saves:
            c.wait()

    vectors = [jax.ShapeDtypeStruct((1, size), F32) for size in sizes]
    vectors.append(jax.ShapeDtypeStruct((hidden // 128, 128), F32))
    kept = [jax.ShapeDtypeStruct(a.shape, a.dtype) for a in passed]
    final = jax.ShapeDtypeStruct((frames, width), BF16)
    grads = jax.ShapeDtypeStruct((frames, 1, width), F32)
    given = (res.ototal, res.igrad, res.ovec, *passed)
    near = [*given, grads, *vectors, final]
    return pl.pallas_call(
        body,
        out_shape=[final, grads, *kept, *vectors],
        in_specs=[pl.BlockSpec(memory_space=pl.ANY)] * len(given),
        out_specs=[pl.BlockSpec(memory_space=pl.ANY)] * (2 + n + 9),
        scratch_shapes=[pltpu.VMEM(a.shape, a.dtype) for a in near] + [pltpu.SemaphoreType.DMA((-(-padded // tile) * 2 + 2 * n + 12,))],
        compiler_params=pltpu.CompilerParams(vmem_limit_bytes=67_043_328),
        name="finish",
    )(*given)


def on_device(
    inputs,
    gain_one,
    shift_one,
    w_query,
    b_query,
    w_key,
    w_value,
    b_value,
    w_out,
    b_out,
    gain_two,
    shift_two,
    w_fc_one,
    b_fc_one,
    w_fc_two,
    b_fc_two,
    cotangent,
    mesh_shape,
):
    clips, frames, width = inputs.shape
    count = clips * frames
    row = lambda v: v.reshape(1, -1)
    res = layer(
        (inputs.reshape(count, width), cotangent.reshape(count, width)),
        tuple(row(v) for v in (gain_one, shift_one, gain_two, shift_two, b_out, b_fc_two)),
        (b_query, b_value, b_fc_one),
        (w_query, w_key, w_value, w_out, w_fc_one, w_fc_two.T),
        mesh_shape,
    )
    outputs, grad, g_query, g_key, g_value, g_out, g_one, g_two, *vectors = finish(res, count)
    g1, s1, b_o, g2, s2, b_two, b_q, b_v, b_one = (v.reshape(-1) for v in vectors)
    return (
        outputs.reshape(clips, frames, width),
        grad.transpose(1, 0, 2).reshape(clips, frames, width),
        g1,
        s1,
        g_query,
        b_q,
        g_key,
        g_value,
        b_v,
        g_out,
        b_o,
        g2,
        s2,
        g_one,
        b_one,
        g_two.T,
        b_two,
    )


def solution(mesh):
    group = ("clip", "seq")
    rows, columns, own, heads = P(group, "head"), P("head", group), P(group), P("head")
    tokens = P("clip", "seq", None)
    return jax.shard_map(
        partial(on_device, mesh_shape=dict(mesh.shape)),
        mesh=mesh,
        in_specs=(
            tokens, own, own, rows, heads, rows, rows, heads, columns,
            own, own, own, rows, heads, columns, own, tokens,
        ),
        out_specs=(
            tokens, tokens, own, own, rows, heads, rows, rows, heads,
            columns, own, own, own, rows, heads, columns, own,
        ),
        check_vma=False,
    )
```
